32 devices in a mesh: dp: 8 (over y, x, core), tensor: 4 (over z).
Axes of the slice: x: 2, y: 2, z: 4, core: 2. Of those that a mesh axis runs over, the one named last changes fastest.
Arguments:
- inputs: bfloat16 [584, 16, 1024], P('tensor', 'dp'), may hold values from -6 to 6
- valid_mask: int32 [16, 584], P('dp'), may hold values from 0 to 1, as said below
- cotangent: bfloat16 [584, 16, 1024], P('tensor', 'dp'), may hold values from -60 to 60
- ln_gain: bfloat16 [2, 1024], P(None, 'dp'), may hold values from 0.25 to 1.75
- d_bias: bfloat16 [4, 1024], P(None, 'dp'), may hold values from -3 to 3
- w_qkv: bfloat16 [1024, 3, 1024], P('dp', None, 'tensor'), may hold values from -0.1875 to 0.1875
- b_qv: bfloat16 [2, 1024], P(None, 'tensor'), may hold values from -3 to 3
- w_o: bfloat16 [1024, 1024], P('tensor', 'dp'), may hold values from -2 to 2
- w_1: bfloat16 [1024, 4096], P('dp', 'tensor'), may hold values from -0.1875 to 0.1875
- b_1: bfloat16 [4096], P('tensor'), may hold values from -3 to 3
- w_2: bfloat16 [4096, 1024], P('tensor', 'dp'), may hold values from -0.09375 to 0.09375
Outputs:
- block_output: bfloat16 [584, 16, 1024], P('tensor', 'dp')
- grad_inputs: float32 [584, 16, 1024], P('tensor', 'dp')
- grad_ln_gain: float32 [2, 1024], P(None, 'dp')
- grad_d_bias: float32 [4, 1024], P(None, 'dp')
- grad_w_qkv: float32 [1024, 3, 1024], P('dp', None, 'tensor')
- grad_b_qv: float32 [2, 1024], P(None, 'tensor')
- grad_w_o: float32 [1024, 1024], P('tensor', 'dp')
- grad_w_1: float32 [1024, 4096], P('dp', 'tensor')
- grad_b_1: float32 [4096], P('tensor')
- grad_w_2: float32 [4096, 1024], P('tensor', 'dp')
The draws below stay inside these ranges and needn't reach their ends.
Inputs may be any that keep to these rules, and one draw needn't show every extreme that they name: `valid_mask`: each image has exactly 577 positions marked 1, the others 0.
All inputs are finite; a program needn't handle non-finite values.
Results may differ from the reference program's by a relative error of at most 0.017.
Values may be sent and summed in bfloat16 or wider, within the bound.
A program may use at most 128 MiB of HBM per device.

```python
import jax
import jax.numpy as jnp
from jax import lax

D = 1024
H = 16
HD = 64
FF = 4096
SEQ = 584
VALID = 577
IMG_DEV = 2
IMAGES = 16
N_DP = 8


def draw_inputs(key, part):
    shape = (SEQ, IMAGES, D)
    return jnp.clip(jax.random.normal(key, shape, jnp.float32), -6.0, 6.0).astype(jnp.bfloat16)


def draw_w_qkv(key, part):
    factor = D ** (-0.5)
    return (jnp.clip(jax.random.normal(key, (D, 3, D), jnp.float32), -6.0, 6.0) * factor).astype(jnp.bfloat16)


def draw_cotangent(key, part):
    shape = (SEQ, IMAGES, D)
    position = lax.broadcasted_iota(jnp.float32, shape, 0) / (SEQ - 1)
    image_rank = lax.broadcasted_iota(jnp.float32, shape, 1) / (IMAGES - 1)
    rising = jnp.exp(jnp.log(3.0) * (position + image_rank))
    return (jnp.clip(jax.random.normal(key, shape, jnp.float32), -6.0, 6.0) * rising).astype(jnp.bfloat16)


def draw_valid_mask(key, part):
    streams = jax.random.split(key, IMAGES)

    def one_image(stream):
        return (jax.random.permutation(stream, SEQ) < VALID).astype(jnp.int32)
    return jax.vmap(one_image)(streams)


def block_scale(key, extent, shards, smallest, top_value):
    level, own = 1.0, jax.random.fold_in(key, 6)
    for axis_at, parts in shards:
        steps = jnp.exp(jax.random.uniform(jax.random.fold_in(own, axis_at), (parts,), jnp.float32, smallest / len(shards), top_value / len(shards)))
        level = level * jnp.repeat(steps, extent[axis_at] // parts).reshape([-1 if axis == axis_at else 1 for axis in range(len(extent))])
    return level


def noise(key, dims, width, limit, cuts=(), held_as=jnp.bfloat16):
    drawn = width * jax.random.normal(key, dims, jnp.float32)
    if cuts:
        drawn = drawn * block_scale(key, dims, cuts, -0.22, 0.18)
    return jnp.clip(drawn, -limit, limit).astype(held_as)


def setup_inputs(seed: int = 0) -> dict:
    arg_keys = jax.random.split(jax.random.key(seed), 12)
    inputs = draw_inputs(jax.random.fold_in(arg_keys[11], 71), 0)
    valid_mask = draw_valid_mask(jax.random.fold_in(arg_keys[11], 71), 0)
    cotangent = draw_cotangent(jax.random.fold_in(arg_keys[11], 71), 0)
    ln_gain = jnp.clip(1.0 + 0.15 * jax.random.normal(arg_keys[3], (2, D), jnp.float32), 0.25, 1.75).astype(jnp.bfloat16)
    d_bias = noise(arg_keys[4], (4, D), 0.5, 3.0, ((1, 8),))
    w_qkv = draw_w_qkv(jax.random.fold_in(arg_keys[11], 71), 0)
    b_qv = noise(arg_keys[6], (2, D), 0.5, 3.0, ((1, 4),))
    w_o = noise(arg_keys[7], (D, D), (D * 4 // SEQ) ** -0.5, 2.0, ((0, 4), (1, 8)))
    w_1 = noise(arg_keys[8], (D, FF), D ** -0.5, 0.1875, ((0, 8), (1, 4)))
    b_1 = noise(arg_keys[9], (FF,), 0.5, 3.0, ((0, 4),))
    w_2 = noise(arg_keys[10], (FF, D), FF ** -0.5, 0.09375, ((0, 4), (1, 8)))
    return dict(inputs=inputs, valid_mask=valid_mask, cotangent=cotangent, ln_gain=ln_gain, d_bias=d_bias, w_qkv=w_qkv, b_qv=b_qv, w_o=w_o, w_1=w_1, b_1=b_1, w_2=w_2)


@jax.custom_vjp
def low(v):
    return lax.optimization_barrier(v.astype(jnp.bfloat16)).astype(jnp.float32)

@jax.custom_vjp
def low_back(v):
    return v

def low_keep(v):
    return (low(v), None)

def low_pass(kept, grad):
    return (grad,)

def back_keep(v):
    return (v, None)

def back_low(kept, grad):
    return (low(grad),)
low.defvjp(low_keep, low_pass)
low_back.defvjp(back_keep, back_low)
EPSILON = 1e-06
MASKED = -1e+30

def product(left, right):
    return jnp.dot(left, right, precision=lax.Precision.HIGHEST, preferred_element_type=jnp.float32)

def layer_norm(values, gain, shift):
    average = lax.optimization_barrier(jnp.mean(values, axis=-1, keepdims=True))
    centred = values - average
    variance = lax.optimization_barrier(jnp.mean(centred * centred, axis=-1, keepdims=True))
    return centred * lax.rsqrt(variance + EPSILON) * gain + shift

def attend_image(bundle):
    packed, valid = bundle
    queries = packed[:, 0]
    keys_part = packed[:, 1]
    values_part = packed[:, 2]
    scores = jnp.einsum('qhd,khd->hqk', queries, keys_part, precision=lax.Precision.HIGHEST)
    scores = low_back(scores * HD ** (-0.5))
    scores = jnp.where(valid[None, None, :] > 0, scores, MASKED)
    highest = lax.optimization_barrier(jnp.max(scores, axis=-1, keepdims=True))
    exponent = jnp.exp(scores - highest)
    attention = exponent / lax.optimization_barrier(jnp.sum(exponent, axis=-1, keepdims=True))
    return jnp.einsum('hqk,khd->qhd', low(attention), values_part, precision=lax.Precision.HIGHEST)

def layer(values, valid, ln_gain, d_bias, w_qkv, b_qv, w_o, w_1, b_1, w_2):
    number = values.shape[0]
    normed1 = low(layer_norm(values, ln_gain[0], d_bias[0]))
    projected = low_back(product(normed1, w_qkv.reshape(D, 3 * D))).reshape(number, SEQ, 3, D)
    qkv_bias = jnp.stack([b_qv[0], jnp.zeros_like(b_qv[0]), b_qv[1]])
    packed = low(projected + qkv_bias).reshape(number, SEQ, 3, H, HD)
    mixture = lax.map(jax.checkpoint(attend_image), (packed, valid))
    mixture = low_back(low(mixture.reshape(number, SEQ, D)))
    hidden1 = values + low_back(product(mixture, w_o)) + d_bias[2]
    normed2 = low(layer_norm(hidden1, ln_gain[1], d_bias[1]))
    hidden_in = low_back(product(normed2, w_1)) + b_1
    active = low(jax.nn.gelu(hidden_in, approximate=False))
    return hidden1 + low_back(product(active, w_2)) + d_bias[3]

def reference(inputs, valid_mask, cotangent, ln_gain, d_bias, w_qkv, b_qv, w_o, w_1, b_1, w_2):
    params = tuple((element.astype(jnp.float32) for element in (ln_gain, d_bias, w_qkv, b_qv, w_o, w_1, b_1, w_2)))

    def regroup(array):
        return jnp.transpose(array, (1, 0, 2)).reshape(N_DP, IMG_DEV, SEQ, D)
    groups = (regroup(inputs), valid_mask.reshape(N_DP, IMG_DEV, SEQ), regroup(cotangent))

    def one_group(running, group):
        block_inputs, block_valid, block_grad = group

        def forward(values, *weights):
            return layer(values, block_valid, *weights)
        output, pullback = jax.vjp(forward, block_inputs.astype(jnp.float32), *params)
        gradients = pullback(block_grad.astype(jnp.float32))
        running = tuple((previous + gradient for previous, gradient in zip(running, gradients[1:])))
        return (running, (output.astype(jnp.bfloat16), gradients[0]))
    initial = tuple((jnp.zeros_like(element) for element in params))
    running, (outputs, input_grads) = lax.scan(one_group, initial, groups)

    def ungroup(array):
        return jnp.transpose(array.reshape(IMAGES, SEQ, D), (1, 0, 2))
    return (ungroup(outputs), ungroup(input_grads), running[0], running[1], running[2], running[3], running[4], running[5], running[6], running[7])
```

```python
import jax
import jax.numpy as jnp
from jax import lax
from jax.sharding import PartitionSpec as P

HD = 64


EPSILON = 1e-06
MASKED = -1e30


def layer_norm(values, gain, shift):
    average = jnp.mean(values, axis=-1, keepdims=True)
    centred = values - average
    variance = jnp.mean(centred * centred, axis=-1, keepdims=True)
    return centred * lax.rsqrt(variance + EPSILON) * gain + shift


def gelu_exact(values):
    return jax.nn.gelu(values, approximate=False)


def gather_layer(ln_gain, d_bias, w_qkv, w_o, w_1, w_2):
    return (
        lax.all_gather(ln_gain, "dp", axis=1, tiled=True),
        lax.all_gather(d_bias, "dp", axis=1, tiled=True),
        lax.all_gather(w_qkv, "dp", axis=0, tiled=True),
        lax.all_gather(w_o, "dp", axis=1, tiled=True),
        lax.all_gather(w_1, "dp", axis=0, tiled=True),
        lax.all_gather(w_2, "dp", axis=1, tiled=True),
    )


def masked_scores(queries, keys_part, valid):
    scores = jnp.einsum(
        "qhd,khd->hqk", queries, keys_part, preferred_element_type=jnp.float32
    ) * HD ** (-0.5)
    return jnp.where(valid[None, None, :] > 0, scores, MASKED)


def attend_forward(bundle):
    packed, valid = bundle
    scores = masked_scores(packed[:, 0], packed[:, 1], valid)
    highest = jnp.max(scores, axis=-1, keepdims=True)
    exponent = jnp.exp(scores - highest)
    denominator = jnp.sum(exponent, axis=-1, keepdims=True)
    attention = (exponent / denominator).astype(jnp.bfloat16)
    mixture = jnp.einsum(
        "hqk,khd->qhd", attention, packed[:, 2], preferred_element_type=jnp.float32
    )
    return (mixture.astype(jnp.bfloat16), (highest + jnp.log(denominator))[..., 0])


def attend_backward(bundle):
    packed, grad_mixture, log_total, valid = bundle
    queries = packed[:, 0]
    keys_part = packed[:, 1]
    values_part = packed[:, 2]
    scores = masked_scores(queries, keys_part, valid)
    attention = jnp.exp(scores - log_total[..., None])
    attention_low = attention.astype(jnp.bfloat16)
    grad_values = jnp.einsum(
        "hqk,qhd->khd", attention_low, grad_mixture, preferred_element_type=jnp.float32
    )
    grad_attention = jnp.einsum(
        "qhd,khd->hqk", grad_mixture, values_part, preferred_element_type=jnp.float32
    )
    inner = jnp.sum(attention * grad_attention, axis=-1, keepdims=True)
    grad_scores = (attention * (grad_attention - inner)).astype(jnp.bfloat16)
    factor = HD ** (-0.5)
    grad_queries = (
        jnp.einsum("hqk,khd->qhd", grad_scores, keys_part, preferred_element_type=jnp.float32)
        * factor
    )
    grad_keys = (
        jnp.einsum("hqk,qhd->khd", grad_scores, queries, preferred_element_type=jnp.float32)
        * factor
    )
    return jnp.stack([grad_queries, grad_keys, grad_values], axis=1)


def body(inputs, valid_mask, cotangent, ln_gain, d_bias, w_qkv, b_qv, w_o, w_1, b_1, w_2):
    local_rows, images, model_width = inputs.shape
    layer = gather_layer(ln_gain, d_bias, w_qkv, w_o, w_1, w_2)
    gains = layer[0].astype(jnp.float32)
    shifts = layer[1].astype(jnp.float32)
    wide_qkv = layer[2].reshape(model_width, -1)
    wide_out = layer[3]
    wide_up = layer[4]
    wide_down = layer[5]
    residual = inputs.astype(jnp.float32)
    normed1 = layer_norm(residual, gains[0], shifts[0]).astype(jnp.bfloat16)
    gathered1 = lax.all_gather(normed1, "tensor", axis=0, tiled=True)
    full_length = gathered1.shape[0]
    columns = b_qv.shape[1]
    heads_local = columns // HD
    projected = jnp.dot(gathered1, wide_qkv, preferred_element_type=jnp.float32).reshape(
        full_length, images, 3, columns
    )
    qkv_bias = jnp.stack([b_qv[0], jnp.zeros_like(b_qv[0]), b_qv[1]]).astype(jnp.float32)
    projected_low = (projected + qkv_bias).astype(jnp.bfloat16)
    per_image = jnp.transpose(projected_low, (1, 0, 2, 3)).reshape(
        images, full_length, 3, heads_local, HD
    )
    mixture, log_total = lax.map(attend_forward, (per_image, valid_mask))
    mixture_seq = jnp.transpose(mixture, (1, 0, 2, 3)).reshape(full_length, images, columns)
    segment = mixture_seq
    attn_sum = lax.psum_scatter(
        jnp.dot(segment, wide_out, preferred_element_type=jnp.float32),
        "tensor",
        scatter_dimension=0,
        tiled=True,
    )
    hidden1 = residual + attn_sum + shifts[2]
    normed2 = layer_norm(hidden1, gains[1], shifts[1]).astype(jnp.bfloat16)
    gathered2 = lax.all_gather(normed2, "tensor", axis=0, tiled=True)
    hidden_in = jnp.dot(gathered2, wide_up, preferred_element_type=jnp.float32) + b_1.astype(
        jnp.float32
    )
    active = gelu_exact(hidden_in).astype(jnp.bfloat16)
    segment = active
    branch_sum = lax.psum_scatter(
        jnp.dot(segment, wide_down, preferred_element_type=jnp.float32).astype(jnp.bfloat16),
        "tensor",
        scatter_dimension=0,
        tiled=True,
    ).astype(jnp.float32)
    block_output = (hidden1 + branch_sum + shifts[3]).astype(jnp.bfloat16)
    layer = gather_layer(ln_gain, d_bias, w_qkv, w_o, w_1, w_2)
    wide_qkv = layer[2].reshape(model_width, -1)
    wide_out = layer[3]
    wide_up = layer[4]
    wide_down = layer[5]
    grad_out = cotangent.astype(jnp.float32)
    grad_gathered = lax.all_gather(cotangent, "tensor", axis=0, tiled=True)
    grad_w_2 = jnp.einsum("sif,sid->fd", active, grad_gathered, preferred_element_type=jnp.float32)
    grad_active = jnp.einsum(
        "sid,fd->sif", grad_gathered, wide_down, preferred_element_type=jnp.float32
    )
    grad_hidden_in = jax.vjp(gelu_exact, hidden_in)[1](grad_active)[0]
    grad_b_1 = jnp.sum(grad_hidden_in, axis=(0, 1))
    grad_hidden_low = grad_hidden_in.astype(jnp.bfloat16)
    grad_w_1 = jnp.einsum(
        "sid,sif->df", gathered2, grad_hidden_low, preferred_element_type=jnp.float32
    )
    segment = grad_hidden_low
    grad_normed2 = lax.psum_scatter(
        jnp.einsum("sif,df->sid", segment, wide_up, preferred_element_type=jnp.float32),
        "tensor",
        scatter_dimension=0,
        tiled=True,
    )
    second_pull = jax.vjp(layer_norm, hidden1, gains[1], shifts[1])[1]
    grad_from_norm, gain2_grad, shift2_grad = second_pull(grad_normed2)
    grad_hidden1 = grad_out + grad_from_norm
    grad_attn_low = grad_hidden1.astype(jnp.bfloat16)
    grad_attn_all = lax.all_gather(grad_attn_low, "tensor", axis=0, tiled=True)
    grad_w_o = jnp.einsum(
        "sic,sid->cd", mixture_seq, grad_attn_all, preferred_element_type=jnp.float32
    )
    grad_mixture = jnp.einsum(
        "sid,cd->sic", grad_attn_all, wide_out, preferred_element_type=jnp.float32
    ).astype(jnp.bfloat16)
    grad_mixture_img = jnp.transpose(
        grad_mixture.reshape(full_length, images, heads_local, HD), (1, 0, 2, 3)
    )
    grad_packed = lax.map(attend_backward, (per_image, grad_mixture_img, log_total, valid_mask))
    grad_projected = jnp.transpose(grad_packed, (1, 0, 2, 3, 4)).reshape(
        full_length, images, 3, columns
    )
    grad_b_qv = jnp.stack(
        [
            jnp.sum(grad_projected[:, :, 0], axis=(0, 1)),
            jnp.sum(grad_projected[:, :, 2], axis=(0, 1)),
        ]
    )
    grad_projected_low = grad_projected.reshape(full_length, images, 3 * columns).astype(
        jnp.bfloat16
    )
    grad_w_qkv = jnp.einsum(
        "sid,sic->dc", gathered1, grad_projected_low, preferred_element_type=jnp.float32
    ).reshape(model_width, 3, columns)
    segment = grad_projected_low
    grad_normed1 = lax.psum_scatter(
        jnp.einsum("sic,dc->sid", segment, wide_qkv, preferred_element_type=jnp.float32).astype(
            jnp.bfloat16
        ),
        "tensor",
        scatter_dimension=0,
        tiled=True,
    ).astype(jnp.float32)
    first_pull = jax.vjp(layer_norm, residual, gains[0], shifts[0])[1]
    grad_from_front, gain1_grad, shift1_grad = first_pull(grad_normed1)
    grad_inputs = grad_hidden1 + grad_from_front
    gain_terms = jnp.stack([gain1_grad, gain2_grad])
    shift_terms = jnp.stack(
        [
            shift1_grad,
            shift2_grad,
            jnp.sum(grad_hidden1, axis=(0, 1)),
            jnp.sum(grad_out, axis=(0, 1)),
        ]
    )
    scattered = (
        lax.psum_scatter(
            gain_terms.astype(jnp.bfloat16), "dp", scatter_dimension=1, tiled=True
        ).astype(jnp.float32),
        lax.psum_scatter(
            shift_terms.astype(jnp.bfloat16), "dp", scatter_dimension=1, tiled=True
        ).astype(jnp.float32),
        lax.psum_scatter(
            grad_w_qkv.astype(jnp.bfloat16), "dp", scatter_dimension=0, tiled=True
        ).astype(jnp.float32),
        lax.psum_scatter(
            grad_w_o.astype(jnp.bfloat16), "dp", scatter_dimension=1, tiled=True
        ).astype(jnp.float32),
        lax.psum_scatter(
            grad_w_1.astype(jnp.bfloat16), "dp", scatter_dimension=0, tiled=True
        ).astype(jnp.float32),
        lax.psum_scatter(
            grad_w_2.astype(jnp.bfloat16), "dp", scatter_dimension=1, tiled=True
        ).astype(jnp.float32),
    )
    gain_sum, shift_sum = lax.psum((scattered[0], scattered[1]), "tensor")
    bias_qv_sum, bias_up_sum = lax.psum((grad_b_qv, grad_b_1), "dp")
    return (
        block_output,
        grad_inputs,
        gain_sum,
        shift_sum,
        scattered[2],
        bias_qv_sum,
        scattered[3],
        scattered[4],
        bias_up_sum,
        scattered[5],
    )


Q = 152


def bits():
    d = lax.axis_index("dp")
    return d // 4, (d // 2) % 2, d % 2, lax.axis_index("tensor")


def table(f):
    pairs = []
    for y in range(2):
        for x in range(2):
            for c in range(2):
                for z in range(4):
                    ty, tx, tc, tz = f(y, x, c, z)
                    pairs.append((((y * 2 + x) * 2 + c) * 4 + z, ((ty * 2 + tx) * 2 + tc) * 4 + tz))
    return pairs


def flip(pairs):
    return [(b, a) for a, b in pairs]


TO_C = table(lambda y, x, c, z: (y, x, 1 - c, z))
TO_X = table(lambda y, x, c, z: (y, 1 - x, c, z))
TO_Y = table(lambda y, x, c, z: (1 - y, x, c, z))
TO_XC = table(lambda y, x, c, z: (y, 1 - x, 1 - c, z))
TO_Z = table(lambda y, x, c, z: (y, x, c, (z + 3) % 4))
SWAP_0 = table(lambda y, x, c, z: (y, x, z // 2, 2 * c + z % 2))
SWAP_1 = table(lambda y, x, c, z: (y, x, z // 2, 2 * c + 1 - z % 2))


def send(value, pairs):
    return lax.ppermute(value, ("dp", "tensor"), pairs)


def pick(bit, first, second):
    return jnp.where(bit == 0, first, second), jnp.where(bit == 0, second, first)


def order4(hi, lo, own, other_lo, other_hi, other_both):
    a0, a1 = pick(lo, own, other_lo)
    b0, b1 = pick(lo, other_hi, other_both)
    first = pick(hi, a0, b0)
    second = pick(hi, a1, b1)
    return first[0], second[0], first[1], second[1]


def ring_gather(piece):
    pieces = [piece]
    for _ in range(3):
        pieces.append(send(pieces[-1], TO_Z))
    return pieces


def ring_scatter(terms):
    total = terms[1]
    for at in (2, 3, 0):
        total = send(total.astype(jnp.bfloat16), TO_Z).astype(jnp.float32) + terms[at]
    return total


def scatter4(blocks, y, x, c):
    kept = send(blocks(1 - x, c), TO_X), send(blocks(x, 1 - c), TO_C), send(blocks(1 - x, 1 - c), TO_XC)
    return order4(x, c, blocks(x, c), kept[1], kept[0], kept[2])


def tokens_in(values, z):
    rows = values.shape[0]
    turned = jnp.pad(jnp.transpose(values, (1, 0, 2)), ((0, 0), (0, Q - rows), (0, 0)))
    first, second = pick(z % 2, turned[0], turned[1])
    return jnp.concatenate([send(first, SWAP_0), send(second, SWAP_1)])


def tokens_out(values, z, rows):
    first = send(values[:Q], flip(SWAP_0))
    second = send(values[Q:], flip(SWAP_1))
    images = pick(z % 2, first, second)
    return jnp.stack([images[0][:rows], images[1][:rows]], axis=1)


def norm_parts(values):
    average = jnp.mean(values, axis=-1, keepdims=True)
    centred = values - average
    variance = jnp.mean(centred * centred, axis=-1, keepdims=True)
    scale = lax.rsqrt(variance + EPSILON)
    return centred * scale, scale


def norm_back(grad, unit, scale, gain):
    q = grad * gain
    return scale * (
        q - jnp.mean(q, axis=-1, keepdims=True) - unit * jnp.mean(q * unit, axis=-1, keepdims=True)
    )


def dot32(left, right, dims):
    return lax.dot_general(left, right, (dims, ((), ())), preferred_element_type=jnp.float32)


NN = ((1,), (0,))
NT = ((1,), (1,))
TN = ((0,), (0,))


def fast_body(inputs, valid_mask, cotangent, ln_gain, d_bias, w_qkv, b_qv, w_o, w_1, b_1, w_2):
    y, x, c, z = bits()
    r = y * 2 + x
    rows = inputs.shape[0]
    bf, f32 = jnp.bfloat16, jnp.float32

    tokens = tokens_in(inputs, z)
    mine_all = jnp.where(c == z // 2, valid_mask, send(valid_mask, TO_C))
    mine = jnp.where(z % 2 == 0, mine_all[0], mine_all[1]).reshape(4, rows)
    mine = jnp.pad(mine, ((0, 0), (0, Q - rows)))
    even = jnp.stack(pick(z % 2, mine[0], mine[1]))
    odd = jnp.stack(pick(z % 2, mine[2], mine[3]))
    valid = jnp.concatenate(pick(c, even, odd)).reshape(4 * Q)

    halves = w_qkv.reshape(128, 3, 2, 128)
    packs = [
        jnp.concatenate([halves[:, :, at].reshape(128, 384), w_o[at * 128 : at * 128 + 128]], axis=1)
        for at in range(2)
    ]
    keep, give = pick(c, packs[0], packs[1])
    chip_pack = jnp.concatenate(pick(c, keep, send(give, TO_C)))

    small = jnp.concatenate([ln_gain, d_bias])
    small = jnp.stack(pick(c, small, send(small, TO_C)))
    small = jnp.stack(pick(x, small, send(small, TO_X)))
    small = jnp.stack(pick(y, small, send(small, TO_Y)))
    small = jnp.transpose(small, (3, 0, 1, 2, 4)).reshape(6, 1024).astype(f32)
    gains, shifts = small[:2], small[2:]

    q_part = 2 * x + c
    bias = jnp.concatenate(
        [
            lax.dynamic_slice(b_qv, (0, c * 128), (2, 128)).reshape(256),
            lax.dynamic_slice(b_1, (q_part * 256,), (256,)),
        ]
    )
    bias = jnp.stack(ring_gather(bias)).astype(f32)
    bias_q = bias[:, :128].reshape(512)
    bias_v = bias[:, 128:256].reshape(512)
    bias_up = bias[:, 256:].reshape(1024)

    attn_pieces = []
    for at, piece in enumerate(ring_gather(chip_pack)):
        if at % 2 == 0:
            by_x = send(piece, TO_X)
            attn_pieces.append(order4(y, x, piece, by_x, send(piece, TO_Y), send(by_x, TO_Y)))
        else:
            by_y = send(piece, TO_Y)
            attn_pieces.append(order4(y, x, piece, send(piece, TO_X), by_y, send(by_y, TO_X)))
    wide_qkv = jnp.stack(
        [jnp.concatenate([piece[:, :384] for piece in four]).reshape(1024, 3, 128) for four in attn_pieces], axis=2
    ).reshape(1024, 1536)
    wide_out = jnp.concatenate(
        [
            jnp.concatenate([piece[at * 128 : at * 128 + 128, 384:] for piece in four for at in range(2)], axis=1)
            for four in attn_pieces
        ]
    )

    up_blocks = lambda bx, bc: lax.dynamic_slice(w_1, (0, (2 * bx + bc) * 256), (128, 256))
    up_piece = jnp.concatenate(scatter4(up_blocks, y, x, c))
    up_pieces = ring_gather(up_piece)
    wide_up = jnp.concatenate(
        [jnp.concatenate(pick(y, piece, send(piece, TO_Y))) for piece in up_pieces], axis=1
    )
    down_blocks = lambda bx, bc: lax.dynamic_slice(w_2, ((2 * bx + bc) * 256, 0), (256, 128))
    down_piece = jnp.concatenate(scatter4(down_blocks, y, x, c), axis=1)
    down_pieces = ring_gather(down_piece)
    wide_down = jnp.concatenate(
        [jnp.concatenate(pick(y, piece, send(piece, TO_Y)), axis=1) for piece in down_pieces]
    )

    grad_out_low = tokens_in(cotangent, z)
    grad_out = grad_out_low.astype(f32)

    residual = tokens.astype(f32)
    unit1, scale1 = norm_parts(residual)
    normed1_own = (unit1 * gains[0] + shifts[0]).astype(bf)
    normed1 = jnp.concatenate([normed1_own, send(normed1_own, TO_C)])
    count = normed1.shape[0]
    qkv_bias = jnp.concatenate([bias_q, jnp.zeros_like(bias_q), bias_v])
    projected = (dot32(normed1, wide_qkv, NN) + qkv_bias).astype(bf)
    per_head = projected.reshape(count, 3, 8, HD)
    queries, keys_part, values_part = per_head[:, 0], per_head[:, 1], per_head[:, 2]
    factor = HD ** (-0.5)
    scores = jnp.einsum("qhd,khd->hqk", queries, keys_part, preferred_element_type=f32) * factor
    scores = jnp.where(valid[None, None, :] > 0, scores, MASKED)
    highest = jnp.max(scores, axis=-1, keepdims=True)
    exponent = jnp.exp(scores - highest)
    denominator = jnp.sum(exponent, axis=-1, keepdims=True)
    attention_low = (exponent / denominator).astype(bf)
    log_total = highest + jnp.log(denominator)
    mixture = jnp.einsum("hqk,khd->qhd", attention_low, values_part, preferred_element_type=f32)
    mixture = mixture.astype(bf).reshape(count, 512)
    half = count // 2
    attn_part = dot32(mixture, wide_out, NN)
    hidden1 = residual + attn_part[:half] + send(attn_part[half:], TO_C) + shifts[2]
    unit2, scale2 = norm_parts(hidden1)
    normed2_own = (unit2 * gains[1] + shifts[1]).astype(bf)

    def spread(own):
        by_x = send(own, TO_X)
        return jnp.concatenate([own, send(own, TO_C), by_x, send(by_x, TO_C)])

    def collect(part):
        a, b, at_x, at_xc = (part[at * half : at * half + half] for at in range(4))
        far = at_x + send(at_xc.astype(bf), TO_C).astype(f32)
        near = a + send(b.astype(bf), TO_C).astype(f32)
        return near + send(far.astype(bf), TO_X).astype(f32)

    normed2 = spread(normed2_own)
    grad_all = spread(grad_out_low)
    hidden_in = dot32(normed2, wide_up, NN) + bias_up
    active = gelu_exact(hidden_in).astype(bf)
    branch = collect(dot32(active, wide_down, NN))
    block_output = tokens_out((hidden1 + branch + shifts[3]).astype(bf), z, rows)

    grad_w_2 = dot32(active, grad_all, TN)
    grad_active = dot32(grad_all, wide_down, NT)
    grad_hidden_in = jax.vjp(gelu_exact, hidden_in)[1](grad_active)[0]
    grad_b_1 = jnp.sum(grad_hidden_in, axis=0)
    grad_hidden_low = grad_hidden_in.astype(bf)
    grad_w_1 = dot32(normed2, grad_hidden_low, TN)
    grad_normed2 = collect(dot32(grad_hidden_low, wide_up, NT))
    grad_hidden1 = grad_out + norm_back(grad_normed2, unit2, scale2, gains[1])
    grad_attn_own = grad_hidden1.astype(bf)
    grad_attn = jnp.concatenate([grad_attn_own, send(grad_attn_own, TO_C)])
    grad_w_o = dot32(mixture, grad_attn, TN)
    grad_mixture = dot32(grad_attn, wide_out, NT).astype(bf).reshape(count, 8, HD)

    attention = jnp.exp(scores - log_total)
    grad_values = jnp.einsum("hqk,qhd->khd", attention_low, grad_mixture, preferred_element_type=f32)
    grad_attention = jnp.einsum("qhd,khd->hqk", grad_mixture, values_part, preferred_element_type=f32)
    inner = jnp.sum(attention * grad_attention, axis=-1, keepdims=True)
    grad_scores = (attention * (grad_attention - inner)).astype(bf)
    grad_queries = jnp.einsum("hqk,khd->qhd", grad_scores, keys_part, preferred_element_type=f32) * factor
    grad_keys = jnp.einsum("hqk,qhd->khd", grad_scores, queries, preferred_element_type=f32) * factor
    grad_projected = jnp.stack([grad_queries, grad_keys, grad_values], axis=1).reshape(count, 3, 512)
    grad_b_qv = jnp.sum(grad_projected, axis=0)
    grad_projected_low = grad_projected.astype(bf).reshape(count, 1536)
    grad_w_qkv = dot32(normed1, grad_projected_low, TN)
    part = dot32(grad_projected_low, wide_qkv, NT)
    grad_normed1 = part[:half] + send(part[half:], TO_C)
    grad_inputs = grad_hidden1 + norm_back(grad_normed1, unit1, scale1, gains[0])
    grad_inputs = tokens_out(grad_inputs.astype(bf), z, rows).astype(f32)

    cut = lambda array, at, size, axis: lax.dynamic_slice_in_dim(array, at * size, size, axis)
    terms = []
    for at in range(4):
        block = grad_w_1[:, at * 256 : at * 256 + 256]
        far = send(cut(block, 1 - y, 512, 0).astype(bf), TO_Y).astype(f32)
        terms.append(cut(block, y, 512, 0) + far)
    total = ring_scatter(terms).astype(bf)
    out_w_1 = jnp.concatenate(
        scatter4(lambda bx, bc: cut(total, 2 * bx + bc, 128, 0), y, x, c), axis=1
    ).astype(f32)
    terms = []
    for at in range(4):
        block = grad_w_2[at * 256 : at * 256 + 256]
        far = send(cut(block, 1 - y, 512, 1).astype(bf), TO_Y).astype(f32)
        terms.append(cut(block, y, 512, 1) + far)
    total2 = ring_scatter(terms).astype(bf)
    out_w_2 = jnp.concatenate(
        scatter4(lambda bx, bc: cut(total2, 2 * bx + bc, 128, 1), y, x, c), axis=0
    ).astype(f32)

    terms = []
    by_head = grad_w_qkv.reshape(1024, 3, 4, 128)
    for at in range(4):

        def block(rel):
            rr = r ^ rel
            left = cut(by_head[:, :, at].reshape(1024, 384), rr, 256, 0)
            right = cut(grad_w_o[at * 128 : at * 128 + 128], rr, 256, 1)
            right = jnp.concatenate([right[:, :128], right[:, 128:]])
            return jnp.concatenate([left, right], axis=1)

        near, far, first, second = (1, 2, TO_X, TO_Y) if at % 2 == 0 else (2, 1, TO_Y, TO_X)
        mid = block(far) + send(block(3).astype(bf), first).astype(f32)
        own = block(0) + send(block(near).astype(bf), first).astype(f32)
        terms.append(own + send(mid.astype(bf), second).astype(f32))
    total3 = ring_scatter(terms).astype(bf)
    keep, give = cut(total3, c, 128, 0), cut(total3, 1 - c, 128, 0)
    both = pick(c, keep, send(give, TO_C))
    out_w_qkv = jnp.stack([half_[:, :384].reshape(128, 3, 128) for half_ in both], axis=2).reshape(128, 3, 256).astype(f32)
    out_w_o = jnp.concatenate([half_[:, 384:] for half_ in both]).astype(f32)

    width = 6 * 1024
    sums = jnp.stack(
        [
            jnp.sum(grad_normed1 * unit1, axis=0),
            jnp.sum(grad_normed2 * unit2, axis=0),
            jnp.sum(grad_normed1, axis=0),
            jnp.sum(grad_normed2, axis=0),
            jnp.sum(grad_hidden1, axis=0),
            jnp.sum(grad_out, axis=0),
        ]
    )
    sums = lax.psum(sums, ("dp", "tensor"))
    own_sums = lax.dynamic_slice(sums, (0, lax.axis_index("dp") * 128), (6, 128))

    place_qv = jnp.zeros((2, 4, 2, 128), f32)
    qv = jnp.stack([grad_b_qv[0], grad_b_qv[2]]).reshape(2, 4, 128)
    place_qv = jnp.where((jnp.arange(2) == c)[None, None, :, None], qv[:, :, None, :], 0.0)
    place_up = jnp.where((jnp.arange(4) == q_part)[None, :, None], grad_b_1.reshape(4, 1, 256), 0.0)
    packed = jnp.concatenate([jnp.transpose(place_qv, (1, 0, 2, 3)).reshape(4, 512), place_up.reshape(4, 1024)], axis=1)
    turn = jnp.stack([lax.dynamic_index_in_dim(packed, (at - z) % 4, 0, keepdims=False) for at in range(4)])
    turn = lax.psum(turn, ("dp", "tensor"))
    mine_b = lax.dynamic_index_in_dim(turn, z, 0, keepdims=False)
    return (
        block_output,
        grad_inputs,
        own_sums[:2],
        own_sums[2:],
        out_w_qkv,
        mine_b[:512].reshape(2, 256),
        out_w_o,
        out_w_1,
        mine_b[512:],
        out_w_2,
    )


def solution(mesh):
    in_specs = (
        P("tensor", "dp", None),
        P("dp", None),
        P("tensor", "dp", None),
        P(None, "dp"),
        P(None, "dp"),
        P("dp", None, "tensor"),
        P(None, "tensor"),
        P("tensor", "dp"),
        P("dp", "tensor"),
        P("tensor"),
        P("tensor", "dp"),
    )
    out_specs = (
        P("tensor", "dp", None),
        P("tensor", "dp", None),
        P(None, "dp"),
        P(None, "dp"),
        P("dp", None, "tensor"),
        P(None, "tensor"),
        P("tensor", "dp"),
        P("dp", "tensor"),
        P("tensor"),
        P("tensor", "dp"),
    )
    run = fast_body if dict(mesh.shape) == {"dp": 8, "tensor": 4} else body
    return jax.shard_map(run, mesh=mesh, in_specs=in_specs, out_specs=out_specs, check_vma=False)
```

```python
import functools

import jax
import jax.numpy as jnp
from jax import lax
from jax.experimental import pallas as pl
from jax.experimental.pallas import tpu as pltpu
from jax.sharding import PartitionSpec as P

HD = 64


EPSILON = 1e-06
MASKED = -1e30


def layer_norm(values, gain, shift):
    average = jnp.mean(values, axis=-1, keepdims=True)
    centred = values - average
    variance = jnp.mean(centred * centred, axis=-1, keepdims=True)
    return centred * lax.rsqrt(variance + EPSILON) * gain + shift


def gelu_exact(values):
    return jax.nn.gelu(values, approximate=False)


def gather_layer(ln_gain, d_bias, w_qkv, w_o, w_1, w_2):
    return (
        lax.all_gather(ln_gain, "dp", axis=1, tiled=True),
        lax.all_gather(d_bias, "dp", axis=1, tiled=True),
        lax.all_gather(w_qkv, "dp", axis=0, tiled=True),
        lax.all_gather(w_o, "dp", axis=1, tiled=True),
        lax.all_gather(w_1, "dp", axis=0, tiled=True),
        lax.all_gather(w_2, "dp", axis=1, tiled=True),
    )


def masked_scores(queries, keys_part, valid):
    scores = jnp.einsum(
        "qhd,khd->hqk", queries, keys_part, preferred_element_type=jnp.float32
    ) * HD ** (-0.5)
    return jnp.where(valid[None, None, :] > 0, scores, MASKED)


def attend_forward(bundle):
    packed, valid = bundle
    scores = masked_scores(packed[:, 0], packed[:, 1], valid)
    highest = jnp.max(scores, axis=-1, keepdims=True)
    exponent = jnp.exp(scores - highest)
    denominator = jnp.sum(exponent, axis=-1, keepdims=True)
    attention = (exponent / denominator).astype(jnp.bfloat16)
    mixture = jnp.einsum(
        "hqk,khd->qhd", attention, packed[:, 2], preferred_element_type=jnp.float32
    )
    return (mixture.astype(jnp.bfloat16), (highest + jnp.log(denominator))[..., 0])


def attend_backward(bundle):
    packed, grad_mixture, log_total, valid = bundle
    queries = packed[:, 0]
    keys_part = packed[:, 1]
    values_part = packed[:, 2]
    scores = masked_scores(queries, keys_part, valid)
    attention = jnp.exp(scores - log_total[..., None])
    attention_low = attention.astype(jnp.bfloat16)
    grad_values = jnp.einsum(
        "hqk,qhd->khd", attention_low, grad_mixture, preferred_element_type=jnp.float32
    )
    grad_attention = jnp.einsum(
        "qhd,khd->hqk", grad_mixture, values_part, preferred_element_type=jnp.float32
    )
    inner = jnp.sum(attention * grad_attention, axis=-1, keepdims=True)
    grad_scores = (attention * (grad_attention - inner)).astype(jnp.bfloat16)
    factor = HD ** (-0.5)
    grad_queries = (
        jnp.einsum("hqk,khd->qhd", grad_scores, keys_part, preferred_element_type=jnp.float32)
        * factor
    )
    grad_keys = (
        jnp.einsum("hqk,qhd->khd", grad_scores, queries, preferred_element_type=jnp.float32)
        * factor
    )
    return jnp.stack([grad_queries, grad_keys, grad_values], axis=1)


def body(inputs, valid_mask, cotangent, ln_gain, d_bias, w_qkv, b_qv, w_o, w_1, b_1, w_2):
    local_rows, images, model_width = inputs.shape
    layer = gather_layer(ln_gain, d_bias, w_qkv, w_o, w_1, w_2)
    gains = layer[0].astype(jnp.float32)
    shifts = layer[1].astype(jnp.float32)
    wide_qkv = layer[2].reshape(model_width, -1)
    wide_out = layer[3]
    wide_up = layer[4]
    wide_down = layer[5]
    residual = inputs.astype(jnp.float32)
    normed1 = layer_norm(residual, gains[0], shifts[0]).astype(jnp.bfloat16)
    gathered1 = lax.all_gather(normed1, "tensor", axis=0, tiled=True)
    full_length = gathered1.shape[0]
    columns = b_qv.shape[1]
    heads_local = columns // HD
    projected = jnp.dot(gathered1, wide_qkv, preferred_element_type=jnp.float32).reshape(
        full_length, images, 3, columns
    )
    qkv_bias = jnp.stack([b_qv[0], jnp.zeros_like(b_qv[0]), b_qv[1]]).astype(jnp.float32)
    projected_low = (projected + qkv_bias).astype(jnp.bfloat16)
    per_image = jnp.transpose(projected_low, (1, 0, 2, 3)).reshape(
        images, full_length, 3, heads_local, HD
    )
    mixture, log_total = lax.map(attend_forward, (per_image, valid_mask))
    mixture_seq = jnp.transpose(mixture, (1, 0, 2, 3)).reshape(full_length, images, columns)
    segment = mixture_seq
    attn_sum = lax.psum_scatter(
        jnp.dot(segment, wide_out, preferred_element_type=jnp.float32),
        "tensor",
        scatter_dimension=0,
        tiled=True,
    )
    hidden1 = residual + attn_sum + shifts[2]
    normed2 = layer_norm(hidden1, gains[1], shifts[1]).astype(jnp.bfloat16)
    gathered2 = lax.all_gather(normed2, "tensor", axis=0, tiled=True)
    hidden_in = jnp.dot(gathered2, wide_up, preferred_element_type=jnp.float32) + b_1.astype(
        jnp.float32
    )
    active = gelu_exact(hidden_in).astype(jnp.bfloat16)
    segment = active
    branch_sum = lax.psum_scatter(
        jnp.dot(segment, wide_down, preferred_element_type=jnp.float32).astype(jnp.bfloat16),
        "tensor",
        scatter_dimension=0,
        tiled=True,
    ).astype(jnp.float32)
    block_output = (hidden1 + branch_sum + shifts[3]).astype(jnp.bfloat16)
    layer = gather_layer(ln_gain, d_bias, w_qkv, w_o, w_1, w_2)
    wide_qkv = layer[2].reshape(model_width, -1)
    wide_out = layer[3]
    wide_up = layer[4]
    wide_down = layer[5]
    grad_out = cotangent.astype(jnp.float32)
    grad_gathered = lax.all_gather(cotangent, "tensor", axis=0, tiled=True)
    grad_w_2 = jnp.einsum("sif,sid->fd", active, grad_gathered, preferred_element_type=jnp.float32)
    grad_active = jnp.einsum(
        "sid,fd->sif", grad_gathered, wide_down, preferred_element_type=jnp.float32
    )
    grad_hidden_in = jax.vjp(gelu_exact, hidden_in)[1](grad_active)[0]
    grad_b_1 = jnp.sum(grad_hidden_in, axis=(0, 1))
    grad_hidden_low = grad_hidden_in.astype(jnp.bfloat16)
    grad_w_1 = jnp.einsum(
        "sid,sif->df", gathered2, grad_hidden_low, preferred_element_type=jnp.float32
    )
    segment = grad_hidden_low
    grad_normed2 = lax.psum_scatter(
        jnp.einsum("sif,df->sid", segment, wide_up, preferred_element_type=jnp.float32),
        "tensor",
        scatter_dimension=0,
        tiled=True,
    )
    second_pull = jax.vjp(layer_norm, hidden1, gains[1], shifts[1])[1]
    grad_from_norm, gain2_grad, shift2_grad = second_pull(grad_normed2)
    grad_hidden1 = grad_out + grad_from_norm
    grad_attn_low = grad_hidden1.astype(jnp.bfloat16)
    grad_attn_all = lax.all_gather(grad_attn_low, "tensor", axis=0, tiled=True)
    grad_w_o = jnp.einsum(
        "sic,sid->cd", mixture_seq, grad_attn_all, preferred_element_type=jnp.float32
    )
    grad_mixture = jnp.einsum(
        "sid,cd->sic", grad_attn_all, wide_out, preferred_element_type=jnp.float32
    ).astype(jnp.bfloat16)
    grad_mixture_img = jnp.transpose(
        grad_mixture.reshape(full_length, images, heads_local, HD), (1, 0, 2, 3)
    )
    grad_packed = lax.map(attend_backward, (per_image, grad_mixture_img, log_total, valid_mask))
    grad_projected = jnp.transpose(grad_packed, (1, 0, 2, 3, 4)).reshape(
        full_length, images, 3, columns
    )
    grad_b_qv = jnp.stack(
        [
            jnp.sum(grad_projected[:, :, 0], axis=(0, 1)),
            jnp.sum(grad_projected[:, :, 2], axis=(0, 1)),
        ]
    )
    grad_projected_low = grad_projected.reshape(full_length, images, 3 * columns).astype(
        jnp.bfloat16
    )
    grad_w_qkv = jnp.einsum(
        "sid,sic->dc", gathered1, grad_projected_low, preferred_element_type=jnp.float32
    ).reshape(model_width, 3, columns)
    segment = grad_projected_low
    grad_normed1 = lax.psum_scatter(
        jnp.einsum("sic,dc->sid", segment, wide_qkv, preferred_element_type=jnp.float32).astype(
            jnp.bfloat16
        ),
        "tensor",
        scatter_dimension=0,
        tiled=True,
    ).astype(jnp.float32)
    first_pull = jax.vjp(layer_norm, residual, gains[0], shifts[0])[1]
    grad_from_front, gain1_grad, shift1_grad = first_pull(grad_normed1)
    grad_inputs = grad_hidden1 + grad_from_front
    gain_terms = jnp.stack([gain1_grad, gain2_grad])
    shift_terms = jnp.stack(
        [
            shift1_grad,
            shift2_grad,
            jnp.sum(grad_hidden1, axis=(0, 1)),
            jnp.sum(grad_out, axis=(0, 1)),
        ]
    )
    scattered = (
        lax.psum_scatter(
            gain_terms.astype(jnp.bfloat16), "dp", scatter_dimension=1, tiled=True
        ).astype(jnp.float32),
        lax.psum_scatter(
            shift_terms.astype(jnp.bfloat16), "dp", scatter_dimension=1, tiled=True
        ).astype(jnp.float32),
        lax.psum_scatter(
            grad_w_qkv.astype(jnp.bfloat16), "dp", scatter_dimension=0, tiled=True
        ).astype(jnp.float32),
        lax.psum_scatter(
            grad_w_o.astype(jnp.bfloat16), "dp", scatter_dimension=1, tiled=True
        ).astype(jnp.float32),
        lax.psum_scatter(
            grad_w_1.astype(jnp.bfloat16), "dp", scatter_dimension=0, tiled=True
        ).astype(jnp.float32),
        lax.psum_scatter(
            grad_w_2.astype(jnp.bfloat16), "dp", scatter_dimension=1, tiled=True
        ).astype(jnp.float32),
    )
    gain_sum, shift_sum = lax.psum((scattered[0], scattered[1]), "tensor")
    bias_qv_sum, bias_up_sum = lax.psum((grad_b_qv, grad_b_1), "dp")
    return (
        block_output,
        grad_inputs,
        gain_sum,
        shift_sum,
        scattered[2],
        bias_qv_sum,
        scattered[3],
        scattered[4],
        bias_up_sum,
        scattered[5],
    )


Q = 160
HALF = 2 * Q
FULL = 4 * Q
BF, F32 = jnp.bfloat16, jnp.float32
MESH = pl.DeviceIdType.MESH


def place(y, x, c, z):
    return (y * 4 + x * 2 + c, z)


def at_rows(start, size, step=8):
    return pl.ds(pl.multiple_of(start, step), size)


def mm(left, right, dims):
    return lax.dot_general(left, right, (dims, ((), ())), preferred_element_type=F32)


NN = ((1,), (0,))
NT = ((1,), (1,))
TN = ((0,), (0,))


class Links:
    def __init__(self, send_sem, recv_sem):
        self.send_sem, self.recv_sem = send_sem, recv_sem
        self.sends, self.used, self.keys = [], 0, {}

    def base(self, key, count):
        if key not in self.keys:
            self.keys[key] = self.used
            self.used += count
        return self.keys[key]

    def copy(self, src, dst, sent, got, to):
        return pltpu.make_async_remote_copy(
            src_ref=src,
            dst_ref=dst,
            send_sem=self.send_sem.at[sent],
            recv_sem=self.recv_sem.at[got],
            device_id=to,
            device_id_type=MESH,
        )

    def each(self, make, act):
        src, dst, sent, got, to, when = make()
        if when is None:
            act(self.copy(src, dst, sent, got, to))
        else:
            pl.when(when)(lambda: act(self.copy(src, dst, sent, got, to)))

    def start(self, make):
        self.sends.append(make)
        self.each(make, lambda copy: copy.start())

    def put(self, src, dst, sent, got, to, when=None):
        self.start(lambda: (src, dst, sent, got, to, when))

    def wait(self, dst, got, to):
        self.copy(dst, dst, 0, got, to).wait_recv()

    def finish(self):
        for make in self.sends:
            self.each(make, lambda copy: copy.wait_send())
        self.sends = []


def where_am_i():
    d = lax.axis_index("dp")
    return d // 4, (d // 2) % 2, d % 2, lax.axis_index("tensor")


def greet(y, x, c, z):
    barrier = pltpu.get_barrier_semaphore()
    peers = [(dy, dx, dc, 0) for dy in range(2) for dx in range(2) for dc in range(2) if dy + dx + dc]
    peers += [(0, 0, dc, dz) for dc in range(2) for dz in range(1, 4)]
    for dy, dx, dc, dz in peers:
        to = place((y + dy) % 2, (x + dx) % 2, (c + dc) % 2, (z + dz) % 4)
        pl.semaphore_signal(barrier, inc=1, device_id=to, device_id_type=MESH)
    pl.semaphore_wait(barrier, len(peers))


def unit_rows(v):
    average = jnp.mean(v, axis=-1, keepdims=True)
    centred = v - average
    variance = jnp.mean(centred * centred, axis=-1, keepdims=True)
    scale = lax.rsqrt(variance + EPSILON)
    return centred * scale, scale


def gelu_both(v):
    cdf = 0.5 * (1.0 + lax.erf(v * 0.7071067811865476))
    density = 0.3989422804014327 * jnp.exp(-0.5 * v * v)
    return v * cdf, cdf + v * density


def forward_kernel(
    tok_in, cot_in, mask_in, norm_in, bias_in, qkv_in, wo_in, w1_in, w2_in,
    tok, cot, mask, norm, bias, qkv, wo, up, down,
    n1, proj, lse, mix, hid, n2, act, slope,
    norm_row, qkv_row, up_row, part, got_part,
    local_sem, send_sem, recv_sem,
):
    y, x, c, z = where_am_i()
    r = y * 2 + x
    links = Links(send_sem, recv_sem)
    me = place(y, x, c, z)
    to_c, to_x, to_y = place(y, x, 1 - c, z), place(y, 1 - x, c, z), place(1 - y, x, c, z)
    up_z, down_z = place(y, x, c, jnp.minimum(z + 1, 3)), place(y, x, c, jnp.maximum(z - 1, 0))
    greet(y, x, c, z)

    def local(at, src, dst):
        return pltpu.make_async_copy(src, dst, local_sem.at[at])

    qkv_at = lambda rr, zz: qkv.at[at_rows(rr * 256, 256, 256), at_rows(zz * 384, 384, 128)]
    wo_at = lambda rr, zz: wo.at[at_rows(zz * 128, 128, 128), at_rows(rr * 256, 256, 128)]
    qkv_shard = qkv.at[at_rows(r * 256 + c * 128, 128, 128), at_rows(z * 384, 384, 128)]
    wo_shard = wo.at[at_rows(z * 128, 128, 128), at_rows(r * 256 + c * 128, 128, 128)]
    qkv_other = qkv.at[at_rows(r * 256 + (1 - c) * 128, 128, 128), at_rows(z * 384, 384, 128)]
    wo_other = wo.at[at_rows(z * 128, 128, 128), at_rows(r * 256 + (1 - c) * 128, 128, 128)]
    s_pc = links.base("pc", 2)
    links.put(qkv_in.at[:, at_rows((1 - c) * 384, 384, 128)], qkv_shard, s_pc, s_pc, to_c)
    links.put(wo_in.at[at_rows((1 - c) * 128, 128, 128), :], wo_shard, s_pc + 1, s_pc + 1, to_c)
    own_qkv = local(0, qkv_in.at[:, at_rows(c * 384, 384, 128)], qkv_shard)
    own_wo = local(1, wo_in.at[at_rows(c * 128, 128, 128), :], wo_shard)
    own_qkv.start()
    own_wo.start()

    s_norm, s_bias, s_mask = links.base("norm", 8), links.base("bias", 4), links.base("mask", 1)
    d = y * 4 + x * 2 + c
    for dd in range(1, 8):
        to = place((y + dd // 4) % 2, (x + (dd // 2) % 2) % 2, (c + dd % 2) % 2, z)
        links.put(norm_in, norm.at[d], s_norm + dd, s_norm + dd, to)
    for dz in range(1, 4):
        links.put(bias_in, bias.at[z], s_bias + dz, s_bias + dz, place(y, x, c, (z + dz) % 4))
    links.put(mask_in, mask.at[c], s_mask, s_mask, to_c)
    own_small = (local(2, norm_in, norm.at[d]), local(3, bias_in, bias.at[z]), local(4, mask_in, mask.at[c]))
    for one in own_small:
        one.start()

    def move_tokens(key, source, target_at, at):
        base = links.base(key, 4)
        target = target_at(z // 2)
        stay = c == z // 2
        rows = at_rows((z % 2) * Q, Q, 16)
        for i in range(2):
            here = jnp.logical_and(stay, z % 2 == i)
            to = place(y, x, z // 2, 2 * c + i)
            to = (jnp.where(here, place(y, x, 1 - c, z)[0], to[0]), to[1])
            links.put(source.at[i], target.at[rows], base + i, base + 2 + z % 2, to, jnp.logical_not(here))

            @pl.when(here)
            def _(i=i):
                local(at, source.at[i], target.at[rows]).start()

    def wait_tokens(key, source, target_at, at):
        base = links.base(key, 4)
        target = target_at(c)
        stay = c == z // 2
        for j in range(2):
            here = jnp.logical_and(stay, z % 2 == j)

            @pl.when(here)
            def _(j=j):
                local(at, source.at[j], target.at[pl.ds(j * Q, Q)]).wait()

            @pl.when(jnp.logical_not(here))
            def _(j=j):
                links.wait(target.at[pl.ds(j * Q, Q)], base + 2 + j, to_c)

    move_tokens("tok", tok_in, lambda cc: tok, 5)

    up_shard = lambda sx, sc: up.at[at_rows(y * 512 + sx * 256 + sc * 128, 128, 128), at_rows(z * 256, 256, 128)]
    down_shard = lambda sx, sc: down.at[at_rows(z * 256, 256, 128), at_rows(y * 512 + sx * 256 + sc * 128, 128, 128)]
    s_up, s_down = links.base("up", 4), links.base("down", 4)
    q = 2 * x + c
    for dx, dc in ((1, 0), (1, 1), (0, 1)):
        tx, tc = (x + dx) % 2, (c + dc) % 2
        to, rel = place(y, tx, tc, z), 2 * dx + dc
        links.put(w1_in.at[:, at_rows((2 * tx + tc) * 256, 256, 128)], up_shard(x, c), s_up + rel, s_up + rel, to)
        links.put(w2_in.at[at_rows((2 * tx + tc) * 256, 256, 128), :], down_shard(x, c), s_down + rel, s_down + rel, to)
    own_up = local(6, w1_in.at[:, at_rows(q * 256, 256, 128)], up_shard(x, c))
    own_down = local(7, w2_in.at[at_rows(q * 256, 256, 128), :], down_shard(x, c))
    own_up.start()
    own_down.start()

    class Line:
        def __init__(self, key, piece, arrived):
            self.piece, self.arrived = piece, arrived
            self.many = many = len(piece(0))
            self.got = [links.base((key, "got", n), 4) for n in range(many)]
            self.up = [links.base((key, "up", n), 4) for n in range(many)]
            self.down = [links.base((key, "down", n), 4) for n in range(many)]

        def push(self, way_up, far):
            def make(n):
                o, there = self.origin(way_up, far)
                ref = self.piece(o)[n]
                sent = (self.up if way_up else self.down)[n] + o
                onward = z < 3 if way_up else z > 0
                when = onward if there is None else jnp.logical_and(there, onward)
                return ref, ref, sent, self.got[n] + o, up_z if way_up else down_z, when

            for n in range(self.many):
                links.start(functools.partial(make, n))

        def origin(self, way_up, far):
            if far == 0:
                return z, None
            o = z - far if way_up else z + far
            return jnp.clip(o, 0, 3), (o >= 0 if way_up else o < 4)

        def begin(self):
            self.push(True, 0)
            self.push(False, 0)
            self.arrived(functools.partial(self.origin, True, 0))

        def step(self, far):
            for way_up in (True, False):
                o, there = self.origin(way_up, far)

                @pl.when(there)
                def _():
                    for n, ref in enumerate(self.piece(o)):
                        links.wait(ref, self.got[n] + o, up_z)

                self.push(way_up, far)
                self.arrived(functools.partial(self.origin, way_up, far))

    s_first = [links.base(("first", n), 4) for n in range(2)]
    s_own = [links.base(("own", n), 4) for n in range(2)]
    s_fwd = [links.base(("fwd", n), 4) for n in range(2)]

    def neighbours(o):
        odd = o % 2
        even = 1 - odd
        y1, x1 = y + odd * (1 - 2 * y), x + even * (1 - 2 * x)
        y2, x2 = y + even * (1 - 2 * y), x + odd * (1 - 2 * x)
        return (y1, x1), (y2, x2)

    def attn_arrived(origin):
        o, there = origin()
        (y1, x1), (y2, x2) = neighbours(o)
        for n, ref in enumerate((qkv_at(r, o), wo_at(r, o))):
            links.put(ref, ref, s_first[n] + o, s_first[n] + o, place(y1, x1, c, z), there)
            links.put(ref, ref, s_own[n] + o, s_own[n] + o, place(y2, x2, c, z), there)

    def attn_forward(o, there):
        (y1, x1), (y2, x2) = neighbours(o)
        r1 = 2 * y1 + x1
        for n, ref in enumerate((qkv_at(r1, o), wo_at(r1, o))):
            def arrive(n=n, ref=ref):
                links.wait(ref, s_first[n] + o, to_x)

            arrive() if there is None else pl.when(there)(arrive)

            links.put(ref, ref, s_fwd[n] + o, s_fwd[n] + o, place(y2, x2, c, z), there)

    def attn_finish():
        for o in range(4):
            (y1, x1), (y2, x2) = neighbours(o)
            for n, at in enumerate((qkv_at, wo_at)):
                links.wait(at(2 * y2 + x2, o), s_own[n] + o, to_x)
                links.wait(at(2 * (1 - y) + 1 - x, o), s_fwd[n] + o, to_x)

    attn_line = Line("attn", lambda o: (qkv_at(r, o), wo_at(r, o)), attn_arrived)
    up_at = lambda yy, o: up.at[at_rows(yy * 512, 512, 512), at_rows(o * 256, 256, 256)]
    down_at = lambda yy, o: down.at[at_rows(o * 256, 256, 256), at_rows(yy * 512, 512, 512)]
    s_upy, s_downy = links.base("upy", 4), links.base("downy", 4)

    def across(at, base):
        def arrived(origin):
            def make():
                o, there = origin()
                return at(y, o), at(y, o), base + o, base + o, to_y, there

            links.start(make)

        return arrived

    up_line = Line("upl", lambda o: (up_at(y, o),), across(up_at, s_upy))
    down_line = Line("downl", lambda o: (down_at(y, o),), across(down_at, s_downy))

    lse[...] = jnp.zeros_like(lse)
    own_qkv.wait()
    own_wo.wait()
    links.wait(qkv_other, s_pc, to_c)
    links.wait(wo_other, s_pc + 1, to_c)
    attn_line.begin()
    for one in own_small:
        one.wait()
    for dd in range(1, 8):
        source = 4 * ((y + dd // 4) % 2) + 2 * ((x + (dd // 2) % 2) % 2) + (c + dd % 2) % 2
        links.wait(norm.at[source], s_norm + dd, to_c)
    for dz in range(1, 4):
        links.wait(bias.at[(z + 4 - dz) % 4], s_bias + dz, to_c)
    links.wait(mask.at[1 - c], s_mask, to_c)
    for dd in range(8):
        norm_row[:, dd * 128 : dd * 128 + 128] = norm[dd]
    for zz in range(4):
        qkv_row[:, zz * 384 : zz * 384 + 128] = bias[zz, 0:1]
        qkv_row[:, zz * 384 + 128 : zz * 384 + 256] = jnp.zeros((1, 128), F32)
        qkv_row[:, zz * 384 + 256 : zz * 384 + 384] = bias[zz, 1:2]
        up_row[:, zz * 256 : zz * 256 + 128] = bias[zz, 2:3]
        up_row[:, zz * 256 + 128 : zz * 256 + 256] = bias[zz, 3:4]

    own_up.wait()
    own_down.wait()
    attn_line.step(1)
    attn_forward(z, None)

    wait_tokens("tok", tok_in, lambda cc: tok, 5)

    @pl.loop(0, HALF // 32)
    def _(i):
        v = tok[at_rows(i * 32, 32, 32), :].astype(F32)
        unit, _ = unit_rows(v)
        n1[at_rows(c * HALF + i * 32, 32, 32), :] = (unit * norm_row[0:1] + norm_row[2:3]).astype(BF)

    s_n1 = links.base("n1", 1)
    half_at = lambda ref, cc: ref.at[at_rows(cc * HALF, HALF, 64), :]
    links.put(half_at(n1, c), half_at(n1, c), s_n1, s_n1, to_c)

    def forward_far(far):
        attn_forward(jnp.clip(z - far, 0, 3), z >= far)
        attn_forward(jnp.clip(z + far, 0, 3), z + far < 4)

    attn_line.step(2)
    forward_far(1)
    attn_line.step(3)
    for dx, dc in ((1, 0), (1, 1), (0, 1)):
        rel, sx, sc = 2 * dx + dc, (x + dx) % 2, (c + dc) % 2
        links.wait(up_shard(sx, sc), s_up + rel, to_c)
    up_line.begin()
    forward_far(2)
    move_tokens("cot", cot_in, lambda cc: cot.at[2 * x + cc], 8)
    for dx, dc in ((1, 0), (1, 1), (0, 1)):
        rel, sx, sc = 2 * dx + dc, (x + dx) % 2, (c + dc) % 2
        links.wait(down_shard(sx, sc), s_down + rel, to_c)
    up_line.step(1)
    forward_far(3)
    down_line.begin()
    links.wait(half_at(n1, 1 - c), s_n1, to_c)
    attn_finish()

    @pl.loop(0, 6)
    def _(j):
        columns = at_rows(j * 256, 256, 256)
        proj[:, columns] = (mm(n1[...], qkv[:, columns], NN) + qkv_row[:, columns]).astype(BF)

    lane = lax.broadcasted_iota(jnp.int32, (1, 128), 1)
    first_head = lane < 64
    zero = jnp.zeros((), BF)
    up_line.step(2)

    @pl.loop(0, 4)
    def _(zz):
        keys = proj[:, at_rows(zz * 384 + 128, 128, 128)]
        values = proj[:, at_rows(zz * 384 + 256, 128, 128)]
        hidden_key = mask[z // 2, z % 2]
        for rb in range(2):
            rows = pl.ds(rb * HALF, HALF)
            pair = proj[rows, at_rows(zz * 384, 128, 128)]
            outs = []
            for hh in range(2):
                own = jnp.where(first_head if hh == 0 else jnp.logical_not(first_head), pair, zero)
                scores = mm(own, keys, NT) * (HD ** (-0.5)) + hidden_key
                highest = jnp.max(scores, axis=-1, keepdims=True)
                exponent = jnp.exp(scores - highest)
                total = jnp.sum(exponent, axis=-1, keepdims=True)
                low = (exponent * (1.0 / total)).astype(BF)
                head = 2 * zz + hh
                lse[rows, :] = jnp.where(lane == head, highest + jnp.log(total), lse[rows, :])
                outs.append(mm(low, values, NN))
            mix[rows, at_rows(zz * 128, 128, 128)] = jnp.where(first_head, outs[0], outs[1]).astype(BF)

        @pl.when(zz == 0)
        def _():
            down_line.step(1)

        @pl.when(zz == 1)
        def _():
            up_line.step(3)

        @pl.when(zz == 2)
        def _():
            down_line.step(2)

    down_line.step(3)

    s_part = links.base("part", 1)

    def project_out(cc, target):
        @pl.loop(0, 4)
        def _(j):
            columns = at_rows(j * 256, 256, 256)
            target[:, columns] = mm(mix[at_rows(cc * HALF, HALF, 64), :], wo[:, columns], NN)

    project_out(1 - c, part)
    links.put(part, got_part, s_part, s_part, to_c)
    project_out(c, hid)
    links.wait(got_part, s_part, to_c)

    @pl.loop(0, HALF // 32)
    def _(i):
        rows = at_rows(i * 32, 32, 32)
        v = hid[rows, :] + got_part[rows, :] + tok[rows, :].astype(F32) + norm_row[4:5]
        hid[rows, :] = v
        unit, _ = unit_rows(v)
        n2[q, rows, :] = (unit * norm_row[1:2] + norm_row[3:4]).astype(BF)

    def spread_start(key, ref):
        base = links.base(("spread", key), 3)
        links.put(ref.at[q], ref.at[q], base, base, to_x)
        links.put(ref.at[q], ref.at[q], base + 1, base + 1, to_c)

    def spread_forward(key, ref):
        base = links.base(("spread", key), 3)
        near, far, both = 2 * x + 1 - c, 2 * (1 - x) + c, 2 * (1 - x) + 1 - c
        links.wait(ref.at[far], base, to_x)
        links.put(ref.at[far], ref.at[far], base + 2, base + 2, to_c)

    def spread_wait_near(key, ref):
        links.wait(ref.at[2 * x + 1 - c], links.base(("spread", key), 3) + 1, to_c)

    def spread_wait_far(key, ref):
        links.wait(ref.at[2 * (1 - x) + 1 - c], links.base(("spread", key), 3) + 2, to_c)

    spread_start("n2", n2)
    wait_tokens("cot", cot_in, lambda cc: cot.at[2 * x + cc], 8)
    spread_start("cot", cot)
    for o in range(4):
        links.wait(up_at(1 - y, o), s_upy + o, to_y)

    def expand(t):
        @pl.loop(0, 4)
        def _(j):
            columns = at_rows(j * 256, 256, 256)
            for rb in range(2):
                rows = pl.ds(rb * Q, Q)
                v = mm(n2[t, rows, :], up[:, columns], NN) + up_row[:, columns]
                value, grade = gelu_both(v)
                act[t, rows, columns] = value.astype(BF)
                slope[t, rows, columns] = grade.astype(BF)

    expand(q)
    spread_wait_near("n2", n2)
    expand(2 * x + 1 - c)
    spread_forward("n2", n2)
    expand(2 * (1 - x) + c)
    spread_wait_far("n2", n2)
    expand(2 * (1 - x) + 1 - c)
    spread_wait_near("cot", cot)
    spread_forward("cot", cot)
    spread_wait_far("cot", cot)
    for o in range(4):
        links.wait(down_at(1 - y, o), s_downy + o, to_y)
    links.finish()


def forward_call(*operands):
    shape = jax.ShapeDtypeStruct
    outs = [
        shape((HALF, 1024), BF), shape((4, HALF, 1024), BF), shape((2, 2, 1, FULL), F32), shape((8, 8, 128), F32),
        shape((4, 8, 128), F32), shape((1024, 1536), BF), shape((512, 1024), BF), shape((1024, 1024), BF),
        shape((1024, 1024), BF), shape((FULL, 1024), BF), shape((FULL, 1536), BF), shape((FULL, 128), F32),
        shape((FULL, 512), BF), shape((HALF, 1024), F32), shape((4, HALF, 1024), BF), shape((4, HALF, 1024), BF),
        shape((4, HALF, 1024), BF),
    ]
    return pl.pallas_call(
        forward_kernel,
        out_shape=outs,
        in_specs=[pl.BlockSpec(memory_space=pl.ANY)] * 9,
        out_specs=[pl.BlockSpec(memory_space=pltpu.VMEM)] * len(outs),
        scratch_shapes=[
            pltpu.VMEM((8, 1024), F32), pltpu.VMEM((1, 1536), F32), pltpu.VMEM((1, 1024), F32),
            pltpu.VMEM((HALF, 1024), F32), pltpu.VMEM((HALF, 1024), F32),
            pltpu.SemaphoreType.DMA((16,)), pltpu.SemaphoreType.DMA((160,)), pltpu.SemaphoreType.DMA((160,)),
        ],
        compiler_params=pltpu.CompilerParams(collective_id=0, has_side_effects=True, vmem_limit_bytes=63 << 20),
        name="layer_forward",
    )(*operands)


def prepare(inputs, valid_mask, cotangent, ln_gain, d_bias, w_qkv, b_qv, b_1):
    y, x, c, z = where_am_i()
    rows = inputs.shape[0]
    turn = lambda v: jnp.pad(jnp.transpose(v, (1, 0, 2)), ((0, 0), (0, Q - rows), (0, 0)))
    mask = jnp.where(valid_mask.reshape(2, 4, rows) > 0, 0.0, MASKED).astype(F32)
    mask = jnp.pad(mask, ((0, 0), (0, 0), (0, Q - rows)), constant_values=MASKED).reshape(2, 1, FULL)
    norm = jnp.pad(jnp.concatenate([ln_gain, d_bias]).astype(F32), ((0, 2), (0, 0)))
    bias = jnp.concatenate(
        [
            lax.dynamic_slice(b_qv, (0, c * 128), (2, 128)),
            lax.dynamic_slice(b_1, ((2 * x + c) * 256,), (256,)).reshape(2, 128),
        ]
    ).astype(F32)
    bias = jnp.pad(bias, ((0, 4), (0, 0)))
    qkv = jnp.transpose(w_qkv.reshape(128, 3, 2, 128), (0, 2, 1, 3)).reshape(128, 768)
    return turn(inputs), turn(cotangent), mask, norm, bias, qkv


def bits():
    d = lax.axis_index("dp")
    return d // 4, (d // 2) % 2, d % 2, lax.axis_index("tensor")


def table(f):
    pairs = []
    for y in range(2):
        for x in range(2):
            for c in range(2):
                for z in range(4):
                    ty, tx, tc, tz = f(y, x, c, z)
                    pairs.append((((y * 2 + x) * 2 + c) * 4 + z, ((ty * 2 + tx) * 2 + tc) * 4 + tz))
    return pairs


def flip(pairs):
    return [(b, a) for a, b in pairs]


TO_C = table(lambda y, x, c, z: (y, x, 1 - c, z))
TO_X = table(lambda y, x, c, z: (y, 1 - x, c, z))
TO_Y = table(lambda y, x, c, z: (1 - y, x, c, z))
TO_XC = table(lambda y, x, c, z: (y, 1 - x, 1 - c, z))
TO_Z = table(lambda y, x, c, z: (y, x, c, (z + 3) % 4))
SWAP_0 = table(lambda y, x, c, z: (y, x, z // 2, 2 * c + z % 2))
SWAP_1 = table(lambda y, x, c, z: (y, x, z // 2, 2 * c + 1 - z % 2))


def send(value, pairs):
    return lax.ppermute(value, ("dp", "tensor"), pairs)


def pick(bit, first, second):
    return jnp.where(bit == 0, first, second), jnp.where(bit == 0, second, first)


def order4(hi, lo, own, other_lo, other_hi, other_both):
    a0, a1 = pick(lo, own, other_lo)
    b0, b1 = pick(lo, other_hi, other_both)
    first = pick(hi, a0, b0)
    second = pick(hi, a1, b1)
    return first[0], second[0], first[1], second[1]


def ring_gather(piece):
    pieces = [piece]
    for _ in range(3):
        pieces.append(send(pieces[-1], TO_Z))
    return pieces


def ring_scatter(terms):
    total = terms[1]
    for at in (2, 3, 0):
        total = send(total.astype(jnp.bfloat16), TO_Z).astype(jnp.float32) + terms[at]
    return total


def scatter4(blocks, y, x, c):
    kept = send(blocks(1 - x, c), TO_X), send(blocks(x, 1 - c), TO_C), send(blocks(1 - x, 1 - c), TO_XC)
    return order4(x, c, blocks(x, c), kept[1], kept[0], kept[2])


def tokens_in(values, z):
    rows = values.shape[0]
    turned = jnp.pad(jnp.transpose(values, (1, 0, 2)), ((0, 0), (0, Q - rows), (0, 0)))
    first, second = pick(z % 2, turned[0], turned[1])
    return jnp.concatenate([send(first, SWAP_0), send(second, SWAP_1)])


def tokens_out(values, z, rows):
    first = send(values[:Q], flip(SWAP_0))
    second = send(values[Q:], flip(SWAP_1))
    images = pick(z % 2, first, second)
    return jnp.stack([images[0][:rows], images[1][:rows]], axis=1)


def norm_parts(values):
    average = jnp.mean(values, axis=-1, keepdims=True)
    centred = values - average
    variance = jnp.mean(centred * centred, axis=-1, keepdims=True)
    scale = lax.rsqrt(variance + EPSILON)
    return centred * scale, scale


def norm_back(grad, unit, scale, gain):
    q = grad * gain
    return scale * (
        q - jnp.mean(q, axis=-1, keepdims=True) - unit * jnp.mean(q * unit, axis=-1, keepdims=True)
    )


def dot32(left, right, dims):
    return lax.dot_general(left, right, (dims, ((), ())), preferred_element_type=jnp.float32)


def fast_body2(inputs, valid_mask, cotangent, ln_gain, d_bias, w_qkv, b_qv, w_o, w_1, b_1, w_2):
    y, x, c, z = where_am_i()
    r, q, rows, f32, bf = 2 * y + x, 2 * x + c, inputs.shape[0], F32, BF
    tok_in, cot_in, mask_in, norm_in, bias_in, qkv_in = prepare(
        inputs, valid_mask, cotangent, ln_gain, d_bias, w_qkv, b_qv, b_1
    )
    (tok, cot, mask, norm, bias, wide_qkv, wide_out, wide_up, wide_down, n1, proj, lse, mix, hid, n2, act, slope) = forward_call(
        tok_in, cot_in, mask_in, norm_in, bias_in, qkv_in, w_o, w_1, w_2
    )
    norm = jnp.transpose(norm, (1, 0, 2)).reshape(8, 1024)
    gains, shifts = norm[:2], norm[2:6]
    key_bias = mask[z // 2, z % 2, 0]
    heads = jnp.transpose(proj.reshape(FULL, 4, 3, 2, HD), (2, 0, 1, 3, 4)).reshape(3, FULL, 8, HD)
    queries, keys_part, values_part = heads[0], heads[1], heads[2]
    factor = HD ** (-0.5)
    scores = jnp.einsum("qhd,khd->hqk", queries, keys_part, preferred_element_type=f32) * factor + key_bias
    log_total = lse[:, :8].T[:, :, None]
    half = HALF
    own_half = lambda v: lax.dynamic_slice_in_dim(v, c * half, half, 0)
    other_half = lambda v: lax.dynamic_slice_in_dim(v, (1 - c) * half, half, 0)
    residual = tok.astype(f32)
    unit1, scale1 = norm_parts(residual)
    unit2, scale2 = norm_parts(hid)
    grad_out = lax.dynamic_index_in_dim(cot, q, 0, keepdims=False).astype(f32)

    def collect(part):
        part = part.reshape(4, half, 1024)
        get = lambda xx, cc: lax.dynamic_index_in_dim(part, 2 * xx + cc, 0, keepdims=False)
        a, b, at_x, at_xc = get(x, c), get(x, 1 - c), get(1 - x, c), get(1 - x, 1 - c)
        far = at_x + send(at_xc.astype(bf), TO_C).astype(f32)
        near = a + send(b.astype(bf), TO_C).astype(f32)
        return near + send(far.astype(bf), TO_X).astype(f32)

    flat = lambda v: v.reshape(4 * half, 1024)
    branch = collect(dot32(flat(act), wide_down, NN))
    s0, s1 = SWAP_0, SWAP_1

    def tokens_back(values):
        images = []
        for i in range(2):
            pass
        first, second = pick(z % 2, values[:Q], values[Q:])
        b0, b1 = send(first, flip(SWAP_0)), send(second, flip(SWAP_1))
        im = pick(z % 2, b0, b1)
        return jnp.stack([im[0][:rows], im[1][:rows]], axis=1)

    block_output = tokens_back((hid + branch + shifts[3]).astype(bf))
    grad_w_2 = dot32(flat(act), flat(cot), TN)
    grad_active = dot32(flat(cot), wide_down, NT)
    grad_hidden_in = grad_active * flat(slope).astype(f32)
    grad_b_1 = jnp.sum(grad_hidden_in, axis=0)
    grad_hidden_low = grad_hidden_in.astype(bf)
    grad_w_1 = dot32(flat(n2), grad_hidden_low, TN)
    grad_normed2 = collect(dot32(grad_hidden_low, wide_up, NT))
    grad_hidden1 = grad_out + norm_back(grad_normed2, unit2, scale2, gains[1])
    grad_attn_own = grad_hidden1.astype(bf)
    grad_attn = jnp.concatenate(pick(c, grad_attn_own, send(grad_attn_own, TO_C)))
    grad_w_o = dot32(mix, grad_attn, TN)
    grad_mixture = dot32(grad_attn, wide_out, NT).astype(bf).reshape(FULL, 8, HD)
    attention = jnp.exp(scores - log_total)
    attention_low = attention.astype(bf)
    grad_values = jnp.einsum("hqk,qhd->khd", attention_low, grad_mixture, preferred_element_type=f32)
    grad_attention = jnp.einsum("qhd,khd->hqk", grad_mixture, values_part, preferred_element_type=f32)
    inner = jnp.sum(attention * grad_attention, axis=-1, keepdims=True)
    grad_scores = (attention * (grad_attention - inner)).astype(bf)
    grad_queries = jnp.einsum("hqk,khd->qhd", grad_scores, keys_part, preferred_element_type=f32) * factor
    grad_keys = jnp.einsum("hqk,qhd->khd", grad_scores, queries, preferred_element_type=f32) * factor
    grad_projected = jnp.stack([grad_queries, grad_keys, grad_values]).reshape(3, FULL, 4, 128)
    grad_b_qv = jnp.sum(grad_projected, axis=1).reshape(3, 4, 128)
    grad_projected_low = jnp.transpose(grad_projected, (1, 2, 0, 3)).astype(bf).reshape(FULL, 1536)
    grad_w_qkv = dot32(n1, grad_projected_low, TN)
    part = dot32(grad_projected_low, wide_qkv, NT)
    grad_normed1 = own_half(part) + send(other_half(part), TO_C)
    grad_inputs = grad_hidden1 + norm_back(grad_normed1, unit1, scale1, gains[0])
    grad_inputs = tokens_back(grad_inputs.astype(bf)).astype(f32)

    cut = lambda array, at, size, axis: lax.dynamic_slice_in_dim(array, at * size, size, axis)
    terms = []
    for at in range(4):
        block = cut(grad_w_1, (z + at) % 4, 256, 1)
        far = send(cut(block, 1 - y, 512, 0).astype(bf), TO_Y).astype(f32)
        terms.append(cut(block, y, 512, 0) + far)
    total = ring_scatter(terms).astype(bf)
    out_w_1 = jnp.concatenate(
        scatter4(lambda bx, bc: cut(total, 2 * bx + bc, 128, 0), y, x, c), axis=1
    ).astype(f32)
    terms = []
    for at in range(4):
        block = cut(grad_w_2, (z + at) % 4, 256, 0)
        far = send(cut(block, 1 - y, 512, 1).astype(bf), TO_Y).astype(f32)
        terms.append(cut(block, y, 512, 1) + far)
    total2 = ring_scatter(terms).astype(bf)
    out_w_2 = jnp.concatenate(
        scatter4(lambda bx, bc: cut(total2, 2 * bx + bc, 128, 1), y, x, c), axis=0
    ).astype(f32)
    terms = []
    for at in range(4):
        zz = (z + at) % 4

        def block(rel):
            rr = r ^ rel
            left = cut(cut(grad_w_qkv, zz, 384, 1), rr, 256, 0)
            right = cut(cut(grad_w_o, zz, 128, 0), rr, 256, 1)
            right = jnp.concatenate([right[:, :128], right[:, 128:]])
            return jnp.concatenate([left, right], axis=1)

        near, far, first, second = (1, 2, TO_X, TO_Y) if at % 2 == 0 else (2, 1, TO_Y, TO_X)
        mid = block(far) + send(block(3).astype(bf), first).astype(f32)
        own = block(0) + send(block(near).astype(bf), first).astype(f32)
        terms.append(own + send(mid.astype(bf), second).astype(f32))
    total3 = ring_scatter(terms).astype(bf)
    keep, give = cut(total3, c, 128, 0), cut(total3, 1 - c, 128, 0)
    both = pick(c, keep, send(give, TO_C))
    out_w_qkv = jnp.stack([h[:, :384].reshape(128, 3, 128) for h in both], axis=2).reshape(128, 3, 256).astype(f32)
    out_w_o = jnp.concatenate([h[:, 384:] for h in both]).astype(f32)
    sums = jnp.stack(
        [
            jnp.sum(grad_normed1 * unit1, axis=0),
            jnp.sum(grad_normed2 * unit2, axis=0),
            jnp.sum(grad_normed1, axis=0),
            jnp.sum(grad_normed2, axis=0),
            jnp.sum(grad_hidden1, axis=0),
            jnp.sum(grad_out, axis=0),
        ]
    )
    sums = lax.psum(sums, ("dp", "tensor"))
    own_sums = lax.dynamic_slice(sums, (0, lax.axis_index("dp") * 128), (6, 128))
    qv = jnp.stack([grad_b_qv[0], grad_b_qv[2]])
    place_qv = jnp.where((jnp.arange(2) == c)[None, None, :, None], qv[:, :, None, :], 0.0)
    place_up = jnp.where((jnp.arange(4) == q)[None, :, None], grad_b_1.reshape(4, 1, 256), 0.0)
    packed = jnp.concatenate([jnp.transpose(place_qv, (1, 0, 2, 3)).reshape(4, 512), place_up.reshape(4, 1024)], axis=1)
    packed = lax.psum(packed, ("dp", "tensor"))
    mine_b = lax.dynamic_index_in_dim(packed, z, 0, keepdims=False)
    return (
        block_output, grad_inputs, own_sums[:2], own_sums[2:], out_w_qkv, mine_b[:512].reshape(2, 256),
        out_w_o, out_w_1, mine_b[512:], out_w_2,
    )


def solution(mesh):
    in_specs = (
        P("tensor", "dp", None),
        P("dp", None),
        P("tensor", "dp", None),
        P(None, "dp"),
        P(None, "dp"),
        P("dp", None, "tensor"),
        P(None, "tensor"),
        P("tensor", "dp"),
        P("dp", "tensor"),
        P("tensor"),
        P("tensor", "dp"),
    )
    out_specs = (
        P("tensor", "dp", None),
        P("tensor", "dp", None),
        P(None, "dp"),
        P(None, "dp"),
        P("dp", None, "tensor"),
        P(None, "tensor"),
        P("tensor", "dp"),
        P("dp", "tensor"),
        P("tensor"),
        P("tensor", "dp"),
    )
    run = fast_body2 if dict(mesh.shape) == {"dp": 8, "tensor": 4} else body
    return jax.shard_map(run, mesh=mesh, in_specs=in_specs, out_specs=out_specs, check_vma=False)
```

```python
import functools

import jax
import jax.numpy as jnp
from jax import lax
from jax.experimental import pallas as pl
from jax.experimental.pallas import tpu as pltpu
from jax.sharding import PartitionSpec as P

HD = 64


EPSILON = 1e-06
MASKED = -1e30


def layer_norm(values, gain, shift):
    average = jnp.mean(values, axis=-1, keepdims=True)
    centred = values - average
    variance = jnp.mean(centred * centred, axis=-1, keepdims=True)
    return centred * lax.rsqrt(variance + EPSILON) * gain + shift


def gelu_exact(values):
    return jax.nn.gelu(values, approximate=False)


def gather_layer(ln_gain, d_bias, w_qkv, w_o, w_1, w_2):
    return (
        lax.all_gather(ln_gain, "dp", axis=1, tiled=True),
        lax.all_gather(d_bias, "dp", axis=1, tiled=True),
        lax.all_gather(w_qkv, "dp", axis=0, tiled=True),
        lax.all_gather(w_o, "dp", axis=1, tiled=True),
        lax.all_gather(w_1, "dp", axis=0, tiled=True),
        lax.all_gather(w_2, "dp", axis=1, tiled=True),
    )


def masked_scores(queries, keys_part, valid):
    scores = jnp.einsum(
        "qhd,khd->hqk", queries, keys_part, preferred_element_type=jnp.float32
    ) * HD ** (-0.5)
    return jnp.where(valid[None, None, :] > 0, scores, MASKED)


def attend_forward(bundle):
    packed, valid = bundle
    scores = masked_scores(packed[:, 0], packed[:, 1], valid)
    highest = jnp.max(scores, axis=-1, keepdims=True)
    exponent = jnp.exp(scores - highest)
    denominator = jnp.sum(exponent, axis=-1, keepdims=True)
    attention = (exponent / denominator).astype(jnp.bfloat16)
    mixture = jnp.einsum(
        "hqk,khd->qhd", attention, packed[:, 2], preferred_element_type=jnp.float32
    )
    return (mixture.astype(jnp.bfloat16), (highest + jnp.log(denominator))[..., 0])


def attend_backward(bundle):
    packed, grad_mixture, log_total, valid = bundle
    queries = packed[:, 0]
    keys_part = packed[:, 1]
    values_part = packed[:, 2]
    scores = masked_scores(queries, keys_part, valid)
    attention = jnp.exp(scores - log_total[..., None])
    attention_low = attention.astype(jnp.bfloat16)
    grad_values = jnp.einsum(
        "hqk,qhd->khd", attention_low, grad_mixture, preferred_element_type=jnp.float32
    )
    grad_attention = jnp.einsum(
        "qhd,khd->hqk", grad_mixture, values_part, preferred_element_type=jnp.float32
    )
    inner = jnp.sum(attention * grad_attention, axis=-1, keepdims=True)
    grad_scores = (attention * (grad_attention - inner)).astype(jnp.bfloat16)
    factor = HD ** (-0.5)
    grad_queries = (
        jnp.einsum("hqk,khd->qhd", grad_scores, keys_part, preferred_element_type=jnp.float32)
        * factor
    )
    grad_keys = (
        jnp.einsum("hqk,qhd->khd", grad_scores, queries, preferred_element_type=jnp.float32)
        * factor
    )
    return jnp.stack([grad_queries, grad_keys, grad_values], axis=1)


def body(inputs, valid_mask, cotangent, ln_gain, d_bias, w_qkv, b_qv, w_o, w_1, b_1, w_2):
    local_rows, images, model_width = inputs.shape
    layer = gather_layer(ln_gain, d_bias, w_qkv, w_o, w_1, w_2)
    gains = layer[0].astype(jnp.float32)
    shifts = layer[1].astype(jnp.float32)
    wide_qkv = layer[2].reshape(model_width, -1)
    wide_out = layer[3]
    wide_up = layer[4]
    wide_down = layer[5]
    residual = inputs.astype(jnp.float32)
    normed1 = layer_norm(residual, gains[0], shifts[0]).astype(jnp.bfloat16)
    gathered1 = lax.all_gather(normed1, "tensor", axis=0, tiled=True)
    full_length = gathered1.shape[0]
    columns = b_qv.shape[1]
    heads_local = columns // HD
    projected = jnp.dot(gathered1, wide_qkv, preferred_element_type=jnp.float32).reshape(
        full_length, images, 3, columns
    )
    qkv_bias = jnp.stack([b_qv[0], jnp.zeros_like(b_qv[0]), b_qv[1]]).astype(jnp.float32)
    projected_low = (projected + qkv_bias).astype(jnp.bfloat16)
    per_image = jnp.transpose(projected_low, (1, 0, 2, 3)).reshape(
        images, full_length, 3, heads_local, HD
    )
    mixture, log_total = lax.map(attend_forward, (per_image, valid_mask))
    mixture_seq = jnp.transpose(mixture, (1, 0, 2, 3)).reshape(full_length, images, columns)
    segment = mixture_seq
    attn_sum = lax.psum_scatter(
        jnp.dot(segment, wide_out, preferred_element_type=jnp.float32),
        "tensor",
        scatter_dimension=0,
        tiled=True,
    )
    hidden1 = residual + attn_sum + shifts[2]
    normed2 = layer_norm(hidden1, gains[1], shifts[1]).astype(jnp.bfloat16)
    gathered2 = lax.all_gather(normed2, "tensor", axis=0, tiled=True)
    hidden_in = jnp.dot(gathered2, wide_up, preferred_element_type=jnp.float32) + b_1.astype(
        jnp.float32
    )
    active = gelu_exact(hidden_in).astype(jnp.bfloat16)
    segment = active
    branch_sum = lax.psum_scatter(
        jnp.dot(segment, wide_down, preferred_element_type=jnp.float32).astype(jnp.bfloat16),
        "tensor",
        scatter_dimension=0,
        tiled=True,
    ).astype(jnp.float32)
    block_output = (hidden1 + branch_sum + shifts[3]).astype(jnp.bfloat16)
    layer = gather_layer(ln_gain, d_bias, w_qkv, w_o, w_1, w_2)
    wide_qkv = layer[2].reshape(model_width, -1)
    wide_out = layer[3]
    wide_up = layer[4]
    wide_down = layer[5]
    grad_out = cotangent.astype(jnp.float32)
    grad_gathered = lax.all_gather(cotangent, "tensor", axis=0, tiled=True)
    grad_w_2 = jnp.einsum("sif,sid->fd", active, grad_gathered, preferred_element_type=jnp.float32)
    grad_active = jnp.einsum(
        "sid,fd->sif", grad_gathered, wide_down, preferred_element_type=jnp.float32
    )
    grad_hidden_in = jax.vjp(gelu_exact, hidden_in)[1](grad_active)[0]
    grad_b_1 = jnp.sum(grad_hidden_in, axis=(0, 1))
    grad_hidden_low = grad_hidden_in.astype(jnp.bfloat16)
    grad_w_1 = jnp.einsum(
        "sid,sif->df", gathered2, grad_hidden_low, preferred_element_type=jnp.float32
    )
    segment = grad_hidden_low
    grad_normed2 = lax.psum_scatter(
        jnp.einsum("sif,df->sid", segment, wide_up, preferred_element_type=jnp.float32),
        "tensor",
        scatter_dimension=0,
        tiled=True,
    )
    second_pull = jax.vjp(layer_norm, hidden1, gains[1], shifts[1])[1]
    grad_from_norm, gain2_grad, shift2_grad = second_pull(grad_normed2)
    grad_hidden1 = grad_out + grad_from_norm
    grad_attn_low = grad_hidden1.astype(jnp.bfloat16)
    grad_attn_all = lax.all_gather(grad_attn_low, "tensor", axis=0, tiled=True)
    grad_w_o = jnp.einsum(
        "sic,sid->cd", mixture_seq, grad_attn_all, preferred_element_type=jnp.float32
    )
    grad_mixture = jnp.einsum(
        "sid,cd->sic", grad_attn_all, wide_out, preferred_element_type=jnp.float32
    ).astype(jnp.bfloat16)
    grad_mixture_img = jnp.transpose(
        grad_mixture.reshape(full_length, images, heads_local, HD), (1, 0, 2, 3)
    )
    grad_packed = lax.map(attend_backward, (per_image, grad_mixture_img, log_total, valid_mask))
    grad_projected = jnp.transpose(grad_packed, (1, 0, 2, 3, 4)).reshape(
        full_length, images, 3, columns
    )
    grad_b_qv = jnp.stack(
        [
            jnp.sum(grad_projected[:, :, 0], axis=(0, 1)),
            jnp.sum(grad_projected[:, :, 2], axis=(0, 1)),
        ]
    )
    grad_projected_low = grad_projected.reshape(full_length, images, 3 * columns).astype(
        jnp.bfloat16
    )
    grad_w_qkv = jnp.einsum(
        "sid,sic->dc", gathered1, grad_projected_low, preferred_element_type=jnp.float32
    ).reshape(model_width, 3, columns)
    segment = grad_projected_low
    grad_normed1 = lax.psum_scatter(
        jnp.einsum("sic,dc->sid", segment, wide_qkv, preferred_element_type=jnp.float32).astype(
            jnp.bfloat16
        ),
        "tensor",
        scatter_dimension=0,
        tiled=True,
    ).astype(jnp.float32)
    first_pull = jax.vjp(layer_norm, residual, gains[0], shifts[0])[1]
    grad_from_front, gain1_grad, shift1_grad = first_pull(grad_normed1)
    grad_inputs = grad_hidden1 + grad_from_front
    gain_terms = jnp.stack([gain1_grad, gain2_grad])
    shift_terms = jnp.stack(
        [
            shift1_grad,
            shift2_grad,
            jnp.sum(grad_hidden1, axis=(0, 1)),
            jnp.sum(grad_out, axis=(0, 1)),
        ]
    )
    scattered = (
        lax.psum_scatter(
            gain_terms.astype(jnp.bfloat16), "dp", scatter_dimension=1, tiled=True
        ).astype(jnp.float32),
        lax.psum_scatter(
            shift_terms.astype(jnp.bfloat16), "dp", scatter_dimension=1, tiled=True
        ).astype(jnp.float32),
        lax.psum_scatter(
            grad_w_qkv.astype(jnp.bfloat16), "dp", scatter_dimension=0, tiled=True
        ).astype(jnp.float32),
        lax.psum_scatter(
            grad_w_o.astype(jnp.bfloat16), "dp", scatter_dimension=1, tiled=True
        ).astype(jnp.float32),
        lax.psum_scatter(
            grad_w_1.astype(jnp.bfloat16), "dp", scatter_dimension=0, tiled=True
        ).astype(jnp.float32),
        lax.psum_scatter(
            grad_w_2.astype(jnp.bfloat16), "dp", scatter_dimension=1, tiled=True
        ).astype(jnp.float32),
    )
    gain_sum, shift_sum = lax.psum((scattered[0], scattered[1]), "tensor")
    bias_qv_sum, bias_up_sum = lax.psum((grad_b_qv, grad_b_1), "dp")
    return (
        block_output,
        grad_inputs,
        gain_sum,
        shift_sum,
        scattered[2],
        bias_qv_sum,
        scattered[3],
        scattered[4],
        bias_up_sum,
        scattered[5],
    )


Q = 160
HALF = 2 * Q
FULL = 4 * Q
BF, F32 = jnp.bfloat16, jnp.float32
MESH = pl.DeviceIdType.MESH


def place(y, x, c, z):
    return (y * 4 + x * 2 + c, z)


def at_rows(start, size, step=8):
    return pl.ds(pl.multiple_of(start, step), size)


def mm(left, right, dims):
    return lax.dot_general(left, right, (dims, ((), ())), preferred_element_type=F32)


NN = ((1,), (0,))
NT = ((1,), (1,))
TN = ((0,), (0,))


class Links:
    def __init__(self, send_sem, recv_sem):
        self.send_sem, self.recv_sem = send_sem, recv_sem
        self.sends, self.used, self.keys, self.dropped = [], 0, {}, set()

    def base(self, key, count):
        if key not in self.keys:
            self.keys[key] = self.used
            self.used += count
        return self.keys[key]

    def copy(self, src, dst, sent, got, to):
        return pltpu.make_async_remote_copy(
            src_ref=src,
            dst_ref=dst,
            send_sem=self.send_sem.at[sent],
            recv_sem=self.recv_sem.at[got],
            device_id=to,
            device_id_type=MESH,
        )

    def drop(self, *sent):
        self.dropped = self.dropped | set(sent)

    def each(self, make, act):
        src, dst, sent, got, to, when = make()
        if when is None:
            act(self.copy(src, dst, sent, got, to))
        else:
            pl.when(when)(lambda: act(self.copy(src, dst, sent, got, to)))

    def start(self, make):
        self.sends.append(make)
        self.each(make, lambda copy: copy.start())

    def put(self, src, dst, sent, got, to, when=None):
        self.start(lambda: (src, dst, sent, got, to, when))

    def wait(self, dst, got, to):
        self.copy(dst, dst, 0, got, to).wait_recv()

    def finish(self):
        for make in self.sends:
            sent = make()[2]
            if not (isinstance(sent, int) and sent in self.dropped):
                self.each(make, lambda copy: copy.wait_send())


def where_am_i():
    d = lax.axis_index("dp")
    return d // 4, (d // 2) % 2, d % 2, lax.axis_index("tensor")


def greet(y, x, c, z):
    barrier = pltpu.get_barrier_semaphore()
    peers = [(dy, dx, dc, 0) for dy in range(2) for dx in range(2) for dc in range(2) if dy + dx + dc]
    peers += [(0, 0, dc, dz) for dc in range(2) for dz in range(1, 4)]
    for dy, dx, dc, dz in peers:
        to = place((y + dy) % 2, (x + dx) % 2, (c + dc) % 2, (z + dz) % 4)
        pl.semaphore_signal(barrier, inc=1, device_id=to, device_id_type=MESH)
    pl.semaphore_wait(barrier, len(peers))


def unit_rows(v):
    average = jnp.mean(v, axis=-1, keepdims=True)
    centred = v - average
    variance = jnp.mean(centred * centred, axis=-1, keepdims=True)
    scale = lax.rsqrt(variance + EPSILON)
    return centred * scale, scale


def gelu_both(v):
    cdf = 0.5 * (1.0 + lax.erf(v * 0.7071067811865476))
    density = 0.3989422804014327 * jnp.exp(-0.5 * v * v)
    return v * cdf, cdf + v * density


def layer_kernel(
    tok_in, cot_in, mask_in, norm_in, bias_in, qkv_in, wo_in, w1_in, w2_in,
    block_out, grad_out, sums_out, qv_out, b1_out, qkv_out, wo_out, w1_out, w2_out,
    tok, cot, mask, norm, bias, qkv, wo, up, down,
    n1, proj, lse, mix, hid, n2, act, slope,
    norm_row, qkv_row, up_row, part, got_part,
    ga, gmix, gproj, d_up, d_down, d_qkv, d_wo, r_up, r_down, z_up, z_down, f_up, f_down, o_up, o_down,
    first_qkv, first_wo, second_qkv, second_wo, z_qkv, z_wo, f_qkv, f_wo, o_qkv, o_wo,
    s_far, s_mid, s_near, g_far, g_mid, g_near, b_far, b_mid, b_near, g_n1,
    sums, sums_row, sums_got, sums_z, gb1, gbq, gbv, bias_pack, bias_got, bias_all,
    local_sem, send_sem, recv_sem,
):
    y, x, c, z = where_am_i()
    r = y * 2 + x
    links = Links(send_sem, recv_sem)
    me = place(y, x, c, z)
    to_c, to_x, to_y = place(y, x, 1 - c, z), place(y, 1 - x, c, z), place(1 - y, x, c, z)
    up_z, down_z = place(y, x, c, jnp.minimum(z + 1, 3)), place(y, x, c, jnp.maximum(z - 1, 0))
    greet(y, x, c, z)

    block_at = lambda ref, t: ref.at[at_rows(t * HALF, HALF, 64), :]
    block_rows = lambda t, start, size: at_rows(t * HALF + start, size, 32)

    def local(at, src, dst):
        return pltpu.make_async_copy(src, dst, local_sem.at[at])

    qkv_at = lambda rr, zz: qkv.at[at_rows(rr * 256, 256, 256), at_rows(zz * 384, 384, 128)]
    wo_at = lambda rr, zz: wo.at[at_rows(zz * 128, 128, 128), at_rows(rr * 256, 256, 128)]
    qkv_shard = qkv.at[at_rows(r * 256 + c * 128, 128, 128), at_rows(z * 384, 384, 128)]
    wo_shard = wo.at[at_rows(z * 128, 128, 128), at_rows(r * 256 + c * 128, 128, 128)]
    qkv_other = qkv.at[at_rows(r * 256 + (1 - c) * 128, 128, 128), at_rows(z * 384, 384, 128)]
    wo_other = wo.at[at_rows(z * 128, 128, 128), at_rows(r * 256 + (1 - c) * 128, 128, 128)]
    s_pc = links.base("pc", 2)
    links.put(qkv_in.at[:, at_rows((1 - c) * 384, 384, 128)], qkv_shard, s_pc, s_pc, to_c)
    links.put(wo_in.at[at_rows((1 - c) * 128, 128, 128), :], wo_shard, s_pc + 1, s_pc + 1, to_c)
    own_qkv = local(0, qkv_in.at[:, at_rows(c * 384, 384, 128)], qkv_shard)
    own_wo = local(1, wo_in.at[at_rows(c * 128, 128, 128), :], wo_shard)
    own_qkv.start()
    own_wo.start()

    s_norm, s_bias, s_mask = links.base("norm", 8), links.base("bias", 4), links.base("mask", 1)
    d = y * 4 + x * 2 + c
    for dd in range(1, 8):
        to = place((y + dd // 4) % 2, (x + (dd // 2) % 2) % 2, (c + dd % 2) % 2, z)
        links.put(norm_in, norm.at[d], s_norm + dd, s_norm + dd, to)
    for dz in range(1, 4):
        links.put(bias_in, bias.at[z], s_bias + dz, s_bias + dz, place(y, x, c, (z + dz) % 4))
    links.put(mask_in, mask.at[c], s_mask, s_mask, to_c)
    own_small = (local(2, norm_in, norm.at[d]), local(3, bias_in, bias.at[z]), local(4, mask_in, mask.at[c]))
    for one in own_small:
        one.start()

    def move_tokens(key, source, target_at, at):
        base = links.base(key, 4)
        target = target_at(z // 2)
        stay = c == z // 2
        rows = at_rows((z % 2) * Q, Q, 16)
        for i in range(2):
            here = jnp.logical_and(stay, z % 2 == i)
            to = place(y, x, z // 2, 2 * c + i)
            to = (jnp.where(here, place(y, x, 1 - c, z)[0], to[0]), to[1])
            links.put(source.at[i], target.at[rows], base + i, base + 2 + z % 2, to, jnp.logical_not(here))

            @pl.when(here)
            def _(i=i):
                local(at, source.at[i], target.at[rows]).start()

    def wait_tokens(key, source, target_at, at):
        base = links.base(key, 4)
        target = target_at(c)
        stay = c == z // 2
        for j in range(2):
            here = jnp.logical_and(stay, z % 2 == j)

            @pl.when(here)
            def _(j=j):
                local(at, source.at[j], target.at[pl.ds(j * Q, Q)]).wait()

            @pl.when(jnp.logical_not(here))
            def _(j=j):
                links.wait(target.at[pl.ds(j * Q, Q)], base + 2 + j, to_c)

    move_tokens("tok", tok_in, lambda cc: tok, 5)

    up_shard = lambda sx, sc: up.at[at_rows(y * 512 + sx * 256 + sc * 128, 128, 128), at_rows(z * 256, 256, 128)]
    down_shard = lambda sx, sc: down.at[at_rows(z * 256, 256, 128), at_rows(y * 512 + sx * 256 + sc * 128, 128, 128)]
    s_up, s_down = links.base("up", 4), links.base("down", 4)
    q = 2 * x + c
    for dx, dc in ((1, 0), (1, 1), (0, 1)):
        tx, tc = (x + dx) % 2, (c + dc) % 2
        to, rel = place(y, tx, tc, z), 2 * dx + dc
        links.put(w1_in.at[:, at_rows((2 * tx + tc) * 256, 256, 128)], up_shard(x, c), s_up + rel, s_up + rel, to)
        links.put(w2_in.at[at_rows((2 * tx + tc) * 256, 256, 128), :], down_shard(x, c), s_down + rel, s_down + rel, to)
    own_up = local(6, w1_in.at[:, at_rows(q * 256, 256, 128)], up_shard(x, c))
    own_down = local(7, w2_in.at[at_rows(q * 256, 256, 128), :], down_shard(x, c))
    own_up.start()
    own_down.start()

    class Line:
        def __init__(self, key, piece, arrived):
            self.piece, self.arrived = piece, arrived
            self.many = many = len(piece(0))
            self.got = [links.base((key, "got", n), 4) for n in range(many)]
            self.up = [links.base((key, "up", n), 4) for n in range(many)]
            self.down = [links.base((key, "down", n), 4) for n in range(many)]

        def push(self, way_up, far):
            def make(n):
                o, there = self.origin(way_up, far)
                ref = self.piece(o)[n]
                sent = (self.up if way_up else self.down)[n] + o
                onward = z < 3 if way_up else z > 0
                when = onward if there is None else jnp.logical_and(there, onward)
                return ref, ref, sent, self.got[n] + o, up_z if way_up else down_z, when

            for n in range(self.many):
                links.start(functools.partial(make, n))

        def origin(self, way_up, far):
            if far == 0:
                return z, None
            o = z - far if way_up else z + far
            return jnp.clip(o, 0, 3), (o >= 0 if way_up else o < 4)

        def begin(self):
            self.push(True, 0)
            self.push(False, 0)
            self.arrived(functools.partial(self.origin, True, 0))

        def step(self, far):
            for way_up in (True, False):
                o, there = self.origin(way_up, far)

                @pl.when(there)
                def _():
                    for n, ref in enumerate(self.piece(o)):
                        links.wait(ref, self.got[n] + o, up_z)

                self.push(way_up, far)
                self.arrived(functools.partial(self.origin, way_up, far))

    s_first = [links.base(("first", n), 4) for n in range(2)]
    s_own = [links.base(("own", n), 4) for n in range(2)]
    s_fwd = [links.base(("fwd", n), 4) for n in range(2)]

    def neighbours(o):
        odd = o % 2
        even = 1 - odd
        y1, x1 = y + odd * (1 - 2 * y), x + even * (1 - 2 * x)
        y2, x2 = y + even * (1 - 2 * y), x + odd * (1 - 2 * x)
        return (y1, x1), (y2, x2)

    def attn_arrived(origin):
        o, there = origin()
        (y1, x1), (y2, x2) = neighbours(o)
        for n, ref in enumerate((qkv_at(r, o), wo_at(r, o))):
            links.put(ref, ref, s_first[n] + o, s_first[n] + o, place(y1, x1, c, z), there)
            links.put(ref, ref, s_own[n] + o, s_own[n] + o, place(y2, x2, c, z), there)

    def attn_forward(o, there):
        (y1, x1), (y2, x2) = neighbours(o)
        r1 = 2 * y1 + x1
        for n, ref in enumerate((qkv_at(r1, o), wo_at(r1, o))):
            def arrive(n=n, ref=ref):
                links.wait(ref, s_first[n] + o, to_x)

            arrive() if there is None else pl.when(there)(arrive)

            links.put(ref, ref, s_fwd[n] + o, s_fwd[n] + o, place(y2, x2, c, z), there)

    def attn_finish():
        for o in range(4):
            (y1, x1), (y2, x2) = neighbours(o)
            for n, at in enumerate((qkv_at, wo_at)):
                links.wait(at(2 * y2 + x2, o), s_own[n] + o, to_x)
                links.wait(at(2 * (1 - y) + 1 - x, o), s_fwd[n] + o, to_x)

    attn_line = Line("attn", lambda o: (qkv_at(r, o), wo_at(r, o)), attn_arrived)
    up_at = lambda yy, o: up.at[at_rows(yy * 512, 512, 512), at_rows(o * 256, 256, 256)]
    down_at = lambda yy, o: down.at[at_rows(o * 256, 256, 256), at_rows(yy * 512, 512, 512)]
    s_upy, s_downy = links.base("upy", 4), links.base("downy", 4)

    def across(at, base):
        def arrived(origin):
            def make():
                o, there = origin()
                return at(y, o), at(y, o), base + o, base + o, to_y, there

            links.start(make)

        return arrived

    up_line = Line("upl", lambda o: (up_at(y, o),), across(up_at, s_upy))
    down_line = Line("downl", lambda o: (down_at(y, o),), across(down_at, s_downy))

    lse[...] = jnp.zeros_like(lse)
    own_qkv.wait()
    own_wo.wait()
    links.wait(qkv_other, s_pc, to_c)
    links.wait(wo_other, s_pc + 1, to_c)
    attn_line.begin()
    for one in own_small:
        one.wait()
    for dd in range(1, 8):
        source = 4 * ((y + dd // 4) % 2) + 2 * ((x + (dd // 2) % 2) % 2) + (c + dd % 2) % 2
        links.wait(norm.at[source], s_norm + dd, to_c)
    for dz in range(1, 4):
        links.wait(bias.at[(z + 4 - dz) % 4], s_bias + dz, to_c)
    links.wait(mask.at[1 - c], s_mask, to_c)
    for dd in range(8):
        norm_row[:, dd * 128 : dd * 128 + 128] = norm[dd]
    for zz in range(4):
        qkv_row[:, zz * 384 : zz * 384 + 128] = bias[zz, 0:1]
        qkv_row[:, zz * 384 + 128 : zz * 384 + 256] = jnp.zeros((1, 128), F32)
        qkv_row[:, zz * 384 + 256 : zz * 384 + 384] = bias[zz, 1:2]
        up_row[:, zz * 256 : zz * 256 + 128] = bias[zz, 2:3]
        up_row[:, zz * 256 + 128 : zz * 256 + 256] = bias[zz, 3:4]

    own_up.wait()
    own_down.wait()
    attn_line.step(1)
    attn_forward(z, None)

    wait_tokens("tok", tok_in, lambda cc: tok, 5)

    @pl.loop(0, HALF // 32)
    def _(i):
        v = tok[at_rows(i * 32, 32, 32), :].astype(F32)
        unit, _ = unit_rows(v)
        n1[at_rows(c * HALF + i * 32, 32, 32), :] = (unit * norm_row[0:1] + norm_row[2:3]).astype(BF)

    s_n1 = links.base("n1", 1)
    half_at = lambda ref, cc: ref.at[at_rows(cc * HALF, HALF, 64), :]
    links.put(half_at(n1, c), half_at(n1, c), s_n1, s_n1, to_c)

    def forward_far(far):
        attn_forward(jnp.clip(z - far, 0, 3), z >= far)
        attn_forward(jnp.clip(z + far, 0, 3), z + far < 4)

    attn_line.step(2)
    forward_far(1)
    attn_line.step(3)
    for dx, dc in ((1, 0), (1, 1), (0, 1)):
        rel, sx, sc = 2 * dx + dc, (x + dx) % 2, (c + dc) % 2
        links.wait(up_shard(sx, sc), s_up + rel, to_c)
    up_line.begin()
    forward_far(2)
    move_tokens("cot", cot_in, lambda cc: block_at(cot, 2 * x + cc), 8)
    for dx, dc in ((1, 0), (1, 1), (0, 1)):
        rel, sx, sc = 2 * dx + dc, (x + dx) % 2, (c + dc) % 2
        links.wait(down_shard(sx, sc), s_down + rel, to_c)
    up_line.step(1)
    forward_far(3)
    down_line.begin()
    links.wait(half_at(n1, 1 - c), s_n1, to_c)
    attn_finish()

    @pl.loop(0, 6)
    def _(j):
        columns = at_rows(j * 256, 256, 256)
        proj[:, columns] = (mm(n1[...], qkv[:, columns], NN) + qkv_row[:, columns]).astype(BF)

    lane = lax.broadcasted_iota(jnp.int32, (1, 128), 1)
    first_head = lane < 64
    zero = jnp.zeros((), BF)
    up_line.step(2)

    @pl.loop(0, 4)
    def _(zz):
        keys = proj[:, at_rows(zz * 384 + 128, 128, 128)]
        values = proj[:, at_rows(zz * 384 + 256, 128, 128)]
        hidden_key = mask[z // 2, z % 2]
        for rb in range(2):
            rows = pl.ds(rb * HALF, HALF)
            pair = proj[rows, at_rows(zz * 384, 128, 128)]
            outs = []
            for hh in range(2):
                own = jnp.where(first_head if hh == 0 else jnp.logical_not(first_head), pair, zero)
                scores = mm(own, keys, NT) * (HD ** (-0.5)) + hidden_key
                highest = jnp.max(scores, axis=-1, keepdims=True)
                exponent = jnp.exp(scores - highest)
                total = jnp.sum(exponent, axis=-1, keepdims=True)
                low = (exponent * (1.0 / total)).astype(BF)
                head = 2 * zz + hh
                lse[rows, :] = jnp.where(lane == head, highest + jnp.log(total), lse[rows, :])
                outs.append(mm(low, values, NN))
            mix[rows, at_rows(zz * 128, 128, 128)] = jnp.where(first_head, outs[0], outs[1]).astype(BF)

        @pl.when(zz == 0)
        def _():
            down_line.step(1)

        @pl.when(zz == 1)
        def _():
            up_line.step(3)

        @pl.when(zz == 2)
        def _():
            down_line.step(2)

    down_line.step(3)

    s_part = links.base("part", 1)

    def project_out(cc, target):
        @pl.loop(0, 4)
        def _(j):
            columns = at_rows(j * 256, 256, 256)
            target[:, columns] = mm(mix[at_rows(cc * HALF, HALF, 64), :], wo[:, columns], NN)

    project_out(1 - c, part)
    links.put(part, got_part, s_part, s_part, to_c)
    project_out(c, hid)
    links.wait(got_part, s_part, to_c)

    @pl.loop(0, HALF // 32)
    def _(i):
        rows = at_rows(i * 32, 32, 32)
        v = hid[rows, :] + got_part[rows, :] + tok[rows, :].astype(F32) + norm_row[4:5]
        hid[rows, :] = v
        unit, _ = unit_rows(v)
        n2[block_rows(q, i * 32, 32), :] = (unit * norm_row[1:2] + norm_row[3:4]).astype(BF)

    def spread_start(key, ref):
        base = links.base(("spread", key), 3)
        links.put(block_at(ref, q), block_at(ref, q), base, base, to_x)
        links.put(block_at(ref, q), block_at(ref, q), base + 1, base + 1, to_c)

    def spread_forward(key, ref):
        base = links.base(("spread", key), 3)
        far = block_at(ref, 2 * (1 - x) + c)
        links.wait(far, base, to_x)
        links.put(far, far, base + 2, base + 2, to_c)

    def spread_wait_near(key, ref):
        links.wait(block_at(ref, 2 * x + 1 - c), links.base(("spread", key), 3) + 1, to_c)

    def spread_wait_far(key, ref):
        links.wait(block_at(ref, 2 * (1 - x) + 1 - c), links.base(("spread", key), 3) + 2, to_c)

    spread_start("n2", n2)
    wait_tokens("cot", cot_in, lambda cc: block_at(cot, 2 * x + cc), 8)
    spread_start("cot", cot)
    for o in range(4):
        links.wait(up_at(1 - y, o), s_upy + o, to_y)

    def expand(t):
        @pl.loop(0, 4)
        def _(j):
            columns = at_rows(j * 256, 256, 256)
            for rb in range(2):
                rows = block_rows(t, rb * Q, Q)
                v = mm(n2[rows, :], up[:, columns], NN) + up_row[:, columns]
                value, grade = gelu_both(v)
                act[rows, columns] = value.astype(BF)
                slope[rows, columns] = grade.astype(BF)

    expand(q)
    spread_wait_near("n2", n2)
    expand(2 * x + 1 - c)
    spread_forward("n2", n2)
    expand(2 * (1 - x) + c)
    spread_wait_far("n2", n2)
    expand(2 * (1 - x) + 1 - c)
    spread_wait_near("cot", cot)
    spread_forward("cot", cot)
    spread_wait_far("cot", cot)
    for o in range(4):
        links.wait(down_at(1 - y, o), s_downy + o, to_y)

    near_other, far_own, far_other = 2 * x + 1 - c, 2 * (1 - x) + c, 2 * (1 - x) + 1 - c
    sums[...] = jnp.zeros_like(sums)
    gb1[...] = jnp.zeros_like(gb1)

    def fold(v):
        return v[0:8] + v[8:16] + v[16:24] + v[24:32]

    def tally(row, v):
        sums[row * 8 : row * 8 + 8, :] += fold(v)

    def send_later(make):
        links.start(make)

    def through_slope(t):
        @pl.loop(0, 4)
        def _(j):
            columns = at_rows(j * 256, 256, 256)
            rows = block_rows(t, 0, HALF)
            v = mm(cot[rows, :], down[columns, :], NT) * slope[rows, columns].astype(F32)
            gb1[:, columns] += jnp.sum(v.reshape(HALF // 8, 8, 256), axis=0)
            slope[rows, columns] = v.astype(BF)

    def back_part(t, target):
        @pl.loop(0, 4)
        def _(j):
            columns = at_rows(j * 256, 256, 256)
            target[:, columns] = mm(slope[block_rows(t, 0, HALF), :], up[columns, :], NT).astype(target.dtype)

    def add_rows(target, *sources):
        @pl.loop(0, HALF // 32)
        def _(i):
            rows = at_rows(i * 32, 32, 32)
            total = sources[0][rows, :].astype(F32)
            for source in sources[1:]:
                total = total + source[rows, :].astype(F32)
            target[rows, :] = total.astype(target.dtype)

    s_gfar, s_gmid, s_gnear = links.base("gfar", 1), links.base("gmid", 1), links.base("gnear", 1)
    s_bfar, s_bmid, s_bnear = links.base("bfar", 1), links.base("bmid", 1), links.base("bnear", 1)
    through_slope(far_other)
    back_part(far_other, s_far)
    links.put(s_far, g_far, s_gfar, s_gfar, to_c)
    through_slope(far_own)
    links.copy(part, got_part, s_part, s_part, to_c).wait_send()
    links.drop(s_part)
    back_part(far_own, part)
    links.wait(g_far, s_gfar, to_c)
    add_rows(s_mid, part, g_far)
    links.put(s_mid, g_mid, s_gmid, s_gmid, to_x)
    through_slope(near_other)
    back_part(near_other, s_near)
    links.put(s_near, g_near, s_gnear, s_gnear, to_c)
    through_slope(q)
    back_part(q, part)

    s_rdown, s_rup = links.base("rdown", 4), links.base("rup", 4)
    d_down_at = lambda yy, o: d_down.at[at_rows(o * 256, 256, 256), at_rows(yy * 512, 512, 512)]
    d_up_at = lambda yy, o: d_up.at[at_rows(yy * 512, 512, 512), at_rows(o * 256, 256, 256)]
    r_down_at = lambda o: r_down.at[at_rows(o * 256, 256, 256), :]
    r_up_at = lambda o: r_up.at[:, at_rows(o * 256, 256, 256)]

    def make_rdown(k):
        o = (z + 1 + k) % 4
        return d_down_at(1 - y, o), r_down_at(o), s_rdown + o, s_rdown + o, to_y, None

    def make_rup(k):
        o = (z + 1 + k) % 4
        return d_up_at(1 - y, o), r_up_at(o), s_rup + o, s_rup + o, to_y, None

    for k in range(4):
        rows = at_rows(((z + 1 + k) % 4) * 256, 256, 256)
        d_down[rows, :] = mm(act[:, rows], cot[...], TN).astype(BF)
        links.start(functools.partial(make_rdown, k))
    for k in range(4):
        columns = at_rows(((z + 1 + k) % 4) * 256, 256, 256)
        d_up[:, columns] = mm(n2[...], slope[:, columns], TN).astype(BF)
        links.start(functools.partial(make_rup, k))

    links.wait(g_near, s_gnear, to_c)
    links.wait(g_mid, s_gmid, to_x)

    @pl.loop(0, HALF // 32)
    def _(i):
        rows = at_rows(i * 32, 32, 32)
        grad = part[rows, :] + g_near[rows, :].astype(F32) + g_mid[rows, :].astype(F32)
        unit, scale = unit_rows(hid[rows, :])
        out = cot[block_rows(q, i * 32, 32), :].astype(F32)
        scaled = grad * norm_row[1:2]
        moved = scale * (
            scaled
            - jnp.mean(scaled, axis=-1, keepdims=True)
            - unit * jnp.mean(scaled * unit, axis=-1, keepdims=True)
        )
        total = out + moved
        tally(1, grad * unit)
        tally(3, grad)
        tally(4, total)
        tally(5, out)
        got_part[rows, :] = total
        ga[at_rows(c * HALF + i * 32, 32, 32), :] = total.astype(BF)

    s_ga = links.base("ga", 1)
    links.put(half_at(ga, c), half_at(ga, c), s_ga, s_ga, to_c)

    def down_part(t, target, base=None):
        @pl.loop(0, 4)
        def _(j):
            columns = at_rows(j * 256, 256, 256)
            v = mm(act[block_rows(t, 0, HALF), :], down[:, columns], NN)
            target[:, columns] = (v if base is None else v + base[:, columns]).astype(target.dtype)

    links.copy(s_far, g_far, s_gfar, s_gfar, to_c).wait_send()
    links.copy(s_mid, g_mid, s_gmid, s_gmid, to_x).wait_send()
    links.copy(s_near, g_near, s_gnear, s_gnear, to_c).wait_send()
    links.drop(s_gfar, s_gmid, s_gnear)
    down_part(far_other, s_far)
    links.put(s_far, b_far, s_bfar, s_bfar, to_c)

    links.wait(half_at(ga, 1 - c), s_ga, to_c)

    @pl.loop(0, 2)
    def _(j):
        columns = at_rows(j * 256, 256, 256)
        gmix[:, columns] = mm(ga[...], wo[columns, :], NT).astype(BF)

    @pl.loop(0, 2)
    def _(j):
        columns = at_rows(j * 256, 256, 256)
        d_wo[columns, :] = mm(mix[:, columns], ga[...], TN).astype(BF)

    d_qkv_at = lambda rr, o: d_qkv.at[at_rows(rr * 256, 256, 256), at_rows(o * 384, 384, 128)]
    d_wo_at = lambda rr, o: d_wo.at[at_rows(o * 128, 128, 128), at_rows(rr * 256, 256, 128)]

    def accumulate(target, *sources):
        count = target.shape[0] // 64

        @pl.loop(0, count)
        def _(i):
            rows = at_rows(i * 64, 64, 64)
            total = target[rows, :].astype(F32)
            for source in sources:
                total = total + source[rows, :].astype(F32)
            target[rows, :] = total.astype(target.dtype)

    class Reduce:
        def __init__(self, key, at, first, second, over_z, final):
            self.at, self.first, self.second, self.over_z, self.final = at, first, second, over_z, final
            self.s1 = [links.base((key, "first", i), 4) for i in range(2)]
            self.s2, self.sz = links.base((key, "second"), 4), links.base((key, "z"), 8)

        def begin(self, o):
            def make(i):
                (y1, x1), (y2, x2) = neighbours(o)
                rr = 2 * y1 + x1 if i == 0 else 3 - r
                return self.at(rr, o), self.first.at[i, o], self.s1[i] + o, self.s1[i] + o, place(y1, x1, c, z), None

            for i in (1, 0):
                links.start(functools.partial(make, i))

        def middle(self, o):
            (y1, x1), (y2, x2) = neighbours(o)
            links.wait(self.first.at[1, o], self.s1[1] + o, to_x)
            accumulate(self.at(2 * y2 + x2, o), self.first.at[1, o])

            def make():
                (y1, x1), (y2, x2) = neighbours(o)
                return self.at(2 * y2 + x2, o), self.second.at[o], self.s2 + o, self.s2 + o, place(y2, x2, c, z), None

            links.start(make)

        def gather(self, k):
            o = (z + 1 + k) % 4
            links.wait(self.first.at[0, o], self.s1[0] + o, to_x)
            links.wait(self.second.at[o], self.s2 + o, to_x)
            accumulate(self.at(r, o), self.first.at[0, o], self.second.at[o])
            if k < 3:
                push_z(self, k, lambda o: self.at(r, o))

        def last(self):
            finish_z(self, self.at(r, z))

    def push_z(owner, k, at):
        def make():
            o = (z + 1 + k) % 4
            return at(o), owner.over_z.at[z], owner.sz + k, owner.sz + 4 + z, place(y, x, c, o), None

        links.start(make)

    def finish_z(owner, own):
        for k in range(3):
            source = (z + 1 + k) % 4
            links.wait(owner.over_z.at[source], owner.sz + 4 + source, up_z_other)
        others = [owner.over_z.at[(z + 1 + k) % 4] for k in range(3)]
        count = own.shape[0] // 64

        @pl.loop(0, count)
        def _(i):
            rows = at_rows(i * 64, 64, 64)
            total = own[rows, :].astype(F32)
            for other in others:
                total = total + other[rows, :].astype(F32)
            owner.final[rows, :] = total.astype(BF)

    up_z_other = to_c
    red_wo = Reduce("red_wo", d_wo_at, first_wo, second_wo, z_wo, f_wo)
    red_qkv = Reduce("red_qkv", d_qkv_at, first_qkv, second_qkv, z_qkv, f_qkv)
    for o in range(4):
        red_wo.begin(o)

    class Half:
        def __init__(self, key, at, got_at, s_got, over_z, final):
            self.at, self.got_at, self.s_got, self.over_z, self.final = at, got_at, s_got, over_z, final
            self.sz = links.base((key, "z"), 8)

        def gather(self, k):
            o = (z + 1 + k) % 4
            links.wait(self.got_at(o), self.s_got + o, to_y)
            accumulate(self.at(y, o), self.got_at(o))
            if k < 3:
                push_z(self, k, lambda o: self.at(y, o))

        def last(self):
            finish_z(self, self.at(y, z))

    half_down = Half("half_down", d_down_at, r_down_at, s_rdown, z_down, f_down)
    half_up = Half("half_up", d_up_at, r_up_at, s_rup, z_up, f_up)

    down_part(far_own, part)
    links.wait(b_far, s_bfar, to_c)
    add_rows(s_mid, part, b_far)
    links.put(s_mid, b_mid, s_bmid, s_bmid, to_x)
    down_part(near_other, s_near)
    links.put(s_near, b_near, s_bnear, s_bnear, to_c)
    down_part(q, hid, hid)

    @pl.loop(0, 4)
    def _(zz):
        base = zz * 384
        keys = proj[:, at_rows(base + 128, 128, 128)]
        values = proj[:, at_rows(base + 256, 128, 128)]
        hidden_key = mask[z // 2, z % 2]
        d_keys = d_values = None
        sum_queries = None
        for rb in range(2):
            rows = pl.ds(rb * HALF, HALF)
            pair = proj[rows, at_rows(base, 128, 128)]
            grads = gmix[rows, at_rows(zz * 128, 128, 128)]
            outs = []
            for hh in range(2):
                keep = first_head if hh == 0 else jnp.logical_not(first_head)
                own = jnp.where(keep, pair, zero)
                own_grad = jnp.where(keep, grads, zero)
                level = jnp.sum(jnp.where(lane == 2 * zz + hh, lse[rows, :], 0.0), axis=-1, keepdims=True)
                attention = jnp.exp(mm(own, keys, NT) * (HD ** (-0.5)) + hidden_key - level)
                grad_attention = mm(own_grad, values, NT)
                inner = jnp.sum(attention * grad_attention, axis=-1, keepdims=True)
                low = (attention * (grad_attention - inner)).astype(BF)
                more_values = mm(attention.astype(BF), own_grad, TN)
                more_keys = mm(low, own, TN)
                d_values = more_values if d_values is None else d_values + more_values
                d_keys = more_keys if d_keys is None else d_keys + more_keys
                outs.append(mm(low, keys, NN))
            d_queries = jnp.where(first_head, outs[0], outs[1]) * (HD ** (-0.5))
            total = jnp.sum(d_queries.reshape(HALF // 8, 8, 128), axis=0)
            sum_queries = total if sum_queries is None else sum_queries + total
            gproj[rows, at_rows(base, 128, 128)] = d_queries.astype(BF)
        gproj[:, at_rows(base + 128, 128, 128)] = (d_keys * (HD ** (-0.5))).astype(BF)
        gproj[:, at_rows(base + 256, 128, 128)] = d_values.astype(BF)
        gbq[:, at_rows(zz * 128, 128, 128)] = sum_queries
        gbv[:, at_rows(zz * 128, 128, 128)] = jnp.sum(d_values.reshape(FULL // 8, 8, 128), axis=0)

        @pl.when(zz == 0)
        def _():
            for o in range(4):
                red_wo.middle(o)

        @pl.when(zz == 1)
        def _():
            for k in range(4):
                half_down.gather(k)

        @pl.when(zz == 2)
        def _():
            for k in range(4):
                half_up.gather(k)

    links.wait(b_near, s_bnear, to_c)
    links.wait(b_mid, s_bmid, to_x)
    links.copy(s_far, b_far, s_bfar, s_bfar, to_c).wait_send()
    links.copy(s_near, b_near, s_bnear, s_bnear, to_c).wait_send()
    links.drop(s_bfar, s_bnear)

    @pl.loop(0, HALF // 32)
    def _(i):
        rows = at_rows(i * 32, 32, 32)
        total = hid[rows, :] + b_near[rows, :].astype(F32) + b_mid[rows, :].astype(F32) + norm_row[5:6]
        s_near[rows, :] = total.astype(BF)

    def send_home(key, source, target, at):
        base = links.base(key, 4)
        for j in range(2):
            def make(j=j):
                here = jnp.logical_and(z // 2 == c, z == 2 * c + j)
                to = place(y, x, z // 2, 2 * c + j)
                to = (jnp.where(here, place(y, x, 1 - c, z)[0], to[0]), to[1])
                return source.at[pl.ds(j * Q, Q)], target.at[z % 2], base + j, base + 2 + z % 2, to, jnp.logical_not(here)

            links.start(make)

            @pl.when(jnp.logical_and(z // 2 == c, z == 2 * c + j))
            def _(j=j):
                local(at, source.at[pl.ds(j * Q, Q)], target.at[z % 2]).start()

    def wait_home(key, source, target, at):
        base = links.base(key, 4)
        for i in range(2):
            here = jnp.logical_and(z // 2 == c, z % 2 == i)

            @pl.when(here)
            def _(i=i):
                local(at, source.at[pl.ds(0, Q)], target.at[i]).wait()

            @pl.when(jnp.logical_not(here))
            def _(i=i):
                links.wait(target.at[i], base + 2 + i, to_c)

    send_home("block", s_near, block_out, 9)

    def weigh(rr):
        d_qkv[at_rows(rr * 256, 256, 256), :] = mm(n1[:, at_rows(rr * 256, 256, 256)], gproj[...], TN).astype(BF)

    weigh(3 - r)
    weigh(2 * y + 1 - x)
    red_qkv.begin(0)
    red_qkv.begin(2)
    weigh(2 * (1 - y) + x)
    red_qkv.begin(1)
    red_qkv.begin(3)

    def front_part(cc, target):
        @pl.loop(0, 4)
        def _(j):
            columns = at_rows(j * 256, 256, 256)
            target[:, columns] = mm(gproj[at_rows(cc * HALF, HALF, 64), :], qkv[columns, :], NT).astype(target.dtype)

    s_gn1 = links.base("gn1", 1)
    front_part(1 - c, s_far)
    links.put(s_far, g_n1, s_gn1, s_gn1, to_c)
    weigh(r)
    front_part(c, part)
    links.wait(g_n1, s_gn1, to_c)
    links.copy(s_mid, b_mid, s_bmid, s_bmid, to_x).wait_send()
    links.drop(s_bmid)

    @pl.loop(0, HALF // 32)
    def _(i):
        rows = at_rows(i * 32, 32, 32)
        grad = part[rows, :] + g_n1[rows, :].astype(F32)
        unit, scale = unit_rows(tok[rows, :].astype(F32))
        scaled = grad * norm_row[0:1]
        moved = scale * (
            scaled
            - jnp.mean(scaled, axis=-1, keepdims=True)
            - unit * jnp.mean(scaled * unit, axis=-1, keepdims=True)
        )
        tally(0, grad * unit)
        tally(2, grad)
        s_mid[rows, :] = (got_part[rows, :] + moved).astype(BF)

    send_home("home", s_mid, grad_out, 10)

    for row in range(6):
        sums_row[row : row + 1, :] = jnp.sum(sums[row * 8 : row * 8 + 8, :], axis=0, keepdims=True)
    sums_row[6:8, :] = jnp.zeros((2, 1024), F32)
    for dd in range(8):
        norm[dd] = sums_row[:, dd * 128 : dd * 128 + 128]
    s_sum, s_sumz = links.base("sum", 8), links.base("sumz", 8)
    for dd in range(1, 8):
        def make(dd=dd):
            ty, tx, tc = (y + dd // 4) % 2, (x + (dd // 2) % 2) % 2, (c + dd % 2) % 2
            return norm.at[4 * ty + 2 * tx + tc], sums_got.at[dd], s_sum + dd, s_sum + dd, place(ty, tx, tc, z), None

        links.start(make)
    for zz in range(4):
        flat = lambda ref, start: jnp.sum(ref[:, start : start + 128], axis=0, keepdims=True)
        bias_pack[zz, 0:1] = flat(gbq, zz * 128)
        bias_pack[zz, 1:2] = flat(gbv, zz * 128)
        bias_pack[zz, 2:3] = flat(gb1, zz * 256)
        bias_pack[zz, 3:4] = flat(gb1, zz * 256 + 128)
        bias_pack[zz, 4:8] = jnp.zeros((4, 128), F32)
    s_bz, s_ball = links.base("bz", 4), links.base("ball", 8)
    for dz in range(1, 4):
        def make(dz=dz):
            tz = (z + dz) % 4
            return bias_pack.at[tz], bias_got.at[dz], s_bz + dz, s_bz + dz, place(y, x, c, tz), None

        links.start(make)

    for o in range(4):
        red_qkv.middle(o)
    for k in range(4):
        red_wo.gather(k)

    for dz in range(1, 4):
        links.wait(bias_got.at[dz], s_bz + dz, to_c)
    bias_all[d] = bias_pack[z] + bias_got[1] + bias_got[2] + bias_got[3]
    for dd in range(1, 8):
        def make(dd=dd):
            to = place((y + dd // 4) % 2, (x + (dd // 2) % 2) % 2, (c + dd % 2) % 2, z)
            return bias_all.at[d], bias_all.at[d], s_ball + dd, s_ball + dd, to, None

        links.start(make)
    for dd in range(1, 8):
        links.wait(sums_got.at[dd], s_sum + dd, to_c)
    total = norm[d]
    for dd in range(1, 8):
        total = total + sums_got[dd]
    sums_z[0] = total
    for dz in range(1, 4):
        def make(dz=dz):
            return sums_z.at[0], sums_z.at[dz], s_sumz + dz, s_sumz + dz, place(y, x, c, (z + dz) % 4), None

        links.start(make)

    half_down.last()
    half_up.last()
    s_oup, s_odown = links.base("oup", 4), links.base("odown", 4)
    for dx, dc in ((1, 0), (1, 1), (0, 1)):
        rel = 2 * dx + dc

        def make_up(dx=dx, dc=dc, rel=rel):
            tx, tc = (x + dx) % 2, (c + dc) % 2
            rows = at_rows((2 * tx + tc) * 128, 128, 128)
            return f_up.at[rows, :], o_up.at[q], s_oup + rel, s_oup + rel, place(y, tx, tc, z), None

        def make_down(dx=dx, dc=dc, rel=rel):
            tx, tc = (x + dx) % 2, (c + dc) % 2
            columns = at_rows((2 * tx + tc) * 128, 128, 128)
            return f_down.at[:, columns], o_down.at[q], s_odown + rel, s_odown + rel, place(y, tx, tc, z), None

        links.start(make_up)
        links.start(make_down)

    for k in range(4):
        red_qkv.gather(k)
    red_wo.last()

    w1_out[:, at_rows(q * 256, 256, 256)] = f_up[at_rows(q * 128, 128, 128), :].astype(F32)
    w2_out[at_rows(q * 256, 256, 256), :] = f_down[:, at_rows(q * 128, 128, 128)].astype(F32)
    for dx, dc in ((1, 0), (1, 1), (0, 1)):
        rel, source = 2 * dx + dc, 2 * ((x + dx) % 2) + (c + dc) % 2
        links.wait(o_up.at[source], s_oup + rel, to_c)
        links.wait(o_down.at[source], s_odown + rel, to_c)
        w1_out[:, at_rows(source * 256, 256, 256)] = o_up[source].astype(F32)
        w2_out[at_rows(source * 256, 256, 256), :] = o_down[source].astype(F32)

    for dd in range(1, 8):
        source = 4 * ((y + dd // 4) % 2) + 2 * ((x + (dd // 2) % 2) % 2) + (c + dd % 2) % 2
        links.wait(bias_all.at[source], s_ball + dd, to_c)
    for cc in range(2):
        together = bias_all[cc] + bias_all[2 + cc] + bias_all[4 + cc] + bias_all[6 + cc]
        qv_out[:, cc * 128 : cc * 128 + 128] = together[0:2]
    for qq in range(4):
        together = bias_all[qq] + bias_all[4 + qq]
        b1_out[qq * 2 : qq * 2 + 2, :] = together[2:4]
    for dz in range(1, 4):
        links.wait(sums_z.at[dz], s_sumz + dz, to_c)
    sums_out[...] = sums_z[0] + sums_z[1] + sums_z[2] + sums_z[3]

    red_qkv.last()
    s_oqkv, s_owo = links.base("oqkv", 1), links.base("owo", 1)
    links.put(f_qkv.at[at_rows((1 - c) * 128, 128, 128), :], o_qkv, s_oqkv, s_oqkv, to_c)
    links.put(f_wo.at[:, at_rows((1 - c) * 128, 128, 128)], o_wo, s_owo, s_owo, to_c)
    qkv_out[:, at_rows(c * 384, 384, 128)] = f_qkv[at_rows(c * 128, 128, 128), :].astype(F32)
    wo_out[at_rows(c * 128, 128, 128), :] = f_wo[:, at_rows(c * 128, 128, 128)].astype(F32)
    links.wait(o_qkv, s_oqkv, to_c)
    links.wait(o_wo, s_owo, to_c)
    qkv_out[:, at_rows((1 - c) * 384, 384, 128)] = o_qkv[...].astype(F32)
    wo_out[at_rows((1 - c) * 128, 128, 128), :] = o_wo[...].astype(F32)
    wait_home("block", s_near, block_out, 9)
    wait_home("home", s_mid, grad_out, 10)
    links.finish()


def prepare(inputs, valid_mask, cotangent, ln_gain, d_bias, w_qkv, b_qv, b_1):
    y, x, c, z = where_am_i()
    rows = inputs.shape[0]
    turn = lambda v: jnp.pad(jnp.transpose(v, (1, 0, 2)), ((0, 0), (0, Q - rows), (0, 0)))
    mask = jnp.where(valid_mask.reshape(2, 4, rows) > 0, 0.0, MASKED).astype(F32)
    mask = jnp.pad(mask, ((0, 0), (0, 0), (0, Q - rows)), constant_values=MASKED).reshape(2, 1, FULL)
    norm = jnp.pad(jnp.concatenate([ln_gain, d_bias]).astype(F32), ((0, 2), (0, 0)))
    bias = jnp.concatenate(
        [
            lax.dynamic_slice(b_qv, (0, c * 128), (2, 128)),
            lax.dynamic_slice(b_1, ((2 * x + c) * 256,), (256,)).reshape(2, 128),
        ]
    ).astype(F32)
    bias = jnp.pad(bias, ((0, 4), (0, 0)))
    qkv = jnp.transpose(w_qkv.reshape(128, 3, 2, 128), (0, 2, 1, 3)).reshape(128, 768)
    return turn(inputs), turn(cotangent), mask, norm, bias, qkv


def layer_call(*operands):
    shape = jax.ShapeDtypeStruct
    hbm, vmem = pl.BlockSpec(memory_space=pl.ANY), pl.BlockSpec(memory_space=pltpu.VMEM)
    outs = [
        shape((2, Q, 1024), BF), shape((2, Q, 1024), BF), shape((8, 128), F32), shape((2, 256), F32),
        shape((8, 128), F32), shape((128, 768), F32), shape((256, 128), F32), shape((128, 1024), F32),
        shape((1024, 128), F32),
    ]
    low = lambda *dims: pltpu.VMEM(dims, BF)
    wide = lambda *dims: pltpu.VMEM(dims, F32)
    scratch = [
        low(HALF, 1024), low(4 * HALF, 1024), wide(2, 2, 1, FULL), wide(8, 8, 128), wide(4, 8, 128),
        low(1024, 1536), low(512, 1024), low(1024, 1024), low(1024, 1024),
        low(FULL, 1024), low(FULL, 1536), wide(FULL, 128), low(FULL, 512), wide(HALF, 1024),
        low(4 * HALF, 1024), low(4 * HALF, 1024), low(4 * HALF, 1024),
        wide(8, 1024), wide(1, 1536), wide(1, 1024), wide(HALF, 1024), wide(HALF, 1024),
        low(FULL, 1024), low(FULL, 512), low(FULL, 1536),
        low(1024, 1024), low(1024, 1024), low(1024, 1536), low(512, 1024),
        low(512, 1024), low(1024, 512), low(4, 512, 256), low(4, 256, 512),
        low(512, 256), low(256, 512), low(4, 128, 256), low(4, 256, 128),
        low(2, 4, 256, 384), low(2, 4, 128, 256), low(4, 256, 384), low(4, 128, 256),
        low(4, 256, 384), low(4, 128, 256), low(256, 384), low(128, 256), low(128, 384), low(128, 128),
        *[low(HALF, 1024)] * 10,
        wide(48, 1024), wide(8, 1024), wide(8, 8, 128), wide(4, 8, 128),
        wide(8, 1024), wide(8, 512), wide(8, 512), wide(4, 8, 128), wide(4, 8, 128), wide(8, 8, 128),
        pltpu.SemaphoreType.DMA((16,)), pltpu.SemaphoreType.DMA((320,)), pltpu.SemaphoreType.DMA((320,)),
    ]
    return pl.pallas_call(
        layer_kernel,
        out_shape=outs,
        in_specs=[hbm] * 9,
        out_specs=[hbm, hbm] + [vmem] * 7,
        scratch_shapes=scratch,
        compiler_params=pltpu.CompilerParams(collective_id=0, has_side_effects=True, vmem_limit_bytes=67043328),
        name="layer",
    )(*operands)


def fast_body(inputs, valid_mask, cotangent, ln_gain, d_bias, w_qkv, b_qv, w_o, w_1, b_1, w_2):
    rows = inputs.shape[0]
    block, grad, sums, qv, b1, qkv, wo, w1, w2 = layer_call(
        *prepare(inputs, valid_mask, cotangent, ln_gain, d_bias, w_qkv, b_qv, b_1), w_o, w_1, w_2
    )
    back = lambda v: jnp.transpose(v[:, :rows], (1, 0, 2))
    w_qkv_grad = jnp.transpose(qkv.reshape(128, 2, 3, 128), (0, 2, 1, 3)).reshape(128, 3, 256)
    return (
        back(block), back(grad).astype(F32), sums[:2], sums[2:6], w_qkv_grad, qv, wo, w1, b1.reshape(1024), w2,
    )


def solution(mesh):
    in_specs = (
        P("tensor", "dp", None),
        P("dp", None),
        P("tensor", "dp", None),
        P(None, "dp"),
        P(None, "dp"),
        P("dp", None, "tensor"),
        P(None, "tensor"),
        P("tensor", "dp"),
        P("dp", "tensor"),
        P("tensor"),
        P("tensor", "dp"),
    )
    out_specs = (
        P("tensor", "dp", None),
        P("tensor", "dp", None),
        P(None, "dp"),
        P(None, "dp"),
        P("dp", None, "tensor"),
        P(None, "tensor"),
        P("tensor", "dp"),
        P("dp", "tensor"),
        P("tensor"),
        P("tensor", "dp"),
    )
    run = fast_body if dict(mesh.shape) == {"dp": 8, "tensor": 4} else body
    return jax.shard_map(run, mesh=mesh, in_specs=in_specs, out_specs=out_specs, check_vma=False)
```

```python
import functools

import jax
import jax.numpy as jnp
from jax import lax
from jax.experimental import pallas as pl
from jax.experimental.pallas import tpu as pltpu
from jax.sharding import PartitionSpec as P

HD = 64


EPSILON = 1e-06
MASKED = -1e30


def layer_norm(values, gain, shift):
    average = jnp.mean(values, axis=-1, keepdims=True)
    centred = values - average
    variance = jnp.mean(centred * centred, axis=-1, keepdims=True)
    return centred * lax.rsqrt(variance + EPSILON) * gain + shift


def gelu_exact(values):
    return jax.nn.gelu(values, approximate=False)


def gather_layer(ln_gain, d_bias, w_qkv, w_o, w_1, w_2):
    return (
        lax.all_gather(ln_gain, "dp", axis=1, tiled=True),
        lax.all_gather(d_bias, "dp", axis=1, tiled=True),
        lax.all_gather(w_qkv, "dp", axis=0, tiled=True),
        lax.all_gather(w_o, "dp", axis=1, tiled=True),
        lax.all_gather(w_1, "dp", axis=0, tiled=True),
        lax.all_gather(w_2, "dp", axis=1, tiled=True),
    )


def masked_scores(queries, keys_part, valid):
    scores = jnp.einsum(
        "qhd,khd->hqk", queries, keys_part, preferred_element_type=jnp.float32
    ) * HD ** (-0.5)
    return jnp.where(valid[None, None, :] > 0, scores, MASKED)


def attend_forward(bundle):
    packed, valid = bundle
    scores = masked_scores(packed[:, 0], packed[:, 1], valid)
    highest = jnp.max(scores, axis=-1, keepdims=True)
    exponent = jnp.exp(scores - highest)
    denominator = jnp.sum(exponent, axis=-1, keepdims=True)
    attention = (exponent / denominator).astype(jnp.bfloat16)
    mixture = jnp.einsum(
        "hqk,khd->qhd", attention, packed[:, 2], preferred_element_type=jnp.float32
    )
    return (mixture.astype(jnp.bfloat16), (highest + jnp.log(denominator))[..., 0])


def attend_backward(bundle):
    packed, grad_mixture, log_total, valid = bundle
    queries = packed[:, 0]
    keys_part = packed[:, 1]
    values_part = packed[:, 2]
    scores = masked_scores(queries, keys_part, valid)
    attention = jnp.exp(scores - log_total[..., None])
    attention_low = attention.astype(jnp.bfloat16)
    grad_values = jnp.einsum(
        "hqk,qhd->khd", attention_low, grad_mixture, preferred_element_type=jnp.float32
    )
    grad_attention = jnp.einsum(
        "qhd,khd->hqk", grad_mixture, values_part, preferred_element_type=jnp.float32
    )
    inner = jnp.sum(attention * grad_attention, axis=-1, keepdims=True)
    grad_scores = (attention * (grad_attention - inner)).astype(jnp.bfloat16)
    factor = HD ** (-0.5)
    grad_queries = (
        jnp.einsum("hqk,khd->qhd", grad_scores, keys_part, preferred_element_type=jnp.float32)
        * factor
    )
    grad_keys = (
        jnp.einsum("hqk,qhd->khd", grad_scores, queries, preferred_element_type=jnp.float32)
        * factor
    )
    return jnp.stack([grad_queries, grad_keys, grad_values], axis=1)


def body(inputs, valid_mask, cotangent, ln_gain, d_bias, w_qkv, b_qv, w_o, w_1, b_1, w_2):
    local_rows, images, model_width = inputs.shape
    layer = gather_layer(ln_gain, d_bias, w_qkv, w_o, w_1, w_2)
    gains = layer[0].astype(jnp.float32)
    shifts = layer[1].astype(jnp.float32)
    wide_qkv = layer[2].reshape(model_width, -1)
    wide_out = layer[3]
    wide_up = layer[4]
    wide_down = layer[5]
    residual = inputs.astype(jnp.float32)
    normed1 = layer_norm(residual, gains[0], shifts[0]).astype(jnp.bfloat16)
    gathered1 = lax.all_gather(normed1, "tensor", axis=0, tiled=True)
    full_length = gathered1.shape[0]
    columns = b_qv.shape[1]
    heads_local = columns // HD
    projected = jnp.dot(gathered1, wide_qkv, preferred_element_type=jnp.float32).reshape(
        full_length, images, 3, columns
    )
    qkv_bias = jnp.stack([b_qv[0], jnp.zeros_like(b_qv[0]), b_qv[1]]).astype(jnp.float32)
    projected_low = (projected + qkv_bias).astype(jnp.bfloat16)
    per_image = jnp.transpose(projected_low, (1, 0, 2, 3)).reshape(
        images, full_length, 3, heads_local, HD
    )
    mixture, log_total = lax.map(attend_forward, (per_image, valid_mask))
    mixture_seq = jnp.transpose(mixture, (1, 0, 2, 3)).reshape(full_length, images, columns)
    segment = mixture_seq
    attn_sum = lax.psum_scatter(
        jnp.dot(segment, wide_out, preferred_element_type=jnp.float32),
        "tensor",
        scatter_dimension=0,
        tiled=True,
    )
    hidden1 = residual + attn_sum + shifts[2]
    normed2 = layer_norm(hidden1, gains[1], shifts[1]).astype(jnp.bfloat16)
    gathered2 = lax.all_gather(normed2, "tensor", axis=0, tiled=True)
    hidden_in = jnp.dot(gathered2, wide_up, preferred_element_type=jnp.float32) + b_1.astype(
        jnp.float32
    )
    active = gelu_exact(hidden_in).astype(jnp.bfloat16)
    segment = active
    branch_sum = lax.psum_scatter(
        jnp.dot(segment, wide_down, preferred_element_type=jnp.float32).astype(jnp.bfloat16),
        "tensor",
        scatter_dimension=0,
        tiled=True,
    ).astype(jnp.float32)
    block_output = (hidden1 + branch_sum + shifts[3]).astype(jnp.bfloat16)
    layer = gather_layer(ln_gain, d_bias, w_qkv, w_o, w_1, w_2)
    wide_qkv = layer[2].reshape(model_width, -1)
    wide_out = layer[3]
    wide_up = layer[4]
    wide_down = layer[5]
    grad_out = cotangent.astype(jnp.float32)
    grad_gathered = lax.all_gather(cotangent, "tensor", axis=0, tiled=True)
    grad_w_2 = jnp.einsum("sif,sid->fd", active, grad_gathered, preferred_element_type=jnp.float32)
    grad_active = jnp.einsum(
        "sid,fd->sif", grad_gathered, wide_down, preferred_element_type=jnp.float32
    )
    grad_hidden_in = jax.vjp(gelu_exact, hidden_in)[1](grad_active)[0]
    grad_b_1 = jnp.sum(grad_hidden_in, axis=(0, 1))
    grad_hidden_low = grad_hidden_in.astype(jnp.bfloat16)
    grad_w_1 = jnp.einsum(
        "sid,sif->df", gathered2, grad_hidden_low, preferred_element_type=jnp.float32
    )
    segment = grad_hidden_low
    grad_normed2 = lax.psum_scatter(
        jnp.einsum("sif,df->sid", segment, wide_up, preferred_element_type=jnp.float32),
        "tensor",
        scatter_dimension=0,
        tiled=True,
    )
    second_pull = jax.vjp(layer_norm, hidden1, gains[1], shifts[1])[1]
    grad_from_norm, gain2_grad, shift2_grad = second_pull(grad_normed2)
    grad_hidden1 = grad_out + grad_from_norm
    grad_attn_low = grad_hidden1.astype(jnp.bfloat16)
    grad_attn_all = lax.all_gather(grad_attn_low, "tensor", axis=0, tiled=True)
    grad_w_o = jnp.einsum(
        "sic,sid->cd", mixture_seq, grad_attn_all, preferred_element_type=jnp.float32
    )
    grad_mixture = jnp.einsum(
        "sid,cd->sic", grad_attn_all, wide_out, preferred_element_type=jnp.float32
    ).astype(jnp.bfloat16)
    grad_mixture_img = jnp.transpose(
        grad_mixture.reshape(full_length, images, heads_local, HD), (1, 0, 2, 3)
    )
    grad_packed = lax.map(attend_backward, (per_image, grad_mixture_img, log_total, valid_mask))
    grad_projected = jnp.transpose(grad_packed, (1, 0, 2, 3, 4)).reshape(
        full_length, images, 3, columns
    )
    grad_b_qv = jnp.stack(
        [
            jnp.sum(grad_projected[:, :, 0], axis=(0, 1)),
            jnp.sum(grad_projected[:, :, 2], axis=(0, 1)),
        ]
    )
    grad_projected_low = grad_projected.reshape(full_length, images, 3 * columns).astype(
        jnp.bfloat16
    )
    grad_w_qkv = jnp.einsum(
        "sid,sic->dc", gathered1, grad_projected_low, preferred_element_type=jnp.float32
    ).reshape(model_width, 3, columns)
    segment = grad_projected_low
    grad_normed1 = lax.psum_scatter(
        jnp.einsum("sic,dc->sid", segment, wide_qkv, preferred_element_type=jnp.float32).astype(
            jnp.bfloat16
        ),
        "tensor",
        scatter_dimension=0,
        tiled=True,
    ).astype(jnp.float32)
    first_pull = jax.vjp(layer_norm, residual, gains[0], shifts[0])[1]
    grad_from_front, gain1_grad, shift1_grad = first_pull(grad_normed1)
    grad_inputs = grad_hidden1 + grad_from_front
    gain_terms = jnp.stack([gain1_grad, gain2_grad])
    shift_terms = jnp.stack(
        [
            shift1_grad,
            shift2_grad,
            jnp.sum(grad_hidden1, axis=(0, 1)),
            jnp.sum(grad_out, axis=(0, 1)),
        ]
    )
    scattered = (
        lax.psum_scatter(
            gain_terms.astype(jnp.bfloat16), "dp", scatter_dimension=1, tiled=True
        ).astype(jnp.float32),
        lax.psum_scatter(
            shift_terms.astype(jnp.bfloat16), "dp", scatter_dimension=1, tiled=True
        ).astype(jnp.float32),
        lax.psum_scatter(
            grad_w_qkv.astype(jnp.bfloat16), "dp", scatter_dimension=0, tiled=True
        ).astype(jnp.float32),
        lax.psum_scatter(
            grad_w_o.astype(jnp.bfloat16), "dp", scatter_dimension=1, tiled=True
        ).astype(jnp.float32),
        lax.psum_scatter(
            grad_w_1.astype(jnp.bfloat16), "dp", scatter_dimension=0, tiled=True
        ).astype(jnp.float32),
        lax.psum_scatter(
            grad_w_2.astype(jnp.bfloat16), "dp", scatter_dimension=1, tiled=True
        ).astype(jnp.float32),
    )
    gain_sum, shift_sum = lax.psum((scattered[0], scattered[1]), "tensor")
    bias_qv_sum, bias_up_sum = lax.psum((grad_b_qv, grad_b_1), "dp")
    return (
        block_output,
        grad_inputs,
        gain_sum,
        shift_sum,
        scattered[2],
        bias_qv_sum,
        scattered[3],
        scattered[4],
        bias_up_sum,
        scattered[5],
    )


Q = 160
HALF = 2 * Q
FULL = 4 * Q
BF, F32 = jnp.bfloat16, jnp.float32
MESH = pl.DeviceIdType.MESH


def place(y, x, c, z):
    return (y * 4 + x * 2 + c, z)


def at_rows(start, size, step=8):
    return pl.ds(pl.multiple_of(start, step), size)


def mm(left, right, dims):
    return lax.dot_general(left, right, (dims, ((), ())), preferred_element_type=F32)


NN = ((1,), (0,))
NT = ((1,), (1,))
TN = ((0,), (0,))


class Links:
    def __init__(self, send_sem, recv_sem):
        self.send_sem, self.recv_sem = send_sem, recv_sem
        self.sends, self.used, self.keys, self.dropped = [], 0, {}, set()

    def base(self, key, count):
        if key not in self.keys:
            self.keys[key] = self.used
            self.used += count
        return self.keys[key]

    def copy(self, src, dst, sent, got, to):
        return pltpu.make_async_remote_copy(
            src_ref=src,
            dst_ref=dst,
            send_sem=self.send_sem.at[sent],
            recv_sem=self.recv_sem.at[got],
            device_id=to,
            device_id_type=MESH,
        )

    def drop(self, *sent):
        self.dropped = self.dropped | set(sent)

    def each(self, make, act):
        src, dst, sent, got, to, when = make()
        if when is None:
            act(self.copy(src, dst, sent, got, to))
        else:
            pl.when(when)(lambda: act(self.copy(src, dst, sent, got, to)))

    def start(self, make):
        self.sends.append(make)
        self.each(make, lambda copy: copy.start())

    def put(self, src, dst, sent, got, to, when=None):
        self.start(lambda: (src, dst, sent, got, to, when))

    def wait(self, dst, got, to):
        self.copy(dst, dst, 0, got, to).wait_recv()

    def finish(self):
        for make in self.sends:
            sent = make()[2]
            if not (isinstance(sent, int) and sent in self.dropped):
                self.each(make, lambda copy: copy.wait_send())


def where_am_i():
    d = lax.axis_index("dp")
    return d // 4, (d // 2) % 2, d % 2, lax.axis_index("tensor")


def greet(y, x, c, z):
    barrier = pltpu.get_barrier_semaphore()
    peers = [(dy, dx, dc, 0) for dy in range(2) for dx in range(2) for dc in range(2) if dy + dx + dc]
    peers += [(0, 0, dc, dz) for dc in range(2) for dz in range(1, 4)]
    for dy, dx, dc, dz in peers:
        to = place((y + dy) % 2, (x + dx) % 2, (c + dc) % 2, (z + dz) % 4)
        pl.semaphore_signal(barrier, inc=1, device_id=to, device_id_type=MESH)
    pl.semaphore_wait(barrier, len(peers))


def unit_rows(v):
    average = jnp.mean(v, axis=-1, keepdims=True)
    centred = v - average
    variance = jnp.mean(centred * centred, axis=-1, keepdims=True)
    scale = lax.rsqrt(variance + EPSILON)
    return centred * scale, scale


def gelu_both(v):
    cdf = 0.5 * (1.0 + lax.erf(v * 0.7071067811865476))
    density = 0.3989422804014327 * jnp.exp(-0.5 * v * v)
    return v * cdf, cdf + v * density


def layer_kernel(
    tok_in, cot_in, mask_in, norm_in, bias_in, qkv_in, wo_in, w1_in, w2_in,
    block_out, grad_out, sums_out, qv_out, b1_out, qkv_out, wo_out, w1_out, w2_out,
    tok, cot, mask, norm, bias, qkv, wo, up, down,
    n1, proj, lse, mix, hid, n2, act, slope,
    norm_row, qkv_row, up_row, part, got_part,
    ga, gmix, gproj, d_up, d_down, d_qkv, d_wo, r_up, r_down, z_up, z_down, f_up, f_down, o_up, o_down,
    first_qkv, first_wo, second_qkv, second_wo, z_qkv, z_wo, f_qkv, f_wo, o_qkv, o_wo,
    s_far, s_mid, s_near, g_far, g_mid, g_near, b_far, b_mid, b_near, g_n1,
    sums, sums_row, sums_got, sums_z, gb1, gbq, gbv, bias_pack, bias_got, bias_all,
    local_sem, send_sem, recv_sem,
):
    y, x, c, z = where_am_i()
    r = y * 2 + x
    links = Links(send_sem, recv_sem)
    me = place(y, x, c, z)
    to_c, to_x, to_y = place(y, x, 1 - c, z), place(y, 1 - x, c, z), place(1 - y, x, c, z)
    greet(y, x, c, z)

    block_at = lambda ref, t: ref.at[at_rows(t * HALF, HALF, 64), :]
    block_rows = lambda t, start, size: at_rows(t * HALF + start, size, 32)

    def local(at, src, dst):
        return pltpu.make_async_copy(src, dst, local_sem.at[at])

    z1, z2, z3 = z + 1 - 2 * (z % 2), (z + 2) % 4, 3 - z
    to_z1, to_z2 = place(y, x, c, z1), place(y, x, c, z2)
    r_x, r_y, r_xy = 2 * y + 1 - x, 2 * (1 - y) + x, 3 - r
    q = 2 * x + c
    d = y * 4 + x * 2 + c

    qkv_at = lambda rr, o, cs: qkv.at[at_rows(rr * 256 + cs * 128, 128, 128), at_rows(o * 384, 384, 128)]
    wo_at = lambda rr, o, cs: wo.at[at_rows(o * 128, 128, 128), at_rows(rr * 256 + cs * 128, 128, 128)]
    s_pc = links.base("pc", 2)
    links.put(qkv_in.at[:, at_rows((1 - c) * 384, 384, 128)], qkv_at(r, z, c), s_pc, s_pc, to_c)
    links.put(wo_in.at[at_rows((1 - c) * 128, 128, 128), :], wo_at(r, z, c), s_pc + 1, s_pc + 1, to_c)
    own_qkv = local(0, qkv_in.at[:, at_rows(c * 384, 384, 128)], qkv_at(r, z, c))
    own_wo = local(1, wo_in.at[at_rows(c * 128, 128, 128), :], wo_at(r, z, c))
    own_qkv.start()
    own_wo.start()

    s_norm, s_bias, s_mask = links.base("norm", 8), links.base("bias", 4), links.base("mask", 1)
    for dd in range(1, 8):
        to = place((y + dd // 4) % 2, (x + (dd // 2) % 2) % 2, (c + dd % 2) % 2, z)
        links.put(norm_in, norm.at[d], s_norm + dd, s_norm + dd, to)
    for dz in range(1, 4):
        links.put(bias_in, bias.at[z], s_bias + dz, s_bias + dz, place(y, x, c, (z + dz) % 4))
    links.put(mask_in, mask.at[c], s_mask, s_mask, to_c)
    own_small = (local(2, norm_in, norm.at[d]), local(3, bias_in, bias.at[z]), local(4, mask_in, mask.at[c]))
    for one in own_small:
        one.start()

    def move_tokens(key, source, target_at, at):
        base = links.base(key, 4)
        target = target_at(z // 2)
        stay = c == z // 2
        rows = at_rows((z % 2) * Q, Q, 16)
        for i in range(2):
            here = jnp.logical_and(stay, z % 2 == i)
            to = place(y, x, z // 2, 2 * c + i)
            to = (jnp.where(here, place(y, x, 1 - c, z)[0], to[0]), to[1])
            links.put(source.at[i], target.at[rows], base + i, base + 2 + z % 2, to, jnp.logical_not(here))

            @pl.when(here)
            def _(i=i):
                local(at, source.at[i], target.at[rows]).start()

    def wait_tokens(key, source, target_at, at):
        base = links.base(key, 4)
        target = target_at(c)
        stay = c == z // 2
        for j in range(2):
            here = jnp.logical_and(stay, z % 2 == j)

            @pl.when(here)
            def _(j=j):
                local(at, source.at[j], target.at[pl.ds(j * Q, Q)]).wait()

            @pl.when(jnp.logical_not(here))
            def _(j=j):
                links.wait(target.at[pl.ds(j * Q, Q)], base + 2 + j, to_c)

    up_shard = lambda sx, sc: up.at[at_rows(y * 512 + sx * 256 + sc * 128, 128, 128), at_rows(z * 256, 256, 128)]
    down_shard = lambda sx, sc: down.at[at_rows(z * 256, 256, 128), at_rows(y * 512 + sx * 256 + sc * 128, 128, 128)]
    s_up, s_down = links.base("up", 4), links.base("down", 4)
    own_up = local(6, w1_in.at[:, at_rows(q * 256, 256, 128)], up_shard(x, c))
    own_down = local(7, w2_in.at[at_rows(q * 256, 256, 128), :], down_shard(x, c))
    own_up.start()
    own_down.start()

    def part_up(dx, dc):
        tx, tc, rel = (x + dx) % 2, (c + dc) % 2, 2 * dx + dc
        to = place(y, tx, tc, z)
        links.put(w1_in.at[:, at_rows((2 * tx + tc) * 256, 256, 128)], up_shard(x, c), s_up + rel, s_up + rel, to)

    def part_down(dx, dc):
        tx, tc, rel = (x + dx) % 2, (c + dc) % 2, 2 * dx + dc
        to = place(y, tx, tc, z)
        links.put(w2_in.at[at_rows((2 * tx + tc) * 256, 256, 128), :], down_shard(x, c), s_down + rel, s_down + rel, to)

    def wait_parts(shard, base):
        for dx, dc in ((0, 1), (1, 0), (1, 1)):
            links.wait(shard((x + dx) % 2, (c + dc) % 2), base + 2 * dx + dc, to_c)

    class Fan:
        def __init__(self, key, piece, arrived):
            self.piece, self.arrived = piece, arrived
            self.many = len(piece(0))
            self.got = [links.base((key, "got", n), 4) for n in range(self.many)]
            self.sent = [links.base((key, "sent", n), 3) for n in range(self.many)]

        def push(self, slot, o, to):
            for n in range(self.many):
                def make(n=n):
                    ref = self.piece(o)[n]
                    return ref, ref, self.sent[n] + slot, self.got[n] + o, to, None

                links.start(make)

        def take(self, o):
            for n, ref in enumerate(self.piece(o)):
                links.wait(ref, self.got[n] + o, to_z1)

        def begin(self):
            self.push(0, z, to_z2)
            self.push(1, z, to_z1)
            self.arrived(z)

        def far(self):
            self.take(z2)
            self.push(2, z2, to_z1)
            self.arrived(z2)

        def pair(self):
            self.take(z1)
            self.arrived(z1)

        def diagonal(self):
            self.take(z3)
            self.arrived(z3)

    attn_at = (qkv_at, wo_at)
    s_first = [links.base(("first", n), 8) for n in range(2)]
    s_own = [links.base(("own", n), 8) for n in range(2)]
    s_fwd = [links.base(("fwd", n), 8) for n in range(2)]
    to_first, to_second = (to_x, to_y), (to_y, to_x)
    r_first, r_second = (r_x, r_y), (r_y, r_x)

    def attn_arrived(o):
        for n, at in enumerate(attn_at):
            for cs in range(2):
                ref, sem = at(r, o, cs), o * 2 + cs
                links.put(ref, ref, s_first[n] + sem, s_first[n] + sem, to_first[cs])
        for n, at in enumerate(attn_at):
            for cs in range(2):
                ref, sem = at(r, o, cs), o * 2 + cs
                links.put(ref, ref, s_own[n] + sem, s_own[n] + sem, to_second[cs])

    def attn_forward(o):
        for n, at in enumerate(attn_at):
            for cs in range(2):
                ref, sem = at(r_first[cs], o, cs), o * 2 + cs
                links.wait(ref, s_first[n] + sem, to_x)
                links.put(ref, ref, s_fwd[n] + sem, s_fwd[n] + sem, to_second[cs])

    def attn_finish():
        for o in range(4):
            for n, at in enumerate(attn_at):
                for cs in range(2):
                    sem = o * 2 + cs
                    links.wait(at(r_second[cs], o, cs), s_own[n] + sem, to_x)
                    links.wait(at(r_xy, o, cs), s_fwd[n] + sem, to_x)

    attn_fan = Fan("attn", lambda o: [at(r, o, cs) for at in attn_at for cs in range(2)], attn_arrived)
    up_at = lambda yy, o: up.at[at_rows(yy * 512, 512, 512), at_rows(o * 256, 256, 256)]
    down_at = lambda yy, o: down.at[at_rows(o * 256, 256, 256), at_rows(yy * 512, 512, 512)]
    s_upy, s_downy = links.base("upy", 4), links.base("downy", 4)

    def across(at, base):
        return lambda o: links.start(lambda: (at(y, o), at(y, o), base + o, base + o, to_y, None))

    up_fan = Fan("upf", lambda o: (up_at(y, o),), across(up_at, s_upy))
    down_fan = Fan("downf", lambda o: (down_at(y, o),), across(down_at, s_downy))

    lse[...] = jnp.zeros_like(lse)
    own_qkv.wait()
    own_wo.wait()
    links.wait(qkv_at(r, z, 1 - c), s_pc, to_c)
    links.wait(wo_at(r, z, 1 - c), s_pc + 1, to_c)
    attn_fan.begin()
    attn_fan.far()
    attn_forward(z)
    move_tokens("tok", tok_in, lambda cc: tok, 5)
    for dx, dc in ((1, 0), (1, 1), (0, 1)):
        part_up(dx, dc)
    attn_fan.pair()
    for one in own_small:
        one.wait()
    for dd in range(1, 8):
        source = 4 * ((y + dd // 4) % 2) + 2 * ((x + (dd // 2) % 2) % 2) + (c + dd % 2) % 2
        links.wait(norm.at[source], s_norm + dd, to_c)
    for dz in range(1, 4):
        links.wait(bias.at[(z + 4 - dz) % 4], s_bias + dz, to_c)
    links.wait(mask.at[1 - c], s_mask, to_c)
    for dd in range(8):
        norm_row[:, dd * 128 : dd * 128 + 128] = norm[dd]
    for zz in range(4):
        qkv_row[:, zz * 384 : zz * 384 + 128] = bias[zz, 0:1]
        qkv_row[:, zz * 384 + 128 : zz * 384 + 256] = jnp.zeros((1, 128), F32)
        qkv_row[:, zz * 384 + 256 : zz * 384 + 384] = bias[zz, 1:2]
        up_row[:, zz * 256 : zz * 256 + 128] = bias[zz, 2:3]
        up_row[:, zz * 256 + 128 : zz * 256 + 256] = bias[zz, 3:4]
    attn_fan.diagonal()
    attn_forward(z2)
    attn_forward(z1)
    for dx, dc in ((1, 0), (1, 1), (0, 1)):
        part_down(dx, dc)
    own_up.wait()
    own_down.wait()
    wait_parts(up_shard, s_up)
    up_fan.begin()
    attn_forward(z3)

    wait_tokens("tok", tok_in, lambda cc: tok, 5)

    @pl.loop(0, HALF // 32)
    def _(i):
        v = tok[at_rows(i * 32, 32, 32), :].astype(F32)
        unit, _ = unit_rows(v)
        n1[at_rows(c * HALF + i * 32, 32, 32), :] = (unit * norm_row[0:1] + norm_row[2:3]).astype(BF)

    s_n1 = links.base("n1", 1)
    half_at = lambda ref, cc: ref.at[at_rows(cc * HALF, HALF, 64), :]
    links.put(half_at(n1, c), half_at(n1, c), s_n1, s_n1, to_c)
    up_fan.far()
    move_tokens("cot", cot_in, lambda cc: block_at(cot, 2 * x + cc), 8)
    wait_parts(down_shard, s_down)
    links.wait(half_at(n1, 1 - c), s_n1, to_c)
    attn_finish()
    up_fan.pair()
    down_fan.begin()

    @pl.loop(0, 6)
    def _(j):
        columns = at_rows(j * 256, 256, 256)
        proj[:, columns] = (mm(n1[...], qkv[:, columns], NN) + qkv_row[:, columns]).astype(BF)

    lane = lax.broadcasted_iota(jnp.int32, (1, 128), 1)
    first_head = lane < 64
    zero = jnp.zeros((), BF)

    def spread_start(key, ref):
        base = links.base(("spread", key), 3)
        links.start(lambda: (block_at(ref, q), block_at(ref, q), base, base, to_x, None))
        links.start(lambda: (block_at(ref, q), block_at(ref, q), base + 1, base + 1, to_c, None))

    def spread_forward(key, ref):
        base = links.base(("spread", key), 3)
        far = lambda: block_at(ref, 2 * (1 - x) + c)
        links.wait(far(), base, to_x)
        links.start(lambda: (far(), far(), base + 2, base + 2, to_c, None))

    def spread_wait_near(key, ref):
        links.wait(block_at(ref, 2 * x + 1 - c), links.base(("spread", key), 3) + 1, to_c)

    def spread_wait_far(key, ref):
        links.wait(block_at(ref, 2 * (1 - x) + 1 - c), links.base(("spread", key), 3) + 2, to_c)

    @pl.loop(0, 4)
    def _(zz):
        keys = proj[:, at_rows(zz * 384 + 128, 128, 128)]
        values = proj[:, at_rows(zz * 384 + 256, 128, 128)]
        hidden_key = mask[z // 2, z % 2]
        for rb in range(2):
            rows = pl.ds(rb * HALF, HALF)
            pair = proj[rows, at_rows(zz * 384, 128, 128)]
            outs = []
            for hh in range(2):
                own = jnp.where(first_head if hh == 0 else jnp.logical_not(first_head), pair, zero)
                scores = mm(own, keys, NT) * (HD ** (-0.5)) + hidden_key
                highest = jnp.max(scores, axis=-1, keepdims=True)
                exponent = jnp.exp(scores - highest)
                total = jnp.sum(exponent, axis=-1, keepdims=True)
                low = (exponent * (1.0 / total)).astype(BF)
                head = 2 * zz + hh
                lse[rows, :] = jnp.where(lane == head, highest + jnp.log(total), lse[rows, :])
                outs.append(mm(low, values, NN))
            mix[rows, at_rows(zz * 128, 128, 128)] = jnp.where(first_head, outs[0], outs[1]).astype(BF)

        @pl.when(zz == 0)
        def _():
            up_fan.diagonal()

        @pl.when(zz == 2)
        def _():
            down_fan.far()

        @pl.when(zz == 3)
        def _():
            wait_tokens("cot", cot_in, lambda cc: block_at(cot, 2 * x + cc), 8)
            spread_start("cot", cot)

    s_part = links.base("part", 1)

    def project_out(cc, target):
        @pl.loop(0, 4)
        def _(j):
            columns = at_rows(j * 256, 256, 256)
            target[:, columns] = mm(mix[at_rows(cc * HALF, HALF, 64), :], wo[:, columns], NN)

    project_out(1 - c, part)
    links.put(part, got_part, s_part, s_part, to_c)
    project_out(c, hid)
    links.wait(got_part, s_part, to_c)

    @pl.loop(0, HALF // 32)
    def _(i):
        rows = at_rows(i * 32, 32, 32)
        v = hid[rows, :] + got_part[rows, :] + tok[rows, :].astype(F32) + norm_row[4:5]
        hid[rows, :] = v
        unit, _ = unit_rows(v)
        n2[block_rows(q, i * 32, 32), :] = (unit * norm_row[1:2] + norm_row[3:4]).astype(BF)

    spread_start("n2", n2)
    down_fan.pair()
    spread_forward("cot", cot)
    spread_wait_near("cot", cot)
    for o in range(4):
        links.wait(up_at(1 - y, o), s_upy + o, to_y)

    def expand(t):
        @pl.loop(0, 4)
        def _(j):
            columns = at_rows(j * 256, 256, 256)
            for rb in range(2):
                rows = block_rows(t, rb * Q, Q)
                v = mm(n2[rows, :], up[:, columns], NN) + up_row[:, columns]
                value, grade = gelu_both(v)
                act[rows, columns] = value.astype(BF)
                slope[rows, columns] = grade.astype(BF)

    expand(q)
    spread_wait_near("n2", n2)
    expand(2 * x + 1 - c)
    down_fan.diagonal()
    spread_forward("n2", n2)
    expand(2 * (1 - x) + c)
    spread_wait_far("n2", n2)
    expand(2 * (1 - x) + 1 - c)
    spread_wait_far("cot", cot)

    near_other, far_own, far_other = 2 * x + 1 - c, 2 * (1 - x) + c, 2 * (1 - x) + 1 - c
    sums[...] = jnp.zeros_like(sums)
    gb1[...] = jnp.zeros_like(gb1)

    def fold(v):
        return v[0:8] + v[8:16] + v[16:24] + v[24:32]

    def tally(row, v):
        sums[row * 8 : row * 8 + 8, :] += fold(v)

    def send_later(make):
        links.start(make)

    def through_slope(t):
        @pl.loop(0, 4)
        def _(j):
            columns = at_rows(j * 256, 256, 256)
            rows = block_rows(t, 0, HALF)
            v = mm(cot[rows, :], down[columns, :], NT) * slope[rows, columns].astype(F32)
            gb1[:, columns] += jnp.sum(v.reshape(HALF // 8, 8, 256), axis=0)
            slope[rows, columns] = v.astype(BF)

    def back_part(t, target):
        @pl.loop(0, 4)
        def _(j):
            columns = at_rows(j * 256, 256, 256)
            target[:, columns] = mm(slope[block_rows(t, 0, HALF), :], up[columns, :], NT).astype(target.dtype)

    def add_rows(target, *sources):
        @pl.loop(0, HALF // 32)
        def _(i):
            rows = at_rows(i * 32, 32, 32)
            total = sources[0][rows, :].astype(F32)
            for source in sources[1:]:
                total = total + source[rows, :].astype(F32)
            target[rows, :] = total.astype(target.dtype)

    z_order = (z3, z1, z2, z)
    s_rdown, s_rup = links.base("rdown", 4), links.base("rup", 4)
    d_down_at = lambda yy, o: d_down.at[at_rows(o * 256, 256, 256), at_rows(yy * 512, 512, 512)]
    d_up_at = lambda yy, o: d_up.at[at_rows(yy * 512, 512, 512), at_rows(o * 256, 256, 256)]
    r_down_at = lambda o: r_down.at[at_rows(o * 256, 256, 256), :]
    r_up_at = lambda o: r_up.at[:, at_rows(o * 256, 256, 256)]

    def accumulate(target, *sources):
        count = target.shape[0] // 64

        @pl.loop(0, count)
        def _(i):
            rows = at_rows(i * 64, 64, 64)
            total = target[rows, :].astype(F32)
            for source in sources:
                total = total + source[rows, :].astype(F32)
            target[rows, :] = total.astype(target.dtype)

    class Fold:
        def __init__(self, key, piece, over_z, final):
            self.piece, self.over_z, self.final = piece, over_z, final
            self.sz = links.base((key, "z"), 3)

        def push(self, o, slot, to):
            links.start(lambda: (self.piece(o), self.over_z.at[slot], self.sz + slot, self.sz + slot, to, None))

        def pair_far(self):
            self.collect(z3)
            self.push(z3, 0, to_z1)

        def pair_near(self):
            self.collect(z1)
            self.push(z1, 1, to_z1)

        def far(self):
            self.collect(z2)
            links.wait(self.over_z.at[0], self.sz, to_z1)
            accumulate(self.piece(z2), self.over_z.at[0])
            self.push(z2, 2, to_z2)

        def last(self):
            self.collect(z)
            links.wait(self.over_z.at[1], self.sz + 1, to_z1)
            links.wait(self.over_z.at[2], self.sz + 2, to_z2)
            own, others = self.piece(z), [self.over_z.at[1], self.over_z.at[2]]
            count = own.shape[0] // 64

            @pl.loop(0, count)
            def _(i):
                rows = at_rows(i * 64, 64, 64)
                total = own[rows, :].astype(F32)
                for other in others:
                    total = total + other[rows, :].astype(F32)
                self.final[rows, :] = total.astype(BF)

    class Half(Fold):
        def __init__(self, key, at, got_at, s_got, over_z, final):
            super().__init__(key, lambda o: at(y, o), over_z, final)
            self.got_at, self.s_got = got_at, s_got

        def collect(self, o):
            links.wait(self.got_at(o), self.s_got + o, to_y)
            accumulate(self.piece(o), self.got_at(o))

    half_down = Half("half_down", d_down_at, r_down_at, s_rdown, z_down, f_down)
    half_up = Half("half_up", d_up_at, r_up_at, s_rup, z_up, f_up)

    def give_down(o):
        rows = at_rows(o * 256, 256, 256)
        d_down[rows, :] = mm(act[:, rows], cot[...], TN).astype(BF)
        links.start(lambda: (d_down_at(1 - y, o), r_down_at(o), s_rdown + o, s_rdown + o, to_y, None))

    def give_up(o):
        columns = at_rows(o * 256, 256, 256)
        d_up[:, columns] = mm(n2[...], slope[:, columns], TN).astype(BF)
        links.start(lambda: (d_up_at(1 - y, o), r_up_at(o), s_rup + o, s_rup + o, to_y, None))

    for o in z_order:
        give_down(o)
    for o in range(4):
        links.wait(down_at(1 - y, o), s_downy + o, to_y)

    s_gfar, s_gmid, s_gnear = links.base("gfar", 1), links.base("gmid", 1), links.base("gnear", 1)
    s_bfar, s_bmid, s_bnear = links.base("bfar", 1), links.base("bmid", 1), links.base("bnear", 1)
    through_slope(far_other)
    back_part(far_other, s_far)
    links.put(s_far, g_far, s_gfar, s_gfar, to_c)
    through_slope(far_own)
    links.copy(part, got_part, s_part, s_part, to_c).wait_send()
    links.drop(s_part)
    back_part(far_own, part)
    links.wait(g_far, s_gfar, to_c)
    add_rows(s_mid, part, g_far)
    links.put(s_mid, g_mid, s_gmid, s_gmid, to_x)
    through_slope(near_other)
    back_part(near_other, s_near)
    links.put(s_near, g_near, s_gnear, s_gnear, to_c)
    through_slope(q)
    back_part(q, part)
    half_down.pair_far()
    half_down.pair_near()
    for o in z_order:
        give_up(o)
    half_down.far()

    links.wait(g_near, s_gnear, to_c)
    links.wait(g_mid, s_gmid, to_x)

    @pl.loop(0, HALF // 32)
    def _(i):
        rows = at_rows(i * 32, 32, 32)
        grad = part[rows, :] + g_near[rows, :].astype(F32) + g_mid[rows, :].astype(F32)
        unit, scale = unit_rows(hid[rows, :])
        out = cot[block_rows(q, i * 32, 32), :].astype(F32)
        scaled = grad * norm_row[1:2]
        moved = scale * (
            scaled
            - jnp.mean(scaled, axis=-1, keepdims=True)
            - unit * jnp.mean(scaled * unit, axis=-1, keepdims=True)
        )
        total = out + moved
        tally(1, grad * unit)
        tally(3, grad)
        tally(4, total)
        tally(5, out)
        got_part[rows, :] = total
        ga[at_rows(c * HALF + i * 32, 32, 32), :] = total.astype(BF)

    s_ga = links.base("ga", 1)
    links.put(half_at(ga, c), half_at(ga, c), s_ga, s_ga, to_c)

    def down_part(t, target, base=None):
        @pl.loop(0, 4)
        def _(j):
            columns = at_rows(j * 256, 256, 256)
            v = mm(act[block_rows(t, 0, HALF), :], down[:, columns], NN)
            target[:, columns] = (v if base is None else v + base[:, columns]).astype(target.dtype)

    links.copy(s_far, g_far, s_gfar, s_gfar, to_c).wait_send()
    links.copy(s_mid, g_mid, s_gmid, s_gmid, to_x).wait_send()
    links.copy(s_near, g_near, s_gnear, s_gnear, to_c).wait_send()
    links.drop(s_gfar, s_gmid, s_gnear)
    down_part(far_other, s_far)
    links.put(s_far, b_far, s_bfar, s_bfar, to_c)

    links.wait(half_at(ga, 1 - c), s_ga, to_c)

    @pl.loop(0, 2)
    def _(j):
        columns = at_rows(j * 256, 256, 256)
        gmix[:, columns] = mm(ga[...], wo[columns, :], NT).astype(BF)

    @pl.loop(0, 2)
    def _(j):
        columns = at_rows(j * 256, 256, 256)
        d_wo[columns, :] = mm(mix[:, columns], ga[...], TN).astype(BF)

    d_qkv_at = lambda rr, o, cs: d_qkv.at[at_rows(rr * 256 + cs * 128, 128, 128), at_rows(o * 384, 384, 128)]
    d_wo_at = lambda rr, o, cs: d_wo.at[at_rows(o * 128, 128, 128), at_rows(rr * 256 + cs * 128, 128, 128)]
    d_qkv_all = lambda o: d_qkv.at[at_rows(r * 256, 256, 256), at_rows(o * 384, 384, 128)]
    d_wo_all = lambda o: d_wo.at[at_rows(o * 128, 128, 128), at_rows(r * 256, 256, 128)]

    class Reduce(Fold):
        def __init__(self, key, at, whole, first, second, over_z, final):
            super().__init__(key, whole, over_z, final)
            self.at, self.first, self.second = at, first, second
            self.s1 = [links.base((key, "first", i), 8) for i in range(2)]
            self.s2 = links.base((key, "second"), 8)

        def begin(self, o, cs):
            sem = 2 * o + cs
            for i, rr in ((1, r_xy), (0, r_first[cs])):
                links.start(
                    lambda i=i, rr=rr: (
                        self.at(rr, o, cs), self.first.at[i, o, cs], self.s1[i] + sem, self.s1[i] + sem, to_first[cs], None,
                    )
                )

        def middle(self, o, cs):
            sem = 2 * o + cs
            links.wait(self.first.at[1, o, cs], self.s1[1] + sem, to_x)
            accumulate(self.at(r_second[cs], o, cs), self.first.at[1, o, cs])
            links.start(
                lambda: (
                    self.at(r_second[cs], o, cs), self.second.at[o, cs], self.s2 + sem, self.s2 + sem, to_second[cs], None,
                )
            )

        def collect(self, o):
            for cs in range(2):
                sem = 2 * o + cs
                links.wait(self.first.at[0, o, cs], self.s1[0] + sem, to_x)
                links.wait(self.second.at[o, cs], self.s2 + sem, to_x)
                accumulate(self.at(r, o, cs), self.first.at[0, o, cs], self.second.at[o, cs])

    red_wo = Reduce("red_wo", d_wo_at, d_wo_all, first_wo, second_wo, z_wo, f_wo)
    red_qkv = Reduce("red_qkv", d_qkv_at, d_qkv_all, first_qkv, second_qkv, z_qkv, f_qkv)
    for cs in range(2):
        for o in z_order:
            red_wo.begin(o, cs)

    down_part(far_own, part)
    links.wait(b_far, s_bfar, to_c)
    add_rows(s_mid, part, b_far)
    links.put(s_mid, b_mid, s_bmid, s_bmid, to_x)
    down_part(near_other, s_near)
    links.put(s_near, b_near, s_bnear, s_bnear, to_c)
    down_part(q, hid, hid)

    s_oup, s_odown = links.base("oup", 4), links.base("odown", 4)

    def scatter_down():
        for dx, dc in ((1, 0), (1, 1), (0, 1)):
            def make(dx=dx, dc=dc):
                rel, tx, tc = 2 * dx + dc, (x + dx) % 2, (c + dc) % 2
                columns = at_rows((2 * tx + tc) * 128, 128, 128)
                return f_down.at[:, columns], o_down.at[q], s_odown + rel, s_odown + rel, place(y, tx, tc, z), None

            links.start(make)

    def scatter_up():
        for dx, dc in ((1, 0), (1, 1), (0, 1)):
            def make(dx=dx, dc=dc):
                rel, tx, tc = 2 * dx + dc, (x + dx) % 2, (c + dc) % 2
                rows = at_rows((2 * tx + tc) * 128, 128, 128)
                return f_up.at[rows, :], o_up.at[q], s_oup + rel, s_oup + rel, place(y, tx, tc, z), None

            links.start(make)

    @pl.loop(0, 4)
    def _(zz):
        base = zz * 384
        keys = proj[:, at_rows(base + 128, 128, 128)]
        values = proj[:, at_rows(base + 256, 128, 128)]
        hidden_key = mask[z // 2, z % 2]
        d_keys = d_values = None
        sum_queries = None
        for rb in range(2):
            rows = pl.ds(rb * HALF, HALF)
            pair = proj[rows, at_rows(base, 128, 128)]
            grads = gmix[rows, at_rows(zz * 128, 128, 128)]
            outs = []
            for hh in range(2):
                keep = first_head if hh == 0 else jnp.logical_not(first_head)
                own = jnp.where(keep, pair, zero)
                own_grad = jnp.where(keep, grads, zero)
                level = jnp.sum(jnp.where(lane == 2 * zz + hh, lse[rows, :], 0.0), axis=-1, keepdims=True)
                attention = jnp.exp(mm(own, keys, NT) * (HD ** (-0.5)) + hidden_key - level)
                grad_attention = mm(own_grad, values, NT)
                inner = jnp.sum(attention * grad_attention, axis=-1, keepdims=True)
                low = (attention * (grad_attention - inner)).astype(BF)
                more_values = mm(attention.astype(BF), own_grad, TN)
                more_keys = mm(low, own, TN)
                d_values = more_values if d_values is None else d_values + more_values
                d_keys = more_keys if d_keys is None else d_keys + more_keys
                outs.append(mm(low, keys, NN))
            d_queries = jnp.where(first_head, outs[0], outs[1]) * (HD ** (-0.5))
            total = jnp.sum(d_queries.reshape(HALF // 8, 8, 128), axis=0)
            sum_queries = total if sum_queries is None else sum_queries + total
            gproj[rows, at_rows(base, 128, 128)] = d_queries.astype(BF)
        gproj[:, at_rows(base + 128, 128, 128)] = (d_keys * (HD ** (-0.5))).astype(BF)
        gproj[:, at_rows(base + 256, 128, 128)] = d_values.astype(BF)
        gbq[:, at_rows(zz * 128, 128, 128)] = sum_queries
        gbv[:, at_rows(zz * 128, 128, 128)] = jnp.sum(d_values.reshape(FULL // 8, 8, 128), axis=0)

        @pl.when(zz == 0)
        def _():
            half_down.last()
            scatter_down()

        @pl.when(zz == 1)
        def _():
            half_up.pair_far()
            half_up.pair_near()

        @pl.when(zz == 2)
        def _():
            half_up.far()

    links.wait(b_near, s_bnear, to_c)
    links.wait(b_mid, s_bmid, to_x)
    links.copy(s_far, b_far, s_bfar, s_bfar, to_c).wait_send()
    links.copy(s_near, b_near, s_bnear, s_bnear, to_c).wait_send()
    links.drop(s_bfar, s_bnear)

    @pl.loop(0, HALF // 32)
    def _(i):
        rows = at_rows(i * 32, 32, 32)
        total = hid[rows, :] + b_near[rows, :].astype(F32) + b_mid[rows, :].astype(F32) + norm_row[5:6]
        s_near[rows, :] = total.astype(BF)

    def send_home(key, source, target, at):
        base = links.base(key, 4)
        for j in range(2):
            def make(j=j):
                here = jnp.logical_and(z // 2 == c, z == 2 * c + j)
                to = place(y, x, z // 2, 2 * c + j)
                to = (jnp.where(here, place(y, x, 1 - c, z)[0], to[0]), to[1])
                return source.at[pl.ds(j * Q, Q)], target.at[z % 2], base + j, base + 2 + z % 2, to, jnp.logical_not(here)

            links.start(make)

            @pl.when(jnp.logical_and(z // 2 == c, z == 2 * c + j))
            def _(j=j):
                local(at, source.at[pl.ds(j * Q, Q)], target.at[z % 2]).start()

    def wait_home(key, source, target, at):
        base = links.base(key, 4)
        for i in range(2):
            here = jnp.logical_and(z // 2 == c, z % 2 == i)

            @pl.when(here)
            def _(i=i):
                local(at, source.at[pl.ds(0, Q)], target.at[i]).wait()

            @pl.when(jnp.logical_not(here))
            def _(i=i):
                links.wait(target.at[i], base + 2 + i, to_c)

    send_home("block", s_near, block_out, 9)

    def weigh(rr):
        d_qkv[at_rows(rr * 256, 256, 256), :] = mm(n1[:, at_rows(rr * 256, 256, 256)], gproj[...], TN).astype(BF)

    weigh(r_xy)
    weigh(r_x)
    for o in z_order:
        red_qkv.begin(o, 0)
    weigh(r_y)
    for o in z_order:
        red_qkv.begin(o, 1)

    def front_part(cc, target):
        @pl.loop(0, 4)
        def _(j):
            columns = at_rows(j * 256, 256, 256)
            target[:, columns] = mm(gproj[at_rows(cc * HALF, HALF, 64), :], qkv[columns, :], NT).astype(target.dtype)

    s_gn1 = links.base("gn1", 1)
    front_part(1 - c, s_far)
    links.put(s_far, g_n1, s_gn1, s_gn1, to_c)
    for o in z_order:
        for cs in range(2):
            red_wo.middle(o, cs)
    weigh(r)
    front_part(c, part)
    links.wait(g_n1, s_gn1, to_c)
    links.copy(s_mid, b_mid, s_bmid, s_bmid, to_x).wait_send()
    links.drop(s_bmid)

    @pl.loop(0, HALF // 32)
    def _(i):
        rows = at_rows(i * 32, 32, 32)
        grad = part[rows, :] + g_n1[rows, :].astype(F32)
        unit, scale = unit_rows(tok[rows, :].astype(F32))
        scaled = grad * norm_row[0:1]
        moved = scale * (
            scaled
            - jnp.mean(scaled, axis=-1, keepdims=True)
            - unit * jnp.mean(scaled * unit, axis=-1, keepdims=True)
        )
        tally(0, grad * unit)
        tally(2, grad)
        s_mid[rows, :] = (got_part[rows, :] + moved).astype(BF)

    send_home("home", s_mid, grad_out, 10)

    for row in range(6):
        sums_row[row : row + 1, :] = jnp.sum(sums[row * 8 : row * 8 + 8, :], axis=0, keepdims=True)
    sums_row[6:8, :] = jnp.zeros((2, 1024), F32)
    for dd in range(8):
        norm[dd] = sums_row[:, dd * 128 : dd * 128 + 128]
    s_sum, s_sumz = links.base("sum", 8), links.base("sumz", 8)
    for dd in range(1, 8):
        def make(dd=dd):
            ty, tx, tc = (y + dd // 4) % 2, (x + (dd // 2) % 2) % 2, (c + dd % 2) % 2
            return norm.at[4 * ty + 2 * tx + tc], sums_got.at[dd], s_sum + dd, s_sum + dd, place(ty, tx, tc, z), None

        links.start(make)
    for zz in range(4):
        flat = lambda ref, start: jnp.sum(ref[:, start : start + 128], axis=0, keepdims=True)
        bias_pack[zz, 0:1] = flat(gbq, zz * 128)
        bias_pack[zz, 1:2] = flat(gbv, zz * 128)
        bias_pack[zz, 2:3] = flat(gb1, zz * 256)
        bias_pack[zz, 3:4] = flat(gb1, zz * 256 + 128)
        bias_pack[zz, 4:8] = jnp.zeros((4, 128), F32)
    s_bz, s_ball = links.base("bz", 4), links.base("ball", 8)
    for dz in range(1, 4):
        def make(dz=dz):
            tz = (z + dz) % 4
            return bias_pack.at[tz], bias_got.at[dz], s_bz + dz, s_bz + dz, place(y, x, c, tz), None

        links.start(make)

    half_up.last()
    scatter_up()
    red_wo.pair_far()
    red_wo.pair_near()
    for o in z_order:
        for cs in range(2):
            red_qkv.middle(o, cs)
    red_wo.far()
    red_qkv.pair_far()
    red_qkv.pair_near()
    red_qkv.far()

    for dz in range(1, 4):
        links.wait(bias_got.at[dz], s_bz + dz, to_c)
    bias_all[d] = bias_pack[z] + bias_got[1] + bias_got[2] + bias_got[3]
    for dd in range(1, 8):
        def make(dd=dd):
            to = place((y + dd // 4) % 2, (x + (dd // 2) % 2) % 2, (c + dd % 2) % 2, z)
            return bias_all.at[d], bias_all.at[d], s_ball + dd, s_ball + dd, to, None

        links.start(make)
    for dd in range(1, 8):
        links.wait(sums_got.at[dd], s_sum + dd, to_c)
    total = norm[d]
    for dd in range(1, 8):
        total = total + sums_got[dd]
    sums_z[0] = total
    for dz in range(1, 4):
        def make(dz=dz):
            return sums_z.at[0], sums_z.at[dz], s_sumz + dz, s_sumz + dz, place(y, x, c, (z + dz) % 4), None

        links.start(make)

    red_wo.last()

    w1_out[:, at_rows(q * 256, 256, 256)] = f_up[at_rows(q * 128, 128, 128), :].astype(F32)
    w2_out[at_rows(q * 256, 256, 256), :] = f_down[:, at_rows(q * 128, 128, 128)].astype(F32)
    for dx, dc in ((1, 0), (1, 1), (0, 1)):
        rel, source = 2 * dx + dc, 2 * ((x + dx) % 2) + (c + dc) % 2
        links.wait(o_up.at[source], s_oup + rel, to_c)
        links.wait(o_down.at[source], s_odown + rel, to_c)
        w1_out[:, at_rows(source * 256, 256, 256)] = o_up[source].astype(F32)
        w2_out[at_rows(source * 256, 256, 256), :] = o_down[source].astype(F32)

    for dd in range(1, 8):
        source = 4 * ((y + dd // 4) % 2) + 2 * ((x + (dd // 2) % 2) % 2) + (c + dd % 2) % 2
        links.wait(bias_all.at[source], s_ball + dd, to_c)
    for cc in range(2):
        together = bias_all[cc] + bias_all[2 + cc] + bias_all[4 + cc] + bias_all[6 + cc]
        qv_out[:, cc * 128 : cc * 128 + 128] = together[0:2]
    for qq in range(4):
        together = bias_all[qq] + bias_all[4 + qq]
        b1_out[qq * 2 : qq * 2 + 2, :] = together[2:4]
    for dz in range(1, 4):
        links.wait(sums_z.at[dz], s_sumz + dz, to_c)
    sums_out[...] = sums_z[0] + sums_z[1] + sums_z[2] + sums_z[3]

    red_qkv.last()
    s_oqkv, s_owo = links.base("oqkv", 1), links.base("owo", 1)
    links.put(f_qkv.at[at_rows((1 - c) * 128, 128, 128), :], o_qkv, s_oqkv, s_oqkv, to_c)
    links.put(f_wo.at[:, at_rows((1 - c) * 128, 128, 128)], o_wo, s_owo, s_owo, to_c)
    qkv_out[:, at_rows(c * 384, 384, 128)] = f_qkv[at_rows(c * 128, 128, 128), :].astype(F32)
    wo_out[at_rows(c * 128, 128, 128), :] = f_wo[:, at_rows(c * 128, 128, 128)].astype(F32)
    links.wait(o_qkv, s_oqkv, to_c)
    links.wait(o_wo, s_owo, to_c)
    qkv_out[:, at_rows((1 - c) * 384, 384, 128)] = o_qkv[...].astype(F32)
    wo_out[at_rows((1 - c) * 128, 128, 128), :] = o_wo[...].astype(F32)
    wait_home("block", s_near, block_out, 9)
    wait_home("home", s_mid, grad_out, 10)
    links.finish()


def prepare(inputs, valid_mask, cotangent, ln_gain, d_bias, w_qkv, b_qv, b_1):
    y, x, c, z = where_am_i()
    rows = inputs.shape[0]
    turn = lambda v: jnp.pad(jnp.transpose(v, (1, 0, 2)), ((0, 0), (0, Q - rows), (0, 0)))
    mask = jnp.where(valid_mask.reshape(2, 4, rows) > 0, 0.0, MASKED).astype(F32)
    mask = jnp.pad(mask, ((0, 0), (0, 0), (0, Q - rows)), constant_values=MASKED).reshape(2, 1, FULL)
    norm = jnp.pad(jnp.concatenate([ln_gain, d_bias]).astype(F32), ((0, 2), (0, 0)))
    bias = jnp.concatenate(
        [
            lax.dynamic_slice(b_qv, (0, c * 128), (2, 128)),
            lax.dynamic_slice(b_1, ((2 * x + c) * 256,), (256,)).reshape(2, 128),
        ]
    ).astype(F32)
    bias = jnp.pad(bias, ((0, 4), (0, 0)))
    qkv = jnp.transpose(w_qkv.reshape(128, 3, 2, 128), (0, 2, 1, 3)).reshape(128, 768)
    return turn(inputs), turn(cotangent), mask, norm, bias, qkv


def layer_call(*operands):
    shape = jax.ShapeDtypeStruct
    hbm, vmem = pl.BlockSpec(memory_space=pl.ANY), pl.BlockSpec(memory_space=pltpu.VMEM)
    outs = [
        shape((2, Q, 1024), BF), shape((2, Q, 1024), BF), shape((8, 128), F32), shape((2, 256), F32),
        shape((8, 128), F32), shape((128, 768), F32), shape((256, 128), F32), shape((128, 1024), F32),
        shape((1024, 128), F32),
    ]
    low = lambda *dims: pltpu.VMEM(dims, BF)
    wide = lambda *dims: pltpu.VMEM(dims, F32)
    scratch = [
        low(HALF, 1024), low(4 * HALF, 1024), wide(2, 2, 1, FULL), wide(8, 8, 128), wide(4, 8, 128),
        low(1024, 1536), low(512, 1024), low(1024, 1024), low(1024, 1024),
        low(FULL, 1024), low(FULL, 1536), wide(FULL, 128), low(FULL, 512), wide(HALF, 1024),
        low(4 * HALF, 1024), low(4 * HALF, 1024), low(4 * HALF, 1024),
        wide(8, 1024), wide(1, 1536), wide(1, 1024), wide(HALF, 1024), wide(HALF, 1024),
        low(FULL, 1024), low(FULL, 512), low(FULL, 1536),
        low(1024, 1024), low(1024, 1024), low(1024, 1536), low(512, 1024),
        low(512, 1024), low(1024, 512), low(3, 512, 256), low(3, 256, 512),
        low(512, 256), low(256, 512), low(4, 128, 256), low(4, 256, 128),
        low(2, 4, 2, 128, 384), low(2, 4, 2, 128, 128), low(4, 2, 128, 384), low(4, 2, 128, 128),
        low(3, 256, 384), low(3, 128, 256), low(256, 384), low(128, 256), low(128, 384), low(128, 128),
        *[low(HALF, 1024)] * 10,
        wide(48, 1024), wide(8, 1024), wide(8, 8, 128), wide(4, 8, 128),
        wide(8, 1024), wide(8, 512), wide(8, 512), wide(4, 8, 128), wide(4, 8, 128), wide(8, 8, 128),
        pltpu.SemaphoreType.DMA((16,)), pltpu.SemaphoreType.DMA((320,)), pltpu.SemaphoreType.DMA((320,)),
    ]
    return pl.pallas_call(
        layer_kernel,
        out_shape=outs,
        in_specs=[hbm] * 9,
        out_specs=[hbm, hbm] + [vmem] * 7,
        scratch_shapes=scratch,
        compiler_params=pltpu.CompilerParams(collective_id=0, has_side_effects=True, vmem_limit_bytes=67043328),
        name="layer",
    )(*operands)


def fast_body(inputs, valid_mask, cotangent, ln_gain, d_bias, w_qkv, b_qv, w_o, w_1, b_1, w_2):
    rows = inputs.shape[0]
    block, grad, sums, qv, b1, qkv, wo, w1, w2 = layer_call(
        *prepare(inputs, valid_mask, cotangent, ln_gain, d_bias, w_qkv, b_qv, b_1), w_o, w_1, w_2
    )
    back = lambda v: jnp.transpose(v[:, :rows], (1, 0, 2))
    w_qkv_grad = jnp.transpose(qkv.reshape(128, 2, 3, 128), (0, 2, 1, 3)).reshape(128, 3, 256)
    return (
        back(block), back(grad).astype(F32), sums[:2], sums[2:6], w_qkv_grad, qv, wo, w1, b1.reshape(1024), w2,
    )


def solution(mesh):
    in_specs = (
        P("tensor", "dp", None),
        P("dp", None),
        P("tensor", "dp", None),
        P(None, "dp"),
        P(None, "dp"),
        P("dp", None, "tensor"),
        P(None, "tensor"),
        P("tensor", "dp"),
        P("dp", "tensor"),
        P("tensor"),
        P("tensor", "dp"),
    )
    out_specs = (
        P("tensor", "dp", None),
        P("tensor", "dp", None),
        P(None, "dp"),
        P(None, "dp"),
        P("dp", None, "tensor"),
        P(None, "tensor"),
        P("tensor", "dp"),
        P("dp", "tensor"),
        P("tensor"),
        P("tensor", "dp"),
    )
    run = fast_body if dict(mesh.shape) == {"dp": 8, "tensor": 4} else body
    return jax.shard_map(run, mesh=mesh, in_specs=in_specs, out_specs=out_specs, check_vma=False)
```

```python
import functools

import jax
import jax.numpy as jnp
from jax import lax
from jax.experimental import pallas as pl
from jax.experimental.pallas import tpu as pltpu
from jax.sharding import PartitionSpec as P

HD = 64


EPSILON = 1e-06
MASKED = -1e30


def layer_norm(values, gain, shift):
    average = jnp.mean(values, axis=-1, keepdims=True)
    centred = values - average
    variance = jnp.mean(centred * centred, axis=-1, keepdims=True)
    return centred * lax.rsqrt(variance + EPSILON) * gain + shift


def gelu_exact(values):
    return jax.nn.gelu(values, approximate=False)


def gather_layer(ln_gain, d_bias, w_qkv, w_o, w_1, w_2):
    return (
        lax.all_gather(ln_gain, "dp", axis=1, tiled=True),
        lax.all_gather(d_bias, "dp", axis=1, tiled=True),
        lax.all_gather(w_qkv, "dp", axis=0, tiled=True),
        lax.all_gather(w_o, "dp", axis=1, tiled=True),
        lax.all_gather(w_1, "dp", axis=0, tiled=True),
        lax.all_gather(w_2, "dp", axis=1, tiled=True),
    )


def masked_scores(queries, keys_part, valid):
    scores = jnp.einsum(
        "qhd,khd->hqk", queries, keys_part, preferred_element_type=jnp.float32
    ) * HD ** (-0.5)
    return jnp.where(valid[None, None, :] > 0, scores, MASKED)


def attend_forward(bundle):
    packed, valid = bundle
    scores = masked_scores(packed[:, 0], packed[:, 1], valid)
    highest = jnp.max(scores, axis=-1, keepdims=True)
    exponent = jnp.exp(scores - highest)
    denominator = jnp.sum(exponent, axis=-1, keepdims=True)
    attention = (exponent / denominator).astype(jnp.bfloat16)
    mixture = jnp.einsum(
        "hqk,khd->qhd", attention, packed[:, 2], preferred_element_type=jnp.float32
    )
    return (mixture.astype(jnp.bfloat16), (highest + jnp.log(denominator))[..., 0])


def attend_backward(bundle):
    packed, grad_mixture, log_total, valid = bundle
    queries = packed[:, 0]
    keys_part = packed[:, 1]
    values_part = packed[:, 2]
    scores = masked_scores(queries, keys_part, valid)
    attention = jnp.exp(scores - log_total[..., None])
    attention_low = attention.astype(jnp.bfloat16)
    grad_values = jnp.einsum(
        "hqk,qhd->khd", attention_low, grad_mixture, preferred_element_type=jnp.float32
    )
    grad_attention = jnp.einsum(
        "qhd,khd->hqk", grad_mixture, values_part, preferred_element_type=jnp.float32
    )
    inner = jnp.sum(attention * grad_attention, axis=-1, keepdims=True)
    grad_scores = (attention * (grad_attention - inner)).astype(jnp.bfloat16)
    factor = HD ** (-0.5)
    grad_queries = (
        jnp.einsum("hqk,khd->qhd", grad_scores, keys_part, preferred_element_type=jnp.float32)
        * factor
    )
    grad_keys = (
        jnp.einsum("hqk,qhd->khd", grad_scores, queries, preferred_element_type=jnp.float32)
        * factor
    )
    return jnp.stack([grad_queries, grad_keys, grad_values], axis=1)


def body(inputs, valid_mask, cotangent, ln_gain, d_bias, w_qkv, b_qv, w_o, w_1, b_1, w_2):
    local_rows, images, model_width = inputs.shape
    layer = gather_layer(ln_gain, d_bias, w_qkv, w_o, w_1, w_2)
    gains = layer[0].astype(jnp.float32)
    shifts = layer[1].astype(jnp.float32)
    wide_qkv = layer[2].reshape(model_width, -1)
    wide_out = layer[3]
    wide_up = layer[4]
    wide_down = layer[5]
    residual = inputs.astype(jnp.float32)
    normed1 = layer_norm(residual, gains[0], shifts[0]).astype(jnp.bfloat16)
    gathered1 = lax.all_gather(normed1, "tensor", axis=0, tiled=True)
    full_length = gathered1.shape[0]
    columns = b_qv.shape[1]
    heads_local = columns // HD
    projected = jnp.dot(gathered1, wide_qkv, preferred_element_type=jnp.float32).reshape(
        full_length, images, 3, columns
    )
    qkv_bias = jnp.stack([b_qv[0], jnp.zeros_like(b_qv[0]), b_qv[1]]).astype(jnp.float32)
    projected_low = (projected + qkv_bias).astype(jnp.bfloat16)
    per_image = jnp.transpose(projected_low, (1, 0, 2, 3)).reshape(
        images, full_length, 3, heads_local, HD
    )
    mixture, log_total = lax.map(attend_forward, (per_image, valid_mask))
    mixture_seq = jnp.transpose(mixture, (1, 0, 2, 3)).reshape(full_length, images, columns)
    segment = mixture_seq
    attn_sum = lax.psum_scatter(
        jnp.dot(segment, wide_out, preferred_element_type=jnp.float32),
        "tensor",
        scatter_dimension=0,
        tiled=True,
    )
    hidden1 = residual + attn_sum + shifts[2]
    normed2 = layer_norm(hidden1, gains[1], shifts[1]).astype(jnp.bfloat16)
    gathered2 = lax.all_gather(normed2, "tensor", axis=0, tiled=True)
    hidden_in = jnp.dot(gathered2, wide_up, preferred_element_type=jnp.float32) + b_1.astype(
        jnp.float32
    )
    active = gelu_exact(hidden_in).astype(jnp.bfloat16)
    segment = active
    branch_sum = lax.psum_scatter(
        jnp.dot(segment, wide_down, preferred_element_type=jnp.float32).astype(jnp.bfloat16),
        "tensor",
        scatter_dimension=0,
        tiled=True,
    ).astype(jnp.float32)
    block_output = (hidden1 + branch_sum + shifts[3]).astype(jnp.bfloat16)
    layer = gather_layer(ln_gain, d_bias, w_qkv, w_o, w_1, w_2)
    wide_qkv = layer[2].reshape(model_width, -1)
    wide_out = layer[3]
    wide_up = layer[4]
    wide_down = layer[5]
    grad_out = cotangent.astype(jnp.float32)
    grad_gathered = lax.all_gather(cotangent, "tensor", axis=0, tiled=True)
    grad_w_2 = jnp.einsum("sif,sid->fd", active, grad_gathered, preferred_element_type=jnp.float32)
    grad_active = jnp.einsum(
        "sid,fd->sif", grad_gathered, wide_down, preferred_element_type=jnp.float32
    )
    grad_hidden_in = jax.vjp(gelu_exact, hidden_in)[1](grad_active)[0]
    grad_b_1 = jnp.sum(grad_hidden_in, axis=(0, 1))
    grad_hidden_low = grad_hidden_in.astype(jnp.bfloat16)
    grad_w_1 = jnp.einsum(
        "sid,sif->df", gathered2, grad_hidden_low, preferred_element_type=jnp.float32
    )
    segment = grad_hidden_low
    grad_normed2 = lax.psum_scatter(
        jnp.einsum("sif,df->sid", segment, wide_up, preferred_element_type=jnp.float32),
        "tensor",
        scatter_dimension=0,
        tiled=True,
    )
    second_pull = jax.vjp(layer_norm, hidden1, gains[1], shifts[1])[1]
    grad_from_norm, gain2_grad, shift2_grad = second_pull(grad_normed2)
    grad_hidden1 = grad_out + grad_from_norm
    grad_attn_low = grad_hidden1.astype(jnp.bfloat16)
    grad_attn_all = lax.all_gather(grad_attn_low, "tensor", axis=0, tiled=True)
    grad_w_o = jnp.einsum(
        "sic,sid->cd", mixture_seq, grad_attn_all, preferred_element_type=jnp.float32
    )
    grad_mixture = jnp.einsum(
        "sid,cd->sic", grad_attn_all, wide_out, preferred_element_type=jnp.float32
    ).astype(jnp.bfloat16)
    grad_mixture_img = jnp.transpose(
        grad_mixture.reshape(full_length, images, heads_local, HD), (1, 0, 2, 3)
    )
    grad_packed = lax.map(attend_backward, (per_image, grad_mixture_img, log_total, valid_mask))
    grad_projected = jnp.transpose(grad_packed, (1, 0, 2, 3, 4)).reshape(
        full_length, images, 3, columns
    )
    grad_b_qv = jnp.stack(
        [
            jnp.sum(grad_projected[:, :, 0], axis=(0, 1)),
            jnp.sum(grad_projected[:, :, 2], axis=(0, 1)),
        ]
    )
    grad_projected_low = grad_projected.reshape(full_length, images, 3 * columns).astype(
        jnp.bfloat16
    )
    grad_w_qkv = jnp.einsum(
        "sid,sic->dc", gathered1, grad_projected_low, preferred_element_type=jnp.float32
    ).reshape(model_width, 3, columns)
    segment = grad_projected_low
    grad_normed1 = lax.psum_scatter(
        jnp.einsum("sic,dc->sid", segment, wide_qkv, preferred_element_type=jnp.float32).astype(
            jnp.bfloat16
        ),
        "tensor",
        scatter_dimension=0,
        tiled=True,
    ).astype(jnp.float32)
    first_pull = jax.vjp(layer_norm, residual, gains[0], shifts[0])[1]
    grad_from_front, gain1_grad, shift1_grad = first_pull(grad_normed1)
    grad_inputs = grad_hidden1 + grad_from_front
    gain_terms = jnp.stack([gain1_grad, gain2_grad])
    shift_terms = jnp.stack(
        [
            shift1_grad,
            shift2_grad,
            jnp.sum(grad_hidden1, axis=(0, 1)),
            jnp.sum(grad_out, axis=(0, 1)),
        ]
    )
    scattered = (
        lax.psum_scatter(
            gain_terms.astype(jnp.bfloat16), "dp", scatter_dimension=1, tiled=True
        ).astype(jnp.float32),
        lax.psum_scatter(
            shift_terms.astype(jnp.bfloat16), "dp", scatter_dimension=1, tiled=True
        ).astype(jnp.float32),
        lax.psum_scatter(
            grad_w_qkv.astype(jnp.bfloat16), "dp", scatter_dimension=0, tiled=True
        ).astype(jnp.float32),
        lax.psum_scatter(
            grad_w_o.astype(jnp.bfloat16), "dp", scatter_dimension=1, tiled=True
        ).astype(jnp.float32),
        lax.psum_scatter(
            grad_w_1.astype(jnp.bfloat16), "dp", scatter_dimension=0, tiled=True
        ).astype(jnp.float32),
        lax.psum_scatter(
            grad_w_2.astype(jnp.bfloat16), "dp", scatter_dimension=1, tiled=True
        ).astype(jnp.float32),
    )
    gain_sum, shift_sum = lax.psum((scattered[0], scattered[1]), "tensor")
    bias_qv_sum, bias_up_sum = lax.psum((grad_b_qv, grad_b_1), "dp")
    return (
        block_output,
        grad_inputs,
        gain_sum,
        shift_sum,
        scattered[2],
        bias_qv_sum,
        scattered[3],
        scattered[4],
        bias_up_sum,
        scattered[5],
    )


Q = 160
SENT = 152
HALF = 2 * Q
FULL = 4 * Q
BF, F32 = jnp.bfloat16, jnp.float32
MESH = pl.DeviceIdType.MESH


def place(y, x, c, z):
    return (y * 4 + x * 2 + c, z)


def at_rows(start, size, step=8):
    return pl.ds(pl.multiple_of(start, step), size)


def mm(left, right, dims):
    return lax.dot_general(left, right, (dims, ((), ())), preferred_element_type=F32)


NN = ((1,), (0,))
NT = ((1,), (1,))
TN = ((0,), (0,))


class Index:
    def __init__(self, links, key, count, offset=0):
        self.links, self.key, self.count, self.offset = links, key, count, offset

    def __add__(self, more):
        return Index(self.links, self.key, self.count, self.offset + more)

    def place(self, table):
        if self.key not in table:
            table[self.key] = table["next"]
            table["next"] += self.count
        return table[self.key] + self.offset


class Links:
    def __init__(self, send_sem, recv_sem):
        self.send_sem, self.recv_sem = send_sem, recv_sem
        self.sends, self.counts, self.dropped = [], {}, set()
        self.sent_at, self.got_at = {"next": 0}, {"next": 0}

    def base(self, key, count):
        count = self.counts.setdefault(key, count)
        return Index(self, key, count)

    def copy(self, src, dst, sent, got, to):
        return pltpu.make_async_remote_copy(
            src_ref=src,
            dst_ref=dst,
            send_sem=self.send_sem.at[0 if sent is None else sent.place(self.sent_at)],
            recv_sem=self.recv_sem.at[got.place(self.got_at)],
            device_id=to,
            device_id_type=MESH,
        )

    def drop(self, *sent):
        self.dropped = self.dropped | {(one.key, one.offset) for one in sent}

    def each(self, make, act):
        src, dst, sent, got, to, when = make()
        if when is None:
            act(self.copy(src, dst, sent, got, to))
        else:
            pl.when(when)(lambda: act(self.copy(src, dst, sent, got, to)))

    def start(self, make):
        self.sends.append(make)
        self.each(make, lambda copy: copy.start())

    def put(self, src, dst, sent, got, to, when=None):
        self.start(lambda: (src, dst, sent, got, to, when))

    def wait(self, dst, got, to):
        self.copy(dst, dst, None, got, to).wait_recv()

    def finish(self, count=None):
        count = len(self.sends) if count is None else count
        for make in self.sends[:count]:
            sent = make()[2]
            if not (isinstance(sent.offset, int) and (sent.key, sent.offset) in self.dropped):
                self.each(make, lambda copy: copy.wait_send())
        self.sends = self.sends[count:]

    def reuse(self, count, keep):
        self.finish(count)
        assert self.sent_at["next"] <= self.send_sem.shape[0]
        held = {key: self.sent_at[key] for key in keep}
        self.sent_at = dict(held, next=max(held[key] + self.counts[key] for key in keep))


def where_am_i():
    d = lax.axis_index("dp")
    return d // 4, (d // 2) % 2, d % 2, lax.axis_index("tensor")


def greet(y, x, c, z):
    barrier = pltpu.get_barrier_semaphore()
    peers = [(dy, dx, dc, 0) for dy in range(2) for dx in range(2) for dc in range(2) if dy + dx + dc]
    peers += [(0, 0, dc, dz) for dc in range(2) for dz in range(1, 4)]
    for dy, dx, dc, dz in peers:
        to = place((y + dy) % 2, (x + dx) % 2, (c + dc) % 2, (z + dz) % 4)
        pl.semaphore_signal(barrier, inc=1, device_id=to, device_id_type=MESH)
    pl.semaphore_wait(barrier, len(peers))


def unit_rows(v):
    average = jnp.mean(v, axis=-1, keepdims=True)
    centred = v - average
    variance = jnp.mean(centred * centred, axis=-1, keepdims=True)
    scale = lax.rsqrt(variance + EPSILON)
    return centred * scale, scale


def gelu_both(v):
    cdf = 0.5 * (1.0 + lax.erf(v * 0.7071067811865476))
    density = 0.3989422804014327 * jnp.exp(-0.5 * v * v)
    return v * cdf, cdf + v * density


def layer_kernel(
    tok_raw, cot_raw, valid_in, gain_in, shift_in, qv_in, b1_in, qkv_in, wo_in, w1_in, w2_in,
    block_out, grad_out, o_up, o_down, o_qkv, o_wo, bias_all, sums_z,
    tok_in, cot_in, mask_in, norm_in, bias_in,
    tok, cot, mask, norm, bias, qkv, wo, up, down,
    n1, proj, lse, mix, hid, n2, act, slope,
    norm_row, qkv_row, up_row, part, got_part,
    n1_t, ga, gmix, gproj, d_up, d_down, d_qkv, d_wo, r_up, r_down, z_up, z_down, f_up, f_down,
    first_qkv, first_wo, second_qkv, second_wo, z_qkv, z_wo, f_qkv, f_wo,
    s_far, s_mid, s_near, g_far, g_mid, g_near, b_far, b_mid, b_near, g_n1,
    sums, sums_row, sums_got, sums_own, gb1, gbq, gbv, bias_pack, bias_got, bias_own,
    local_sem, send_sem, recv_sem,
):
    y, x, c, z = where_am_i()
    r = y * 2 + x
    links = Links(send_sem, recv_sem)
    early = links.base("rdown", 4)
    early.place(links.sent_at)
    for j in range(2):
        tok[j * Q + SENT : j * Q + Q, :] = jnp.zeros((Q - SENT, 1024), BF)
        for qq in range(4):
            cot[qq * HALF + j * Q + SENT : qq * HALF + j * Q + Q, :] = jnp.zeros((Q - SENT, 1024), BF)
    me = place(y, x, c, z)
    to_c, to_x, to_y = place(y, x, 1 - c, z), place(y, 1 - x, c, z), place(1 - y, x, c, z)
    greet(y, x, c, z)

    block_at = lambda ref, t: ref.at[at_rows(t * HALF, HALF, 64), :]
    block_rows = lambda t, start, size: at_rows(t * HALF + start, size, 32)

    def local(at, src, dst):
        return pltpu.make_async_copy(src, dst, local_sem.at[at])

    z1, z2, z3 = z + 1 - 2 * (z % 2), (z + 2) % 4, 3 - z
    to_z1, to_z2 = place(y, x, c, z1), place(y, x, c, z2)
    r_x, r_y, r_xy = 2 * y + 1 - x, 2 * (1 - y) + x, 3 - r
    q = 2 * x + c
    d = y * 4 + x * 2 + c

    qkv_at = lambda rr, o, cs: qkv.at[at_rows(rr * 256 + cs * 128, 128, 128), at_rows(o * 384, 384, 128)]
    wo_at = lambda rr, o, cs: wo.at[at_rows(o * 128, 128, 128), at_rows(rr * 256 + cs * 128, 128, 128)]
    s_pc = links.base("pc", 2)
    qkv_third = lambda t, cs: qkv_in.at[t, :, at_rows(cs * 128, 128, 128)]
    qkv_spot = lambda t, cs: qkv.at[at_rows(r * 256 + cs * 128, 128, 128), at_rows(z * 384 + t * 128, 128, 128)]
    s_pc3 = links.base("pc3", 3)
    for t in range(3):
        links.put(qkv_third(t, 1 - c), qkv_spot(t, c), s_pc3 + t, s_pc3 + t, to_c)
    links.put(wo_in.at[at_rows((1 - c) * 128, 128, 128), :], wo_at(r, z, c), s_pc + 1, s_pc + 1, to_c)
    own_qkv = [local(at, qkv_third(t, c), qkv_spot(t, c)) for t, at in enumerate((0, 11, 12))]
    own_wo = local(1, wo_in.at[at_rows(c * 128, 128, 128), :], wo_at(r, z, c))
    for one in own_qkv:
        one.start()
    own_wo.start()

    norm_in[0:2, :] = gain_in[...].astype(F32)
    norm_in[2:6, :] = shift_in[...].astype(F32)
    norm_in[6:8, :] = jnp.zeros((2, 128), F32)
    bias_in[0:2, :] = qv_in[:, at_rows(c * 128, 128, 128)].astype(F32)
    bias_in[2:4, :] = jnp.where(q == 0, b1_in[0:2, :], jnp.where(q == 1, b1_in[2:4, :], jnp.where(q == 2, b1_in[4:6, :], b1_in[6:8, :]))).astype(F32)
    bias_in[4:8, :] = jnp.zeros((4, 128), F32)
    length = valid_in.shape[1]
    quarter = length // 4
    source = lax.broadcasted_iota(jnp.int32, (length, FULL), 0)
    target = lax.broadcasted_iota(jnp.int32, (length, FULL), 1)
    chosen = None
    for at in range(4):
        inside = jnp.logical_and(target >= at * Q, target < at * Q + quarter)
        match = jnp.logical_and(inside, target - source == at * (Q - quarter))
        chosen = match if chosen is None else jnp.logical_or(chosen, match)
    spread = mm((valid_in[...] > 0).astype(F32).astype(BF), chosen.astype(F32).astype(BF), NN)
    hidden = jnp.where(spread > 0.5, 0.0, MASKED)
    mask_in[0] = hidden[0:1]
    mask_in[1] = hidden[1:2]
    number = tok_raw.shape[0]
    full_rows = number // 16 * 16
    for one_raw, one_in in ((tok_raw, tok_in), (cot_raw, cot_in)):
        for i in range(2):
            one_in[i, full_rows:Q, :] = jnp.zeros((Q - full_rows, 1024), BF)
            one_in[i, 0:number, :] = one_raw[:, i, :]
    s_norm, s_bias, s_mask = links.base("norm", 8), links.base("bias", 4), links.base("mask", 1)
    for dd in range(1, 8):
        to = place((y + dd // 4) % 2, (x + (dd // 2) % 2) % 2, (c + dd % 2) % 2, z)
        links.put(norm_in, norm.at[d], s_norm + dd, s_norm + dd, to)
    for dz in range(1, 4):
        links.put(bias_in, bias.at[z], s_bias + dz, s_bias + dz, place(y, x, c, (z + dz) % 4))
    links.put(mask_in, mask.at[c], s_mask, s_mask, to_c)
    own_small = (local(2, norm_in, norm.at[d]), local(3, bias_in, bias.at[z]), local(4, mask_in, mask.at[c]))
    for one in own_small:
        one.start()

    def move_tokens(key, source, target_at, at):
        base, got = links.base((key, "sent"), 2), links.base((key, "got"), 2)
        target = target_at(z // 2)
        stay = c == z // 2
        rows = at_rows((z % 2) * Q, SENT, 16)
        for i in range(2):
            here = jnp.logical_and(stay, z % 2 == i)
            to = place(y, x, z // 2, 2 * c + i)
            to = (jnp.where(here, place(y, x, 1 - c, z)[0], to[0]), to[1])
            mine = source.at[i, pl.ds(0, SENT)]
            links.put(mine, target.at[rows], base + i, got + z % 2, to, jnp.logical_not(here))

            @pl.when(here)
            def _(mine=mine):
                local(at, mine, target.at[rows]).start()

    def wait_tokens(key, source, target_at, at):
        got = links.base((key, "got"), 2)
        target = target_at(c)
        stay = c == z // 2
        for j in range(2):
            here = jnp.logical_and(stay, z % 2 == j)

            @pl.when(here)
            def _(j=j):
                local(at, source.at[j, pl.ds(0, SENT)], target.at[pl.ds(j * Q, SENT)]).wait()

            @pl.when(jnp.logical_not(here))
            def _(j=j):
                links.wait(target.at[pl.ds(j * Q, SENT)], got + j, to_c)

    up_shard = lambda sx, sc: up.at[at_rows(y * 512 + sx * 256 + sc * 128, 128, 128), at_rows(z * 256, 256, 128)]
    down_shard = lambda sx, sc: down.at[at_rows(z * 256, 256, 128), at_rows(y * 512 + sx * 256 + sc * 128, 128, 128)]
    s_up, s_down = links.base("up", 4), links.base("down", 4)
    own_up = local(6, w1_in.at[:, at_rows(q * 256, 256, 128)], up_shard(x, c))
    own_down = local(7, w2_in.at[at_rows(q * 256, 256, 128), :], down_shard(x, c))
    own_up.start()
    own_down.start()

    def part_up(dx, dc):
        tx, tc, rel = (x + dx) % 2, (c + dc) % 2, 2 * dx + dc
        to = place(y, tx, tc, z)
        links.put(w1_in.at[:, at_rows((2 * tx + tc) * 256, 256, 128)], up_shard(x, c), s_up + rel, s_up + rel, to)

    def part_down(dx, dc):
        tx, tc, rel = (x + dx) % 2, (c + dc) % 2, 2 * dx + dc
        to = place(y, tx, tc, z)
        links.put(w2_in.at[at_rows((2 * tx + tc) * 256, 256, 128), :], down_shard(x, c), s_down + rel, s_down + rel, to)

    def wait_parts(shard, base):
        for dx, dc in ((0, 1), (1, 0), (1, 1)):
            links.wait(shard((x + dx) % 2, (c + dc) % 2), base + 2 * dx + dc, to_c)

    class Fan:
        def __init__(self, key, piece, arrived):
            self.piece, self.arrived = piece, arrived
            self.many = len(piece(0))
            self.got = [links.base((key, "got", n), 4) for n in range(self.many)]
            self.sent = [links.base((key, "sent", n), 3) for n in range(self.many)]

        def push(self, slot, o, to):
            for n in range(self.many):
                def make(n=n):
                    ref = self.piece(o)[n]
                    return ref, ref, self.sent[n] + slot, self.got[n] + o, to, None

                links.start(make)

        def take(self, o):
            for n, ref in enumerate(self.piece(o)):
                links.wait(ref, self.got[n] + o, to_z1)

        def begin(self):
            self.push(1, z, to_z1)
            self.push(0, z, to_z2)
            self.arrived(z)

        def far(self):
            self.take(z2)
            self.push(2, z2, to_z1)
            self.arrived(z2)

        def pair(self):
            self.take(z1)
            self.arrived(z1)

        def diagonal(self):
            self.take(z3)
            self.arrived(z3)

    class Line:
        def __init__(self, key, piece, arrived):
            self.piece, self.arrived = piece, arrived
            self.many = len(piece(0))
            self.got = [links.base((key, "got", n), 4) for n in range(self.many)]
            self.sent = [links.base((key, "sent", n), 8) for n in range(self.many)]

        def push(self, upward, o, there):
            onward = z < 3 if upward else z > 0
            to = place(y, x, c, jnp.minimum(z + 1, 3) if upward else jnp.maximum(z - 1, 0))
            to = (jnp.where(onward, to[0], to_c[0]), to[1])
            for n, ref in enumerate(self.piece(o)):
                links.put(ref, ref, self.sent[n] + 4 * upward + o, self.got[n] + o, to, jnp.logical_and(there, onward))

        def begin(self):
            self.push(1, z, z >= 0)
            self.push(0, z, z >= 0)
            self.arrived(z, None)

        def step(self, far):
            for upward in (1, 0):
                o = z - far if upward else z + far
                there = o >= 0 if upward else o < 4
                o = jnp.clip(o, 0, 3)

                @pl.when(there)
                def _():
                    for n, ref in enumerate(self.piece(o)):
                        links.wait(ref, self.got[n] + o, to_z1)

                self.push(upward, o, there)
                self.arrived(o, there)

    attn_at = (qkv_at, wo_at)

    def attn_whole(o):
        return (
            qkv.at[at_rows(r * 256, 256, 256), at_rows(o * 384, 384, 128)],
            wo.at[at_rows(o * 128, 128, 128), at_rows(r * 256, 256, 256)],
        )

    s_first = [links.base(("first", n), 8) for n in range(2)]
    s_own = [links.base(("own", n), 8) for n in range(2)]
    s_fwd = [links.base(("fwd", n), 8) for n in range(2)]
    to_first, to_second = (to_x, to_y), (to_y, to_x)
    r_first, r_second = (r_x, r_y), (r_y, r_x)

    def attn_arrived(o, there):
        for n, at in enumerate(attn_at):
            for cs in range(2):
                ref, sem = at(r, o, cs), o * 2 + cs
                links.put(ref, ref, s_first[n] + sem, s_first[n] + sem, to_first[cs], there)
        for n, at in enumerate(attn_at):
            for cs in range(2):
                ref, sem = at(r, o, cs), o * 2 + cs
                links.put(ref, ref, s_own[n] + sem, s_own[n] + sem, to_second[cs], there)

    def attn_forward(o, there=None):
        for n, at in enumerate(attn_at):
            for cs in range(2):
                ref, sem = at(r_first[cs], o, cs), o * 2 + cs

                def arrive(n=n, ref=ref, sem=sem):
                    links.wait(ref, s_first[n] + sem, to_x)

                arrive() if there is None else pl.when(there)(arrive)
                links.put(ref, ref, s_fwd[n] + sem, s_fwd[n] + sem, to_second[cs], there)

    def attn_forward_far(far):
        attn_forward(jnp.clip(z - far, 0, 3), z >= far)
        attn_forward(jnp.clip(z + far, 0, 3), z + far < 4)

    def attn_finish():
        for o in range(4):
            for n, at in enumerate(attn_at):
                for cs in range(2):
                    sem = o * 2 + cs
                    links.wait(at(r_second[cs], o, cs), s_own[n] + sem, to_x)
                    links.wait(at(r_xy, o, cs), s_fwd[n] + sem, to_x)

    attn_line = Line("attn", lambda o: attn_whole(o), attn_arrived)
    up_at = lambda yy, o: up.at[at_rows(yy * 512, 512, 512), at_rows(o * 256, 256, 256)]
    down_at = lambda yy, o: down.at[at_rows(o * 256, 256, 256), at_rows(yy * 512, 512, 512)]
    s_upy, s_downy = links.base("upy", 4), links.base("downy", 4)

    def across(at, base):
        return lambda o: links.start(lambda: (at(y, o), at(y, o), base + o, base + o, to_y, None))

    up_fan = Fan("upf", lambda o: (up_at(y, o),), across(up_at, s_upy))
    down_fan = Fan("downf", lambda o: (down_at(y, o),), across(down_at, s_downy))

    lse[...] = jnp.zeros_like(lse)
    for one in own_qkv:
        one.wait()
    own_wo.wait()
    for t in range(3):
        links.wait(qkv_spot(t, 1 - c), s_pc3 + t, to_c)
    links.wait(wo_at(r, z, 1 - c), s_pc + 1, to_c)
    def spread_start(key, ref):
        base = links.base(("spread", key), 3)
        links.start(lambda: (block_at(ref, q), block_at(ref, q), base, base, to_x, None))
        links.start(lambda: (block_at(ref, q), block_at(ref, q), base + 1, base + 1, to_c, None))

    def spread_forward(key, ref):
        base = links.base(("spread", key), 3)
        far = lambda: block_at(ref, 2 * (1 - x) + c)
        links.wait(far(), base, to_x)
        links.start(lambda: (far(), far(), base + 2, base + 2, to_c, None))

    def spread_wait_near(key, ref):
        links.wait(block_at(ref, 2 * x + 1 - c), links.base(("spread", key), 3) + 1, to_c)

    def spread_wait_far(key, ref):
        links.wait(block_at(ref, 2 * (1 - x) + 1 - c), links.base(("spread", key), 3) + 2, to_c)

    attn_line.begin()
    attn_line.step(1)
    attn_forward(z)
    attn_line.step(2)
    move_tokens("tok", tok_in, lambda cc: tok, 5)
    move_tokens("cot", cot_in, lambda cc: block_at(cot, 2 * x + cc), 8)
    for one in own_small:
        one.wait()
    for dd in range(1, 8):
        source = 4 * ((y + dd // 4) % 2) + 2 * ((x + (dd // 2) % 2) % 2) + (c + dd % 2) % 2
        links.wait(norm.at[source], s_norm + dd, to_c)
    for dz in range(1, 4):
        links.wait(bias.at[(z + 4 - dz) % 4], s_bias + dz, to_c)
    links.wait(mask.at[1 - c], s_mask, to_c)
    for dd in range(8):
        norm_row[:, dd * 128 : dd * 128 + 128] = norm[dd]
    for zz in range(4):
        qkv_row[:, zz * 384 : zz * 384 + 128] = bias[zz, 0:1]
        qkv_row[:, zz * 384 + 128 : zz * 384 + 256] = jnp.zeros((1, 128), F32)
        qkv_row[:, zz * 384 + 256 : zz * 384 + 384] = bias[zz, 1:2]
        up_row[:, zz * 256 : zz * 256 + 128] = bias[zz, 2:3]
        up_row[:, zz * 256 + 128 : zz * 256 + 256] = bias[zz, 3:4]
    attn_forward_far(1)
    attn_line.step(3)
    attn_forward_far(2)
    for dx, dc in ((1, 0), (1, 1), (0, 1)):
        part_up(dx, dc)
    for dx, dc in ((1, 0), (1, 1), (0, 1)):
        part_down(dx, dc)
    own_up.wait()
    own_down.wait()
    wait_tokens("tok", tok_in, lambda cc: tok, 5)

    @pl.loop(0, HALF // 32)
    def _(i):
        v = tok[at_rows(i * 32, 32, 32), :].astype(F32)
        unit, _ = unit_rows(v)
        n1[at_rows(c * HALF + i * 32, 32, 32), :] = (unit * norm_row[0:1] + norm_row[2:3]).astype(BF)

    s_n1 = links.base("n1", 1)
    half_at = lambda ref, cc: ref.at[at_rows(cc * HALF, HALF, 64), :]
    links.put(half_at(n1, c), half_at(n1, c), s_n1, s_n1, to_c)
    attn_forward_far(3)
    wait_parts(up_shard, s_up)
    up_fan.begin()
    wait_parts(down_shard, s_down)
    down_fan.begin()
    links.wait(half_at(n1, 1 - c), s_n1, to_c)
    attn_finish()

    @pl.loop(0, 6)
    def _(j):
        columns = at_rows(j * 256, 256, 256)
        proj[:, columns] = (mm(n1[...], qkv[:, columns], NN) + qkv_row[:, columns]).astype(BF)

    lane = lax.broadcasted_iota(jnp.int32, (1, 128), 1)
    first_head = lane < 64
    zero = jnp.zeros((), BF)

    @pl.loop(0, 4)
    def _(zz):
        keys = proj[:, at_rows(zz * 384 + 128, 128, 128)]
        values = proj[:, at_rows(zz * 384 + 256, 128, 128)]
        hidden_key = mask[z // 2, z % 2]
        for rb in range(2):
            rows = pl.ds(rb * HALF, HALF)
            pair = proj[rows, at_rows(zz * 384, 128, 128)]
            outs = []
            for hh in range(2):
                own = jnp.where(first_head if hh == 0 else jnp.logical_not(first_head), pair, zero)
                scores = mm(own, keys, NT) * (HD ** (-0.5)) + hidden_key
                highest = jnp.max(scores, axis=-1, keepdims=True)
                exponent = jnp.exp(scores - highest)
                total = jnp.sum(exponent, axis=-1, keepdims=True)
                low = (exponent * (1.0 / total)).astype(BF)
                head = 2 * zz + hh
                lse[rows, :] = jnp.where(lane == head, highest + jnp.log(total), lse[rows, :])
                outs.append(mm(low, values, NN))
            mix[rows, at_rows(zz * 128, 128, 128)] = jnp.where(first_head, outs[0], outs[1]).astype(BF)

        @pl.when(zz == 0)
        def _():
            wait_tokens("cot", cot_in, lambda cc: block_at(cot, 2 * x + cc), 8)
            spread_start("cot", cot)

        @pl.when(zz == 1)
        def _():
            up_fan.pair()

    s_part = links.base("part", 1)

    def project_out(cc, target):
        @pl.loop(0, 4)
        def _(j):
            columns = at_rows(j * 256, 256, 256)
            target[:, columns] = mm(mix[at_rows(cc * HALF, HALF, 64), :], wo[:, columns], NN)

    project_out(1 - c, part)
    links.put(part, got_part, s_part, s_part, to_c)
    project_out(c, hid)
    links.wait(got_part, s_part, to_c)

    @pl.loop(0, HALF // 32)
    def _(i):
        rows = at_rows(i * 32, 32, 32)
        v = hid[rows, :] + got_part[rows, :] + tok[rows, :].astype(F32) + norm_row[4:5]
        hid[rows, :] = v
        unit, _ = unit_rows(v)
        n2[block_rows(q, i * 32, 32), :] = (unit * norm_row[1:2] + norm_row[3:4]).astype(BF)

    spread_start("n2", n2)
    up_fan.far()
    down_fan.pair()
    spread_forward("cot", cot)
    spread_wait_near("cot", cot)

    def expand(o, start, blocks):
        columns = at_rows(o * 256, 256, 256)

        @pl.loop(0, blocks)
        def _(i):
            rows = at_rows(start + i * Q, Q, 32)
            v = mm(n2[rows, :], up[:, columns], NN) + up_row[:, columns]
            value, grade = gelu_both(v)
            act[rows, columns] = value.astype(BF)
            slope[rows, columns] = grade.astype(BF)

    n1_t[...] = n1[...].T
    spread_wait_near("n2", n2)
    for at, o in enumerate((z, z1, z2, z3)):
        links.wait(up_at(1 - y, o), s_upy + o, to_y)
        expand(o, 2 * x * HALF, 4)
        if at == 0:
            up_fan.diagonal()
        if at == 2:
            down_fan.far()
    spread_forward("n2", n2)
    for at, o in enumerate((z, z1, z2, z3)):
        expand(o, (2 * (1 - x) + c) * HALF, 2)
    down_fan.diagonal()
    spread_wait_far("n2", n2)
    for o in (z, z1, z2, z3):
        expand(o, (2 * (1 - x) + 1 - c) * HALF, 2)
    spread_wait_far("cot", cot)

    forward_sends = len(links.sends)
    near_other, far_own, far_other = 2 * x + 1 - c, 2 * (1 - x) + c, 2 * (1 - x) + 1 - c
    sums[...] = jnp.zeros_like(sums)
    gb1[...] = jnp.zeros_like(gb1)

    def fold(v):
        return v[0:8] + v[8:16] + v[16:24] + v[24:32]

    def tally(row, v):
        sums[row * 8 : row * 8 + 8, :] += fold(v)

    def send_later(make):
        links.start(make)

    def through_slope(t):
        @pl.loop(0, 4)
        def _(j):
            columns = at_rows(j * 256, 256, 256)
            rows = block_rows(t, 0, HALF)
            v = mm(cot[rows, :], down[columns, :], NT) * slope[rows, columns].astype(F32)
            gb1[:, columns] += jnp.sum(v.reshape(HALF // 8, 8, 256), axis=0)
            slope[rows, columns] = v.astype(BF)

    def back_part(t, target):
        @pl.loop(0, 4)
        def _(j):
            columns = at_rows(j * 256, 256, 256)
            target[:, columns] = mm(slope[block_rows(t, 0, HALF), :], up[columns, :], NT).astype(target.dtype)

    def add_rows(target, *sources):
        @pl.loop(0, HALF // 32)
        def _(i):
            rows = at_rows(i * 32, 32, 32)
            total = sources[0][rows, :].astype(F32)
            for source in sources[1:]:
                total = total + source[rows, :].astype(F32)
            target[rows, :] = total.astype(target.dtype)

    z_order = (z3, z1, z2, z)
    s_rdown, s_rup = links.base("rdown", 4), links.base("rup", 4)
    d_down_at = lambda yy, o: d_down.at[at_rows(o * 256, 256, 256), at_rows(yy * 512, 512, 512)]
    d_up_at = lambda yy, o: d_up.at[at_rows(yy * 512, 512, 512), at_rows(o * 256, 256, 256)]
    r_down_at = lambda o: r_down.at[at_rows(o * 256, 256, 256), :]
    r_up_at = lambda o: r_up.at[:, at_rows(o * 256, 256, 256)]

    def accumulate(target, *sources):
        step = 64 if target.shape[0] % 64 == 0 else 32
        count = target.shape[0] // step

        @pl.loop(0, count)
        def _(i):
            rows = at_rows(i * step, step, step)
            total = target[rows, :].astype(F32)
            for source in sources:
                total = total + source[rows, :].astype(F32)
            target[rows, :] = total.astype(target.dtype)

    class Fold:
        def __init__(self, key, piece, over_z, final):
            self.piece, self.over_z, self.final = piece, over_z, final
            self.sz = links.base((key, "z"), 3)

        def push(self, o, slot, to):
            links.start(lambda: (self.piece(o), self.over_z.at[slot], self.sz + slot, self.sz + slot, to, None))

        def pair_far(self):
            self.collect(z3)
            self.push(z3, 0, to_z1)

        def pair_near(self):
            self.collect(z1)
            self.push(z1, 1, to_z1)

        def far(self):
            self.collect(z2)
            links.wait(self.over_z.at[0], self.sz, to_z1)
            accumulate(self.piece(z2), self.over_z.at[0])
            self.push(z2, 2, to_z2)

        def last(self):
            self.collect(z)
            links.wait(self.over_z.at[1], self.sz + 1, to_z1)
            links.wait(self.over_z.at[2], self.sz + 2, to_z2)
            own, others = self.piece(z), [self.over_z.at[1], self.over_z.at[2]]
            count = own.shape[0] // 64

            @pl.loop(0, count)
            def _(i):
                rows = at_rows(i * 64, 64, 64)
                total = own[rows, :].astype(F32)
                for other in others:
                    total = total + other[rows, :].astype(F32)
                self.final[rows, :] = total.astype(BF)

    class Half(Fold):
        def __init__(self, key, at, got_at, s_got, over_z, final):
            super().__init__(key, lambda o: at(y, o), over_z, final)
            self.got_at, self.s_got = got_at, s_got

        def collect(self, o):
            links.wait(self.got_at(o), self.s_got + o, to_y)
            accumulate(self.piece(o), self.got_at(o))

    half_down = Half("half_down", d_down_at, r_down_at, s_rdown, z_down, f_down)
    half_up = Half("half_up", d_up_at, r_up_at, s_rup, z_up, f_up)

    def give_down(o):
        rows = at_rows(o * 256, 256, 256)
        d_down[rows, :] = mm(act[:, rows], cot[...], TN).astype(BF)
        links.start(lambda: (d_down_at(1 - y, o), r_down_at(o), s_rdown + o, s_rdown + o, to_y, None))

    def give_up(o):
        columns = at_rows(o * 256, 256, 256)
        d_up[:, columns] = mm(n2[...], slope[:, columns], TN).astype(BF)
        links.start(lambda: (d_up_at(1 - y, o), r_up_at(o), s_rup + o, s_rup + o, to_y, None))

    for o in z_order:
        give_down(o)
    for o in range(4):
        links.wait(down_at(1 - y, o), s_downy + o, to_y)
    links.reuse(forward_sends, ("rdown",))

    s_gfar, s_gmid, s_gnear = links.base("gfar", 1), links.base("gmid", 1), links.base("gnear", 1)
    s_bfar, s_bmid, s_bnear = links.base("bfar", 1), links.base("bmid", 1), links.base("bnear", 1)
    through_slope(far_other)
    back_part(far_other, s_far)
    links.put(s_far, g_far, s_gfar, s_gfar, to_c)
    through_slope(far_own)
    back_part(far_own, part)
    links.wait(g_far, s_gfar, to_c)
    add_rows(s_mid, part, g_far)
    links.put(s_mid, g_mid, s_gmid, s_gmid, to_x)
    half_down.pair_far()
    through_slope(near_other)
    back_part(near_other, s_near)
    links.put(s_near, g_near, s_gnear, s_gnear, to_c)
    half_down.pair_near()
    through_slope(q)
    back_part(q, part)
    def down_part(t, target, base=None):
        @pl.loop(0, 4)
        def _(j):
            columns = at_rows(j * 256, 256, 256)
            v = mm(act[block_rows(t, 0, HALF), :], down[:, columns], NN)
            target[:, columns] = (v if base is None else v + base[:, columns]).astype(target.dtype)

    links.copy(s_far, g_far, s_gfar, s_gfar, to_c).wait_send()
    links.drop(s_gfar)
    down_part(far_other, s_far)
    links.put(s_far, b_far, s_bfar, s_bfar, to_c)
    down_part(far_own, got_part)
    half_down.far()
    give_up(z3)
    give_up(z1)
    links.wait(b_far, s_bfar, to_c)
    links.copy(s_mid, g_mid, s_gmid, s_gmid, to_x).wait_send()
    links.drop(s_gmid)
    add_rows(s_mid, got_part, b_far)
    links.put(s_mid, b_mid, s_bmid, s_bmid, to_x)
    give_up(z2)
    give_up(z)

    links.wait(g_near, s_gnear, to_c)
    links.wait(g_mid, s_gmid, to_x)

    @pl.loop(0, HALF // 32)
    def _(i):
        rows = at_rows(i * 32, 32, 32)
        grad = part[rows, :] + g_near[rows, :].astype(F32) + g_mid[rows, :].astype(F32)
        unit, scale = unit_rows(hid[rows, :])
        out = cot[block_rows(q, i * 32, 32), :].astype(F32)
        scaled = grad * norm_row[1:2]
        moved = scale * (
            scaled
            - jnp.mean(scaled, axis=-1, keepdims=True)
            - unit * jnp.mean(scaled * unit, axis=-1, keepdims=True)
        )
        total = out + moved
        tally(1, grad * unit)
        tally(3, grad)
        tally(4, total)
        tally(5, out)
        got_part[rows, :] = total
        ga[at_rows(c * HALF + i * 32, 32, 32), :] = total.astype(BF)

    s_ga = links.base("ga", 1)
    links.put(half_at(ga, c), half_at(ga, c), s_ga, s_ga, to_c)

    links.copy(s_near, g_near, s_gnear, s_gnear, to_c).wait_send()
    links.drop(s_gnear)
    down_part(near_other, s_near)
    links.put(s_near, b_near, s_bnear, s_bnear, to_c)
    down_part(q, hid, hid)
    half_up.pair_far()
    links.wait(half_at(ga, 1 - c), s_ga, to_c)

    @pl.loop(0, 2)
    def _(j):
        columns = at_rows(j * 256, 256, 256)
        gmix[:, columns] = mm(ga[...], wo[columns, :], NT).astype(BF)

    @pl.loop(0, 2)
    def _(j):
        columns = at_rows(j * 256, 256, 256)
        d_wo[columns, :] = mm(mix[:, columns], ga[...], TN).astype(BF)

    d_qkv_at = lambda rr, o, start, size: d_qkv.at[at_rows(rr * 256 + start, size, 32), at_rows(o * 384, 384, 128)]
    d_wo_at = lambda rr, o, start, size: d_wo.at[at_rows(o * 128, 128, 128), at_rows(rr * 256 + start, size, 128)]

    class Reduce(Fold):
        def __init__(self, key, at, parts, first, second, over_z, final):
            super().__init__(key, lambda o: at(r, o, 0, parts[-1][0] + parts[-1][1]), over_z, final)
            self.at, self.parts, self.first, self.second = at, parts, first, second
            self.s1 = [links.base((key, "first", i), 4 * len(parts)) for i in range(2)]
            self.s2 = links.base((key, "second"), 4 * len(parts))

        def block(self, rr, o, p):
            return self.at(rr, o, self.parts[p][0], self.parts[p][1])

        def spot(self, ref, p):
            return cut_of(self, ref, self.parts[p][0], self.parts[p][1])

        def make(self, o, p, i):
            way = self.parts[p][2]
            rr, sem = (r_first[way] if i == 0 else r_xy), self.s1[i] + (len(self.parts) * o + p)
            return self.block(rr, o, p), self.spot(self.first.at[i, o], p), sem, sem, to_first[way], None

        def offer(self, o):
            for p in range(len(self.parts)):
                for i in (1, 0):
                    links.each(functools.partial(self.make, o, p, i), lambda copy: copy.start())

        def promised(self):
            for o in range(4):
                for p in range(len(self.parts)):
                    for i in range(2):
                        links.sends.append(functools.partial(self.make, o, p, i))

        def middle(self, o):
            for p in range(len(self.parts)):
                way = self.parts[p][2]
                got = self.spot(self.first.at[1, o], p)
                links.wait(got, self.s1[1] + (len(self.parts) * o + p), to_x)
                accumulate(self.block(r_second[way], o, p), got)

                def make(p=p, way=way):
                    sem = self.s2 + (len(self.parts) * o + p)
                    return self.block(r_second[way], o, p), self.spot(self.second.at[o], p), sem, sem, to_second[way], None

                links.start(make)

        def collect(self, o):
            for p in range(len(self.parts)):
                links.wait(self.spot(self.first.at[0, o], p), self.s1[0] + (len(self.parts) * o + p), to_x)
                links.wait(self.spot(self.second.at[o], p), self.s2 + (len(self.parts) * o + p), to_x)
            accumulate(self.piece(o), self.first.at[0, o], self.second.at[o])

    def cut_of(owner, ref, start, size):
        return ref.at[pl.ds(start, size), :] if owner.by_rows else ref.at[:, pl.ds(start, size)]

    Reduce.by_rows = True
    red_wo = Reduce("red_wo", d_wo_at, ((0, 256, 0),), first_wo, second_wo, z_wo, f_wo)
    red_wo.by_rows = False
    red_qkv = Reduce("red_qkv", d_qkv_at, ((0, 160, 0), (160, 96, 1)), first_qkv, second_qkv, z_qkv, f_qkv)
    for o in z_order:
        red_wo.offer(o)
    red_wo.promised()

    half_up.pair_near()

    s_oup, s_odown = links.base("oup", 4), links.base("odown", 4)

    def scatter_down():
        for dx, dc in ((1, 0), (1, 1), (0, 1)):
            def make(dx=dx, dc=dc):
                rel, tx, tc = 2 * dx + dc, (x + dx) % 2, (c + dc) % 2
                columns = at_rows((2 * tx + tc) * 128, 128, 128)
                return f_down.at[:, columns], o_down.at[q], s_odown + rel, s_odown + rel, place(y, tx, tc, z), None

            links.start(make)

    def scatter_up():
        for dx, dc in ((1, 0), (1, 1), (0, 1)):
            def make(dx=dx, dc=dc):
                rel, tx, tc = 2 * dx + dc, (x + dx) % 2, (c + dc) % 2
                rows = at_rows((2 * tx + tc) * 128, 128, 128)
                return f_up.at[rows, :], o_up.at[q], s_oup + rel, s_oup + rel, place(y, tx, tc, z), None

            links.start(make)

    def send_home(key, source, target, at):
        base, got = links.base((key, "sent"), 2), links.base((key, "got"), 2)
        for j in range(2):
            def make(j=j):
                here = jnp.logical_and(z // 2 == c, z == 2 * c + j)
                to = place(y, x, z // 2, 2 * c + j)
                to = (jnp.where(here, place(y, x, 1 - c, z)[0], to[0]), to[1])
                return source.at[pl.ds(j * Q, SENT)], target.at[z % 2, pl.ds(0, SENT)], base + j, got + z % 2, to, jnp.logical_not(here)

            links.start(make)

            @pl.when(jnp.logical_and(z // 2 == c, z == 2 * c + j))
            def _(j=j):
                local(at, source.at[pl.ds(j * Q, SENT)], target.at[z % 2, pl.ds(0, SENT)]).start()

    def wait_home(key, source, target, at):
        got = links.base((key, "got"), 2)
        for i in range(2):
            here = jnp.logical_and(z // 2 == c, z % 2 == i)

            @pl.when(here)
            def _(i=i):
                local(at, source.at[pl.ds(0, SENT)], target.at[i, pl.ds(0, SENT)]).wait()

            @pl.when(jnp.logical_not(here))
            def _(i=i):
                links.wait(target.at[i, pl.ds(0, SENT)], got + i, to_c)

    def finish_block():
        links.wait(b_near, s_bnear, to_c)
        links.wait(b_mid, s_bmid, to_x)
        links.copy(s_near, b_near, s_bnear, s_bnear, to_c).wait_send()

        @pl.loop(0, HALF // 32)
        def _(i):
            rows = at_rows(i * 32, 32, 32)
            total = hid[rows, :] + b_near[rows, :].astype(F32) + b_mid[rows, :].astype(F32) + norm_row[5:6]
            s_near[rows, :] = total.astype(BF)

        send_home("block", s_near, block_out, 9)

    links.drop(s_bnear)

    kept = []

    def keep(at, source, target):
        kept.append(local(at, source, target))
        kept[-1].start()

    @pl.loop(0, 4)
    def _(kk):
        zz = 2 * ((z // 2 + 1 - kk % 2) % 2) + (z % 2 + 1 - kk // 2) % 2
        base = zz * 384
        keys = proj[:, at_rows(base + 128, 128, 128)]
        values = proj[:, at_rows(base + 256, 128, 128)]
        hidden_key = mask[z // 2, z % 2]
        d_keys = d_values = None
        sum_queries = None
        for rb in range(2):
            rows = pl.ds(rb * HALF, HALF)
            pair = proj[rows, at_rows(base, 128, 128)]
            grads = gmix[rows, at_rows(zz * 128, 128, 128)]
            outs = []
            for hh in range(2):
                keep = first_head if hh == 0 else jnp.logical_not(first_head)
                own = jnp.where(keep, pair, zero)
                own_grad = jnp.where(keep, grads, zero)
                level = jnp.sum(jnp.where(lane == 2 * zz + hh, lse[rows, :], 0.0), axis=-1, keepdims=True)
                attention = jnp.exp(mm(own, keys, NT) * (HD ** (-0.5)) + hidden_key - level)
                grad_attention = mm(own_grad, values, NT)
                inner = jnp.sum(attention * grad_attention, axis=-1, keepdims=True)
                low = (attention * (grad_attention - inner)).astype(BF)
                more_values = mm(attention.astype(BF), own_grad, TN)
                more_keys = mm(low, own, TN)
                d_values = more_values if d_values is None else d_values + more_values
                d_keys = more_keys if d_keys is None else d_keys + more_keys
                outs.append(mm(low, keys, NN))
            d_queries = jnp.where(first_head, outs[0], outs[1]) * (HD ** (-0.5))
            total = jnp.sum(d_queries.reshape(HALF // 8, 8, 128), axis=0)
            sum_queries = total if sum_queries is None else sum_queries + total
            gproj[rows, at_rows(base, 128, 128)] = d_queries.astype(BF)
        gproj[:, at_rows(base + 128, 128, 128)] = (d_keys * (HD ** (-0.5))).astype(BF)
        gproj[:, at_rows(base + 256, 128, 128)] = d_values.astype(BF)
        gbq[:, at_rows(zz * 128, 128, 128)] = sum_queries
        gbv[:, at_rows(zz * 128, 128, 128)] = jnp.sum(d_values.reshape(FULL // 8, 8, 128), axis=0)

        columns = at_rows(base, 384, 128)
        for rr in range(4):
            rows = pl.ds(rr * 256, 256)
            d_qkv[rows, columns] = mm(n1_t[rows, :], gproj[:, columns], NN).astype(BF)
        red_qkv.offer(zz)

        @pl.when(kk == 0)
        def _():
            finish_block()

        @pl.when(kk == 1)
        def _():
            half_up.far()

        @pl.when(kk == 2)
        def _():
            red_qkv.middle(z3)

        @pl.when(kk == 3)
        def _():
            for o in z_order:
                red_wo.middle(o)

    red_qkv.promised()
    for zz in range(4):
        flat = lambda ref, start: jnp.sum(ref[:, start : start + 128], axis=0, keepdims=True)
        bias_pack[zz, 0:1] = flat(gbq, zz * 128)
        bias_pack[zz, 1:2] = flat(gbv, zz * 128)
        bias_pack[zz, 2:3] = flat(gb1, zz * 256)
        bias_pack[zz, 3:4] = flat(gb1, zz * 256 + 128)
        bias_pack[zz, 4:8] = jnp.zeros((4, 128), F32)
    s_bz, s_ball = links.base("bz", 4), links.base("ball", 8)
    for dz in range(1, 4):
        def make(dz=dz):
            tz = (z + dz) % 4
            return bias_pack.at[tz], bias_got.at[dz], s_bz + dz, s_bz + dz, place(y, x, c, tz), None

        links.start(make)

    def front_part(cc, target):
        @pl.loop(0, 4)
        def _(j):
            columns = at_rows(j * 256, 256, 256)
            target[:, columns] = mm(gproj[at_rows(cc * HALF, HALF, 64), :], qkv[columns, :], NT).astype(target.dtype)

    s_gn1 = links.base("gn1", 1)
    links.copy(s_far, b_far, s_bfar, s_bfar, to_c).wait_send()
    links.drop(s_bfar)
    front_part(1 - c, s_far)
    links.put(s_far, g_n1, s_gn1, s_gn1, to_c)
    front_part(c, part)
    for o in (z1, z2):
        red_qkv.middle(o)
    red_qkv.pair_far()
    links.wait(g_n1, s_gn1, to_c)
    links.copy(s_mid, b_mid, s_bmid, s_bmid, to_x).wait_send()
    links.drop(s_bmid)

    @pl.loop(0, HALF // 32)
    def _(i):
        rows = at_rows(i * 32, 32, 32)
        grad = part[rows, :] + g_n1[rows, :].astype(F32)
        unit, scale = unit_rows(tok[rows, :].astype(F32))
        scaled = grad * norm_row[0:1]
        moved = scale * (
            scaled
            - jnp.mean(scaled, axis=-1, keepdims=True)
            - unit * jnp.mean(scaled * unit, axis=-1, keepdims=True)
        )
        tally(0, grad * unit)
        tally(2, grad)
        s_mid[rows, :] = (got_part[rows, :] + moved).astype(BF)

    for row in range(6):
        sums_row[row : row + 1, :] = jnp.sum(sums[row * 8 : row * 8 + 8, :], axis=0, keepdims=True)
    sums_row[6:8, :] = jnp.zeros((2, 1024), F32)
    for dd in range(8):
        norm[dd] = sums_row[:, dd * 128 : dd * 128 + 128]
    s_sum, s_sumz = links.base("sum", 8), links.base("sumz", 4)
    for dd in range(1, 8):
        def make(dd=dd):
            ty, tx, tc = (y + dd // 4) % 2, (x + (dd // 2) % 2) % 2, (c + dd % 2) % 2
            return norm.at[4 * ty + 2 * tx + tc], sums_got.at[dd], s_sum + dd, s_sum + dd, place(ty, tx, tc, z), None

        links.start(make)
    send_home("home", s_mid, grad_out, 10)
    red_qkv.pair_near()
    red_qkv.middle(z)
    red_qkv.far()
    red_wo.pair_far()
    red_wo.pair_near()
    red_wo.far()
    half_down.last()
    scatter_down()
    keep(17, f_down.at[:, at_rows(q * 128, 128, 128)], o_down.at[q])
    half_up.last()
    scatter_up()
    keep(18, f_up.at[at_rows(q * 128, 128, 128), :], o_up.at[q])
    for dz in range(1, 4):
        links.wait(bias_got.at[dz], s_bz + dz, to_c)
    bias_own[...] = bias_pack[z] + bias_got[1] + bias_got[2] + bias_got[3]
    keep(13, bias_own, bias_all.at[d])
    for dd in range(1, 8):
        def make(dd=dd):
            to = place((y + dd // 4) % 2, (x + (dd // 2) % 2) % 2, (c + dd % 2) % 2, z)
            return bias_own, bias_all.at[d], s_ball + dd, s_ball + dd, to, None

        links.start(make)
    for dd in range(1, 8):
        links.wait(sums_got.at[dd], s_sum + dd, to_c)
    total = norm[d]
    for dd in range(1, 8):
        total = total + sums_got[dd]
    sums_own[...] = total
    keep(14, sums_own, sums_z.at[0])
    for dz in range(1, 4):
        def make(dz=dz):
            return sums_own, sums_z.at[dz], s_sumz + dz, s_sumz + dz, place(y, x, c, (z + dz) % 4), None

        links.start(make)
    red_wo.last()
    s_owo = links.base("owo", 1)
    links.put(f_wo.at[:, at_rows((1 - c) * 128, 128, 128)], o_wo.at[c], s_owo, s_owo, to_c)
    keep(16, f_wo.at[:, at_rows(c * 128, 128, 128)], o_wo.at[c])

    for dx, dc in ((1, 0), (1, 1), (0, 1)):
        rel, source = 2 * dx + dc, 2 * ((x + dx) % 2) + (c + dc) % 2
        links.wait(o_up.at[source], s_oup + rel, to_c)
        links.wait(o_down.at[source], s_odown + rel, to_c)

    for dd in range(1, 8):
        source = 4 * ((y + dd // 4) % 2) + 2 * ((x + (dd // 2) % 2) % 2) + (c + dd % 2) % 2
        links.wait(bias_all.at[source], s_ball + dd, to_c)
    for dz in range(1, 4):
        links.wait(sums_z.at[dz], s_sumz + dz, to_c)

    red_qkv.last()
    s_oqkv, s_owo = links.base("oqkv", 1), links.base("owo", 1)
    links.put(f_qkv.at[at_rows((1 - c) * 128, 128, 128), :], o_qkv.at[c], s_oqkv, s_oqkv, to_c)
    keep(15, f_qkv.at[at_rows(c * 128, 128, 128), :], o_qkv.at[c])
    links.wait(o_qkv.at[1 - c], s_oqkv, to_c)
    links.wait(o_wo.at[1 - c], s_owo, to_c)
    wait_home("block", s_near, block_out, 9)
    wait_home("home", s_mid, grad_out, 10)
    for one in kept:
        one.wait()
    links.finish()
    assert links.got_at["next"] <= recv_sem.shape[0]
    assert links.sent_at["next"] <= send_sem.shape[0]


def layer_call(*operands):
    shape = jax.ShapeDtypeStruct
    hbm, vmem = pl.BlockSpec(memory_space=pl.ANY), pl.BlockSpec(memory_space=pltpu.VMEM)
    outs = [
        shape((2, Q, 1024), BF), shape((2, Q, 1024), BF), shape((4, 128, 256), BF), shape((4, 256, 128), BF),
        shape((2, 128, 384), BF), shape((2, 128, 128), BF), shape((8, 8, 128), F32), shape((4, 8, 128), F32),
    ]
    low = lambda *dims: pltpu.VMEM(dims, BF)
    wide = lambda *dims: pltpu.VMEM(dims, F32)
    scratch = [
        low(2, Q, 1024), low(2, Q, 1024), wide(2, 1, FULL), wide(8, 128), wide(8, 128),
        low(HALF, 1024), low(4 * HALF, 1024), wide(2, 2, 1, FULL), wide(8, 8, 128), wide(4, 8, 128),
        low(1024, 1536), low(512, 1024), low(1024, 1024), low(1024, 1024),
        low(FULL, 1024), low(FULL, 1536), wide(FULL, 128), low(FULL, 512), wide(HALF, 1024),
        low(4 * HALF, 1024), low(4 * HALF, 1024), low(4 * HALF, 1024),
        wide(8, 1024), wide(1, 1536), wide(1, 1024), wide(HALF, 1024), wide(HALF, 1024),
        low(1024, FULL), low(FULL, 1024), low(FULL, 512), low(FULL, 1536),
        low(1024, 1024), low(1024, 1024), low(1024, 1536), low(512, 1024),
        low(512, 1024), low(1024, 512), low(3, 512, 256), low(3, 256, 512),
        low(512, 256), low(256, 512),
        low(2, 4, 256, 384), low(2, 4, 128, 256), low(4, 256, 384), low(4, 128, 256),
        low(3, 256, 384), low(3, 128, 256), low(256, 384), low(128, 256),
        *[low(HALF, 1024)] * 10,
        wide(48, 1024), wide(8, 1024), wide(8, 8, 128), wide(8, 128),
        wide(8, 1024), wide(8, 512), wide(8, 512), wide(4, 8, 128), wide(4, 8, 128), wide(8, 128),
        pltpu.SemaphoreType.DMA((19,)), pltpu.SemaphoreType.DMA((130,)), pltpu.SemaphoreType.DMA((212,)),
    ]
    return pl.pallas_call(
        layer_kernel,
        out_shape=outs,
        in_specs=[vmem] * 7 + [hbm] * 4,
        out_specs=[hbm] * 8,
        scratch_shapes=scratch,
        compiler_params=pltpu.CompilerParams(collective_id=0, has_side_effects=True, vmem_limit_bytes=67043328),
        name="layer",
    )(*operands)


def finish_kernel(
    block_in, grad_in, up_in, down_in, qkv_in, wo_in, bias_in, sums_in,
    block, grad, gain, shift, qkv, qv, wo, w1, b1, w2,
):
    rows = grad.shape[0]
    for i in range(2):
        grad[:, i, :] = grad_in[i, 0:rows, :].astype(F32)
    block[...] = jnp.stack([block_in[0, 0:rows, :], block_in[1, 0:rows, :]], axis=1)
    total = sums_in[0] + sums_in[1] + sums_in[2] + sums_in[3]
    gain[...] = total[0:2]
    shift[...] = total[2:6]
    for cc in range(2):
        lanes = pl.ds(cc * 128, 128)
        for t in range(3):
            qkv[t, :, lanes] = qkv_in[cc, :, t * 128 : t * 128 + 128].astype(F32)
        qv[:, lanes] = (bias_in[cc] + bias_in[2 + cc] + bias_in[4 + cc] + bias_in[6 + cc])[0:2]
        wo[pl.ds(cc * 128, 128), :] = wo_in[cc].astype(F32)
    for qq in range(4):
        w1[:, pl.ds(qq * 256, 256)] = up_in[qq].astype(F32)
        w2[pl.ds(qq * 256, 256), :] = down_in[qq].astype(F32)
        b1[pl.ds(qq * 2, 2), :] = (bias_in[qq] + bias_in[4 + qq])[2:4]


def finish_call(rows, *parts):
    shape = jax.ShapeDtypeStruct
    return pl.pallas_call(
        finish_kernel,
        out_shape=[
            shape((rows, 2, 1024), BF), shape((rows, 2, 1024), F32), shape((2, 128), F32), shape((4, 128), F32),
            shape((3, 128, 256), F32), shape((2, 256), F32), shape((256, 128), F32), shape((128, 1024), F32),
            shape((8, 128), F32), shape((1024, 128), F32),
        ],
        in_specs=[pl.BlockSpec(memory_space=pltpu.VMEM)] * 8,
        out_specs=[pl.BlockSpec(memory_space=pltpu.VMEM)] * 10,
        name="finish",
    )(*parts)


def fast_body(inputs, valid_mask, cotangent, ln_gain, d_bias, w_qkv, b_qv, w_o, w_1, b_1, w_2):
    rows = inputs.shape[0]
    parts = layer_call(
        inputs, cotangent, valid_mask, ln_gain, d_bias, b_qv, b_1.reshape(8, 128),
        jnp.transpose(w_qkv, (1, 0, 2)), w_o, w_1, w_2,
    )
    block, grad, gain, shift, qkv, qv, wo, w1, b1, w2 = finish_call(rows, *parts)
    return block, grad, gain, shift, jnp.transpose(qkv, (1, 0, 2)), qv, wo, w1, b1.reshape(1024), w2


def solution(mesh):
    in_specs = (
        P("tensor", "dp", None),
        P("dp", None),
        P("tensor", "dp", None),
        P(None, "dp"),
        P(None, "dp"),
        P("dp", None, "tensor"),
        P(None, "tensor"),
        P("tensor", "dp"),
        P("dp", "tensor"),
        P("tensor"),
        P("tensor", "dp"),
    )
    out_specs = (
        P("tensor", "dp", None),
        P("tensor", "dp", None),
        P(None, "dp"),
        P(None, "dp"),
        P("dp", None, "tensor"),
        P(None, "tensor"),
        P("tensor", "dp"),
        P("dp", "tensor"),
        P("tensor"),
        P("tensor", "dp"),
    )
    run = fast_body if dict(mesh.shape) == {"dp": 8, "tensor": 4} else body
    return jax.shard_map(run, mesh=mesh, in_specs=in_specs, out_specs=out_specs, check_vma=False)
```

```python
import functools

import jax
import jax.numpy as jnp
from jax import lax
from jax.experimental import pallas as pl
from jax.experimental.pallas import tpu as pltpu
from jax.sharding import PartitionSpec as P

HD = 64


EPSILON = 1e-06
MASKED = -1e30


def layer_norm(values, gain, shift):
    average = jnp.mean(values, axis=-1, keepdims=True)
    centred = values - average
    variance = jnp.mean(centred * centred, axis=-1, keepdims=True)
    return centred * lax.rsqrt(variance + EPSILON) * gain + shift


def gelu_exact(values):
    return jax.nn.gelu(values, approximate=False)


def gather_layer(ln_gain, d_bias, w_qkv, w_o, w_1, w_2):
    return (
        lax.all_gather(ln_gain, "dp", axis=1, tiled=True),
        lax.all_gather(d_bias, "dp", axis=1, tiled=True),
        lax.all_gather(w_qkv, "dp", axis=0, tiled=True),
        lax.all_gather(w_o, "dp", axis=1, tiled=True),
        lax.all_gather(w_1, "dp", axis=0, tiled=True),
        lax.all_gather(w_2, "dp", axis=1, tiled=True),
    )


def masked_scores(queries, keys_part, valid):
    scores = jnp.einsum(
        "qhd,khd->hqk", queries, keys_part, preferred_element_type=jnp.float32
    ) * HD ** (-0.5)
    return jnp.where(valid[None, None, :] > 0, scores, MASKED)


def attend_forward(bundle):
    packed, valid = bundle
    scores = masked_scores(packed[:, 0], packed[:, 1], valid)
    highest = jnp.max(scores, axis=-1, keepdims=True)
    exponent = jnp.exp(scores - highest)
    denominator = jnp.sum(exponent, axis=-1, keepdims=True)
    attention = (exponent / denominator).astype(jnp.bfloat16)
    mixture = jnp.einsum(
        "hqk,khd->qhd", attention, packed[:, 2], preferred_element_type=jnp.float32
    )
    return (mixture.astype(jnp.bfloat16), (highest + jnp.log(denominator))[..., 0])


def attend_backward(bundle):
    packed, grad_mixture, log_total, valid = bundle
    queries = packed[:, 0]
    keys_part = packed[:, 1]
    values_part = packed[:, 2]
    scores = masked_scores(queries, keys_part, valid)
    attention = jnp.exp(scores - log_total[..., None])
    attention_low = attention.astype(jnp.bfloat16)
    grad_values = jnp.einsum(
        "hqk,qhd->khd", attention_low, grad_mixture, preferred_element_type=jnp.float32
    )
    grad_attention = jnp.einsum(
        "qhd,khd->hqk", grad_mixture, values_part, preferred_element_type=jnp.float32
    )
    inner = jnp.sum(attention * grad_attention, axis=-1, keepdims=True)
    grad_scores = (attention * (grad_attention - inner)).astype(jnp.bfloat16)
    factor = HD ** (-0.5)
    grad_queries = (
        jnp.einsum("hqk,khd->qhd", grad_scores, keys_part, preferred_element_type=jnp.float32)
        * factor
    )
    grad_keys = (
        jnp.einsum("hqk,qhd->khd", grad_scores, queries, preferred_element_type=jnp.float32)
        * factor
    )
    return jnp.stack([grad_queries, grad_keys, grad_values], axis=1)


def body(inputs, valid_mask, cotangent, ln_gain, d_bias, w_qkv, b_qv, w_o, w_1, b_1, w_2):
    local_rows, images, model_width = inputs.shape
    layer = gather_layer(ln_gain, d_bias, w_qkv, w_o, w_1, w_2)
    gains = layer[0].astype(jnp.float32)
    shifts = layer[1].astype(jnp.float32)
    wide_qkv = layer[2].reshape(model_width, -1)
    wide_out = layer[3]
    wide_up = layer[4]
    wide_down = layer[5]
    residual = inputs.astype(jnp.float32)
    normed1 = layer_norm(residual, gains[0], shifts[0]).astype(jnp.bfloat16)
    gathered1 = lax.all_gather(normed1, "tensor", axis=0, tiled=True)
    full_length = gathered1.shape[0]
    columns = b_qv.shape[1]
    heads_local = columns // HD
    projected = jnp.dot(gathered1, wide_qkv, preferred_element_type=jnp.float32).reshape(
        full_length, images, 3, columns
    )
    qkv_bias = jnp.stack([b_qv[0], jnp.zeros_like(b_qv[0]), b_qv[1]]).astype(jnp.float32)
    projected_low = (projected + qkv_bias).astype(jnp.bfloat16)
    per_image = jnp.transpose(projected_low, (1, 0, 2, 3)).reshape(
        images, full_length, 3, heads_local, HD
    )
    mixture, log_total = lax.map(attend_forward, (per_image, valid_mask))
    mixture_seq = jnp.transpose(mixture, (1, 0, 2, 3)).reshape(full_length, images, columns)
    segment = mixture_seq
    attn_sum = lax.psum_scatter(
        jnp.dot(segment, wide_out, preferred_element_type=jnp.float32),
        "tensor",
        scatter_dimension=0,
        tiled=True,
    )
    hidden1 = residual + attn_sum + shifts[2]
    normed2 = layer_norm(hidden1, gains[1], shifts[1]).astype(jnp.bfloat16)
    gathered2 = lax.all_gather(normed2, "tensor", axis=0, tiled=True)
    hidden_in = jnp.dot(gathered2, wide_up, preferred_element_type=jnp.float32) + b_1.astype(
        jnp.float32
    )
    active = gelu_exact(hidden_in).astype(jnp.bfloat16)
    segment = active
    branch_sum = lax.psum_scatter(
        jnp.dot(segment, wide_down, preferred_element_type=jnp.float32).astype(jnp.bfloat16),
        "tensor",
        scatter_dimension=0,
        tiled=True,
    ).astype(jnp.float32)
    block_output = (hidden1 + branch_sum + shifts[3]).astype(jnp.bfloat16)
    layer = gather_layer(ln_gain, d_bias, w_qkv, w_o, w_1, w_2)
    wide_qkv = layer[2].reshape(model_width, -1)
    wide_out = layer[3]
    wide_up = layer[4]
    wide_down = layer[5]
    grad_out = cotangent.astype(jnp.float32)
    grad_gathered = lax.all_gather(cotangent, "tensor", axis=0, tiled=True)
    grad_w_2 = jnp.einsum("sif,sid->fd", active, grad_gathered, preferred_element_type=jnp.float32)
    grad_active = jnp.einsum(
        "sid,fd->sif", grad_gathered, wide_down, preferred_element_type=jnp.float32
    )
    grad_hidden_in = jax.vjp(gelu_exact, hidden_in)[1](grad_active)[0]
    grad_b_1 = jnp.sum(grad_hidden_in, axis=(0, 1))
    grad_hidden_low = grad_hidden_in.astype(jnp.bfloat16)
    grad_w_1 = jnp.einsum(
        "sid,sif->df", gathered2, grad_hidden_low, preferred_element_type=jnp.float32
    )
    segment = grad_hidden_low
    grad_normed2 = lax.psum_scatter(
        jnp.einsum("sif,df->sid", segment, wide_up, preferred_element_type=jnp.float32),
        "tensor",
        scatter_dimension=0,
        tiled=True,
    )
    second_pull = jax.vjp(layer_norm, hidden1, gains[1], shifts[1])[1]
    grad_from_norm, gain2_grad, shift2_grad = second_pull(grad_normed2)
    grad_hidden1 = grad_out + grad_from_norm
    grad_attn_low = grad_hidden1.astype(jnp.bfloat16)
    grad_attn_all = lax.all_gather(grad_attn_low, "tensor", axis=0, tiled=True)
    grad_w_o = jnp.einsum(
        "sic,sid->cd", mixture_seq, grad_attn_all, preferred_element_type=jnp.float32
    )
    grad_mixture = jnp.einsum(
        "sid,cd->sic", grad_attn_all, wide_out, preferred_element_type=jnp.float32
    ).astype(jnp.bfloat16)
    grad_mixture_img = jnp.transpose(
        grad_mixture.reshape(full_length, images, heads_local, HD), (1, 0, 2, 3)
    )
    grad_packed = lax.map(attend_backward, (per_image, grad_mixture_img, log_total, valid_mask))
    grad_projected = jnp.transpose(grad_packed, (1, 0, 2, 3, 4)).reshape(
        full_length, images, 3, columns
    )
    grad_b_qv = jnp.stack(
        [
            jnp.sum(grad_projected[:, :, 0], axis=(0, 1)),
            jnp.sum(grad_projected[:, :, 2], axis=(0, 1)),
        ]
    )
    grad_projected_low = grad_projected.reshape(full_length, images, 3 * columns).astype(
        jnp.bfloat16
    )
    grad_w_qkv = jnp.einsum(
        "sid,sic->dc", gathered1, grad_projected_low, preferred_element_type=jnp.float32
    ).reshape(model_width, 3, columns)
    segment = grad_projected_low
    grad_normed1 = lax.psum_scatter(
        jnp.einsum("sic,dc->sid", segment, wide_qkv, preferred_element_type=jnp.float32).astype(
            jnp.bfloat16
        ),
        "tensor",
        scatter_dimension=0,
        tiled=True,
    ).astype(jnp.float32)
    first_pull = jax.vjp(layer_norm, residual, gains[0], shifts[0])[1]
    grad_from_front, gain1_grad, shift1_grad = first_pull(grad_normed1)
    grad_inputs = grad_hidden1 + grad_from_front
    gain_terms = jnp.stack([gain1_grad, gain2_grad])
    shift_terms = jnp.stack(
        [
            shift1_grad,
            shift2_grad,
            jnp.sum(grad_hidden1, axis=(0, 1)),
            jnp.sum(grad_out, axis=(0, 1)),
        ]
    )
    scattered = (
        lax.psum_scatter(
            gain_terms.astype(jnp.bfloat16), "dp", scatter_dimension=1, tiled=True
        ).astype(jnp.float32),
        lax.psum_scatter(
            shift_terms.astype(jnp.bfloat16), "dp", scatter_dimension=1, tiled=True
        ).astype(jnp.float32),
        lax.psum_scatter(
            grad_w_qkv.astype(jnp.bfloat16), "dp", scatter_dimension=0, tiled=True
        ).astype(jnp.float32),
        lax.psum_scatter(
            grad_w_o.astype(jnp.bfloat16), "dp", scatter_dimension=1, tiled=True
        ).astype(jnp.float32),
        lax.psum_scatter(
            grad_w_1.astype(jnp.bfloat16), "dp", scatter_dimension=0, tiled=True
        ).astype(jnp.float32),
        lax.psum_scatter(
            grad_w_2.astype(jnp.bfloat16), "dp", scatter_dimension=1, tiled=True
        ).astype(jnp.float32),
    )
    gain_sum, shift_sum = lax.psum((scattered[0], scattered[1]), "tensor")
    bias_qv_sum, bias_up_sum = lax.psum((grad_b_qv, grad_b_1), "dp")
    return (
        block_output,
        grad_inputs,
        gain_sum,
        shift_sum,
        scattered[2],
        bias_qv_sum,
        scattered[3],
        scattered[4],
        bias_up_sum,
        scattered[5],
    )


Q = 160
SENT = 152
HALF = 2 * Q
FULL = 4 * Q
BF, F32 = jnp.bfloat16, jnp.float32
MESH = pl.DeviceIdType.MESH


def place(y, x, c, z):
    return (y * 4 + x * 2 + c, z)


def at_rows(start, size, step=8):
    return pl.ds(pl.multiple_of(start, step), size)


def mm(left, right, dims):
    return lax.dot_general(left, right, (dims, ((), ())), preferred_element_type=F32)


NN = ((1,), (0,))
NT = ((1,), (1,))
TN = ((0,), (0,))


class Index:
    def __init__(self, links, key, count, offset=0):
        self.links, self.key, self.count, self.offset = links, key, count, offset

    def __add__(self, more):
        return Index(self.links, self.key, self.count, self.offset + more)

    def place(self, table):
        if self.key not in table:
            table[self.key] = table["next"]
            table["next"] += self.count
        return table[self.key] + self.offset


class Links:
    def __init__(self, send_sem, recv_sem):
        self.send_sem, self.recv_sem = send_sem, recv_sem
        self.sends, self.counts, self.dropped = [], {}, set()
        self.sent_at, self.got_at = {"next": 0}, {"next": 0}

    def base(self, key, count):
        count = self.counts.setdefault(key, count)
        return Index(self, key, count)

    def copy(self, src, dst, sent, got, to):
        return pltpu.make_async_remote_copy(
            src_ref=src,
            dst_ref=dst,
            send_sem=self.send_sem.at[0 if sent is None else sent.place(self.sent_at)],
            recv_sem=self.recv_sem.at[got.place(self.got_at)],
            device_id=to,
            device_id_type=MESH,
        )

    def drop(self, *sent):
        self.dropped = self.dropped | {(one.key, one.offset) for one in sent}

    def each(self, make, act):
        src, dst, sent, got, to, when = make()
        if when is None:
            act(self.copy(src, dst, sent, got, to))
        else:
            pl.when(when)(lambda: act(self.copy(src, dst, sent, got, to)))

    def start(self, make):
        self.sends.append(make)
        self.each(make, lambda copy: copy.start())

    def put(self, src, dst, sent, got, to, when=None):
        self.start(lambda: (src, dst, sent, got, to, when))

    def wait(self, dst, got, to):
        self.copy(dst, dst, None, got, to).wait_recv()

    def finish(self, count=None):
        count = len(self.sends) if count is None else count
        for make in self.sends[:count]:
            sent = make()[2]
            if not (isinstance(sent.offset, int) and (sent.key, sent.offset) in self.dropped):
                self.each(make, lambda copy: copy.wait_send())
        self.sends = self.sends[count:]

    def reuse(self, count, keep):
        self.finish(count)
        assert self.sent_at["next"] <= self.send_sem.shape[0]
        held = {key: self.sent_at[key] for key in keep}
        self.sent_at = dict(held, next=max(held[key] + self.counts[key] for key in keep))


def where_am_i():
    d = lax.axis_index("dp")
    return d // 4, (d // 2) % 2, d % 2, lax.axis_index("tensor")


def greet(y, x, c, z):
    barrier = pltpu.get_barrier_semaphore()
    peers = [(dy, dx, dc, 0) for dy in range(2) for dx in range(2) for dc in range(2) if dy + dx + dc]
    peers += [(0, 0, dc, dz) for dc in range(2) for dz in range(1, 4)]
    for dy, dx, dc, dz in peers:
        to = place((y + dy) % 2, (x + dx) % 2, (c + dc) % 2, (z + dz) % 4)
        pl.semaphore_signal(barrier, inc=1, device_id=to, device_id_type=MESH)
    pl.semaphore_wait(barrier, len(peers))


def unit_rows(v):
    average = jnp.mean(v, axis=-1, keepdims=True)
    centred = v - average
    variance = jnp.mean(centred * centred, axis=-1, keepdims=True)
    scale = lax.rsqrt(variance + EPSILON)
    return centred * scale, scale


def gelu_both(v):
    cdf = 0.5 * (1.0 + lax.erf(v * 0.7071067811865476))
    density = 0.3989422804014327 * jnp.exp(-0.5 * v * v)
    return v * cdf, cdf + v * density


def layer_kernel(
    tok_src, cot_src, valid_in, gain_in, shift_in, qv_in, b1_in, qkv_in, wo_in, w1_in, w2_in,
    block_out, grad_out, o_up, o_down, o_qkv, o_wo, bias_all, sums_z,
    tok_raw, cot_raw, tok_in, cot_in, mask_in, norm_in, bias_in,
    tok, cot, mask, norm, bias, qkv, wo, up, down,
    n1, proj, lse, mix, hid, n2, act, slope,
    norm_row, qkv_row, up_row, part, got_part,
    n1_t, ga, gmix, gproj, d_up, d_down, d_qkv, d_wo, r_up, r_down, z_up, z_down, f_up, f_down,
    first_qkv, first_wo, second_qkv, second_wo, z_qkv, z_wo, f_qkv, f_wo,
    s_far, s_mid, s_near, g_far, g_mid, g_near, b_far, b_mid, b_near, g_n1,
    sums, sums_row, sums_got, sums_own, gb1, gbq, gbv, bias_pack, bias_got, bias_own,
    local_sem, send_sem, recv_sem,
):
    y, x, c, z = where_am_i()
    r = y * 2 + x
    links = Links(send_sem, recv_sem)
    early = links.base("rdown", 4)
    early.place(links.sent_at)
    for j in range(2):
        tok[j * Q + SENT : j * Q + Q, :] = jnp.zeros((Q - SENT, 1024), BF)
        for qq in range(4):
            cot[qq * HALF + j * Q + SENT : qq * HALF + j * Q + Q, :] = jnp.zeros((Q - SENT, 1024), BF)
    me = place(y, x, c, z)
    to_c, to_x, to_y = place(y, x, 1 - c, z), place(y, 1 - x, c, z), place(1 - y, x, c, z)
    raw_copies = [
        pltpu.make_async_copy(source, target, local_sem.at[at])
        for source, target, at in ((tok_src, tok_raw, 19), (cot_src, cot_raw, 20))
    ]
    for one in raw_copies:
        one.start()
    greet(y, x, c, z)

    block_at = lambda ref, t: ref.at[at_rows(t * HALF, HALF, 64), :]
    block_rows = lambda t, start, size: at_rows(t * HALF + start, size, 32)

    def local(at, src, dst):
        return pltpu.make_async_copy(src, dst, local_sem.at[at])

    z1, z2, z3 = z + 1 - 2 * (z % 2), (z + 2) % 4, 3 - z
    to_z1, to_z2 = place(y, x, c, z1), place(y, x, c, z2)
    r_x, r_y, r_xy = 2 * y + 1 - x, 2 * (1 - y) + x, 3 - r
    q = 2 * x + c
    d = y * 4 + x * 2 + c

    qkv_at = lambda rr, o, cs: qkv.at[at_rows(rr * 256 + cs * 128, 128, 128), at_rows(o * 384, 384, 128)]
    wo_at = lambda rr, o, cs: wo.at[at_rows(o * 128, 128, 128), at_rows(rr * 256 + cs * 128, 128, 128)]
    s_pc = links.base("pc", 2)
    qkv_third = lambda t, cs: qkv_in.at[t, :, at_rows(cs * 128, 128, 128)]
    qkv_spot = lambda t, cs: qkv.at[at_rows(r * 256 + cs * 128, 128, 128), at_rows(z * 384 + t * 128, 128, 128)]
    s_pc3 = links.base("pc3", 3)
    for t in range(3):
        links.put(qkv_third(t, 1 - c), qkv_spot(t, c), s_pc3 + t, s_pc3 + t, to_c)
    links.put(wo_in.at[at_rows((1 - c) * 128, 128, 128), :], wo_at(r, z, c), s_pc + 1, s_pc + 1, to_c)
    own_qkv = [local(at, qkv_third(t, c), qkv_spot(t, c)) for t, at in enumerate((0, 11, 12))]
    own_wo = local(1, wo_in.at[at_rows(c * 128, 128, 128), :], wo_at(r, z, c))
    for one in own_qkv:
        one.start()
    own_wo.start()

    def move_tokens(key, source, target_at, at):
        base, got = links.base((key, "sent"), 2), links.base((key, "got"), 2)
        target = target_at(z // 2)
        stay = c == z // 2
        rows = at_rows((z % 2) * Q, SENT, 16)
        for i in range(2):
            here = jnp.logical_and(stay, z % 2 == i)
            to = place(y, x, z // 2, 2 * c + i)
            to = (jnp.where(here, place(y, x, 1 - c, z)[0], to[0]), to[1])
            mine = source.at[i, pl.ds(0, SENT)]
            links.put(mine, target.at[rows], base + i, got + z % 2, to, jnp.logical_not(here))

            @pl.when(here)
            def _(mine=mine):
                local(at, mine, target.at[rows]).start()

    def wait_tokens(key, source, target_at, at):
        got = links.base((key, "got"), 2)
        target = target_at(c)
        stay = c == z // 2
        for j in range(2):
            here = jnp.logical_and(stay, z % 2 == j)

            @pl.when(here)
            def _(j=j):
                local(at, source.at[j, pl.ds(0, SENT)], target.at[pl.ds(j * Q, SENT)]).wait()

            @pl.when(jnp.logical_not(here))
            def _(j=j):
                links.wait(target.at[pl.ds(j * Q, SENT)], got + j, to_c)

    up_shard = lambda sx, sc: up.at[at_rows(y * 512 + sx * 256 + sc * 128, 128, 128), at_rows(z * 256, 256, 128)]
    down_shard = lambda sx, sc: down.at[at_rows(z * 256, 256, 128), at_rows(y * 512 + sx * 256 + sc * 128, 128, 128)]
    s_up, s_down = links.base("up", 4), links.base("down", 4)
    own_up = local(6, w1_in.at[:, at_rows(q * 256, 256, 128)], up_shard(x, c))
    own_down = local(7, w2_in.at[at_rows(q * 256, 256, 128), :], down_shard(x, c))
    own_up.start()
    own_down.start()

    def part_up(dx, dc):
        tx, tc, rel = (x + dx) % 2, (c + dc) % 2, 2 * dx + dc
        to = place(y, tx, tc, z)
        links.put(w1_in.at[:, at_rows((2 * tx + tc) * 256, 256, 128)], up_shard(x, c), s_up + rel, s_up + rel, to)

    def part_down(dx, dc):
        tx, tc, rel = (x + dx) % 2, (c + dc) % 2, 2 * dx + dc
        to = place(y, tx, tc, z)
        links.put(w2_in.at[at_rows((2 * tx + tc) * 256, 256, 128), :], down_shard(x, c), s_down + rel, s_down + rel, to)

    def wait_parts(shard, base):
        for dx, dc in ((0, 1), (1, 0), (1, 1)):
            links.wait(shard((x + dx) % 2, (c + dc) % 2), base + 2 * dx + dc, to_c)

    class Fan:
        def __init__(self, key, piece, arrived):
            self.piece, self.arrived = piece, arrived
            self.many = len(piece(0))
            self.got = [links.base((key, "got", n), 4) for n in range(self.many)]
            self.sent = [links.base((key, "sent", n), 3) for n in range(self.many)]

        def push(self, slot, o, to):
            for n in range(self.many):
                def make(n=n):
                    ref = self.piece(o)[n]
                    return ref, ref, self.sent[n] + slot, self.got[n] + o, to, None

                links.start(make)

        def take(self, o):
            for n, ref in enumerate(self.piece(o)):
                links.wait(ref, self.got[n] + o, to_z1)

        def begin(self):
            self.push(1, z, to_z1)
            self.push(0, z, to_z2)
            self.arrived(z)

        def far(self):
            self.take(z2)
            self.push(2, z2, to_z1)
            self.arrived(z2)

        def pair(self):
            self.take(z1)
            self.arrived(z1)

        def diagonal(self):
            self.take(z3)
            self.arrived(z3)

    class Line:
        def __init__(self, key, piece, arrived):
            self.piece, self.arrived = piece, arrived
            self.many = len(piece(0))
            self.got = [links.base((key, "got", n), 4) for n in range(self.many)]
            self.sent = [links.base((key, "sent", n), 8) for n in range(self.many)]

        def push(self, upward, o, there):
            onward = z < 3 if upward else z > 0
            to = place(y, x, c, jnp.minimum(z + 1, 3) if upward else jnp.maximum(z - 1, 0))
            to = (jnp.where(onward, to[0], to_c[0]), to[1])
            for n, ref in enumerate(self.piece(o)):
                links.put(ref, ref, self.sent[n] + 4 * upward + o, self.got[n] + o, to, jnp.logical_and(there, onward))

        def begin(self):
            self.push(1, z, z >= 0)
            self.push(0, z, z >= 0)
            self.arrived(z, None)

        def step(self, far):
            for upward in (1, 0):
                o = z - far if upward else z + far
                there = o >= 0 if upward else o < 4
                o = jnp.clip(o, 0, 3)

                @pl.when(there)
                def _():
                    for n, ref in enumerate(self.piece(o)):
                        links.wait(ref, self.got[n] + o, to_z1)

                self.push(upward, o, there)
                self.arrived(o, there)

    attn_at = (qkv_at, wo_at)

    def attn_whole(o):
        return (
            qkv.at[at_rows(r * 256, 256, 256), at_rows(o * 384, 384, 128)],
            wo.at[at_rows(o * 128, 128, 128), at_rows(r * 256, 256, 256)],
        )

    s_first = [links.base(("first", n), 8) for n in range(2)]
    s_own = [links.base(("own", n), 8) for n in range(2)]
    s_fwd = [links.base(("fwd", n), 8) for n in range(2)]
    to_first, to_second = (to_x, to_y), (to_y, to_x)
    r_first, r_second = (r_x, r_y), (r_y, r_x)

    def attn_arrived(o, there):
        for n, at in enumerate(attn_at):
            for cs in range(2):
                ref, sem = at(r, o, cs), o * 2 + cs
                links.put(ref, ref, s_first[n] + sem, s_first[n] + sem, to_first[cs], there)
        for n, at in enumerate(attn_at):
            for cs in range(2):
                ref, sem = at(r, o, cs), o * 2 + cs
                links.put(ref, ref, s_own[n] + sem, s_own[n] + sem, to_second[cs], there)

    def attn_forward(o, there=None):
        for n, at in enumerate(attn_at):
            for cs in range(2):
                ref, sem = at(r_first[cs], o, cs), o * 2 + cs

                def arrive(n=n, ref=ref, sem=sem):
                    links.wait(ref, s_first[n] + sem, to_x)

                arrive() if there is None else pl.when(there)(arrive)
                links.put(ref, ref, s_fwd[n] + sem, s_fwd[n] + sem, to_second[cs], there)

    def attn_forward_far(far):
        attn_forward(jnp.clip(z - far, 0, 3), z >= far)
        attn_forward(jnp.clip(z + far, 0, 3), z + far < 4)

    def attn_finish():
        for o in range(4):
            for n, at in enumerate(attn_at):
                for cs in range(2):
                    sem = o * 2 + cs
                    links.wait(at(r_second[cs], o, cs), s_own[n] + sem, to_x)
                    links.wait(at(r_xy, o, cs), s_fwd[n] + sem, to_x)

    attn_line = Line("attn", lambda o: attn_whole(o), attn_arrived)
    up_at = lambda yy, o: up.at[at_rows(yy * 512, 512, 512), at_rows(o * 256, 256, 256)]
    down_at = lambda yy, o: down.at[at_rows(o * 256, 256, 256), at_rows(yy * 512, 512, 512)]
    s_upy, s_downy = links.base("upy", 4), links.base("downy", 4)

    def across(at, base):
        return lambda o: links.start(lambda: (at(y, o), at(y, o), base + o, base + o, to_y, None))

    up_fan = Fan("upf", lambda o: (up_at(y, o),), across(up_at, s_upy))
    down_fan = Fan("downf", lambda o: (down_at(y, o),), across(down_at, s_downy))

    lse[...] = jnp.zeros_like(lse)
    for one in own_qkv:
        one.wait()
    own_wo.wait()
    for t in range(3):
        links.wait(qkv_spot(t, 1 - c), s_pc3 + t, to_c)
    links.wait(wo_at(r, z, 1 - c), s_pc + 1, to_c)
    def spread_start(key, ref):
        base = links.base(("spread", key), 3)
        links.start(lambda: (block_at(ref, q), block_at(ref, q), base, base, to_x, None))
        links.start(lambda: (block_at(ref, q), block_at(ref, q), base + 1, base + 1, to_c, None))

    def spread_forward(key, ref):
        base = links.base(("spread", key), 3)
        far = lambda: block_at(ref, 2 * (1 - x) + c)
        links.wait(far(), base, to_x)
        links.start(lambda: (far(), far(), base + 2, base + 2, to_c, None))

    def spread_wait_near(key, ref):
        links.wait(block_at(ref, 2 * x + 1 - c), links.base(("spread", key), 3) + 1, to_c)

    def spread_wait_far(key, ref):
        links.wait(block_at(ref, 2 * (1 - x) + 1 - c), links.base(("spread", key), 3) + 2, to_c)

    attn_line.begin()
    norm_in[0:2, :] = gain_in[...].astype(F32)
    norm_in[2:6, :] = shift_in[...].astype(F32)
    norm_in[6:8, :] = jnp.zeros((2, 128), F32)
    bias_in[0:2, :] = qv_in[:, at_rows(c * 128, 128, 128)].astype(F32)
    bias_in[2:4, :] = jnp.where(q == 0, b1_in[0:2, :], jnp.where(q == 1, b1_in[2:4, :], jnp.where(q == 2, b1_in[4:6, :], b1_in[6:8, :]))).astype(F32)
    bias_in[4:8, :] = jnp.zeros((4, 128), F32)
    length = valid_in.shape[1]
    quarter = length // 4
    source = lax.broadcasted_iota(jnp.int32, (length, FULL), 0)
    target = lax.broadcasted_iota(jnp.int32, (length, FULL), 1)
    chosen = None
    for at in range(4):
        inside = jnp.logical_and(target >= at * Q, target < at * Q + quarter)
        match = jnp.logical_and(inside, target - source == at * (Q - quarter))
        chosen = match if chosen is None else jnp.logical_or(chosen, match)
    spread = mm((valid_in[...] > 0).astype(F32).astype(BF), chosen.astype(F32).astype(BF), NN)
    hidden = jnp.where(spread > 0.5, 0.0, MASKED)
    mask_in[0] = hidden[0:1]
    mask_in[1] = hidden[1:2]
    number = tok_raw.shape[0]
    full_rows = number // 16 * 16
    for one in raw_copies:
        one.wait()
    for one_raw, one_in in ((tok_raw, tok_in), (cot_raw, cot_in)):
        for i in range(2):
            one_in[i, full_rows:Q, :] = jnp.zeros((Q - full_rows, 1024), BF)
            one_in[i, 0:number, :] = one_raw[:, i, :]
    s_norm, s_bias, s_mask = links.base("norm", 8), links.base("bias", 4), links.base("mask", 1)
    for dd in range(1, 8):
        to = place((y + dd // 4) % 2, (x + (dd // 2) % 2) % 2, (c + dd % 2) % 2, z)
        links.put(norm_in, norm.at[d], s_norm + dd, s_norm + dd, to)
    for dz in range(1, 4):
        links.put(bias_in, bias.at[z], s_bias + dz, s_bias + dz, place(y, x, c, (z + dz) % 4))
    links.put(mask_in, mask.at[c], s_mask, s_mask, to_c)
    own_small = (local(2, norm_in, norm.at[d]), local(3, bias_in, bias.at[z]), local(4, mask_in, mask.at[c]))
    for one in own_small:
        one.start()

    attn_line.step(1)
    attn_forward(z)
    attn_line.step(2)
    move_tokens("tok", tok_in, lambda cc: tok, 5)
    move_tokens("cot", cot_in, lambda cc: block_at(cot, 2 * x + cc), 8)
    for one in own_small:
        one.wait()
    for dd in range(1, 8):
        source = 4 * ((y + dd // 4) % 2) + 2 * ((x + (dd // 2) % 2) % 2) + (c + dd % 2) % 2
        links.wait(norm.at[source], s_norm + dd, to_c)
    for dz in range(1, 4):
        links.wait(bias.at[(z + 4 - dz) % 4], s_bias + dz, to_c)
    links.wait(mask.at[1 - c], s_mask, to_c)
    for dd in range(8):
        norm_row[:, dd * 128 : dd * 128 + 128] = norm[dd]
    for zz in range(4):
        qkv_row[:, zz * 384 : zz * 384 + 128] = bias[zz, 0:1]
        qkv_row[:, zz * 384 + 128 : zz * 384 + 256] = jnp.zeros((1, 128), F32)
        qkv_row[:, zz * 384 + 256 : zz * 384 + 384] = bias[zz, 1:2]
        up_row[:, zz * 256 : zz * 256 + 128] = bias[zz, 2:3]
        up_row[:, zz * 256 + 128 : zz * 256 + 256] = bias[zz, 3:4]
    attn_forward_far(1)
    attn_line.step(3)
    attn_forward_far(2)
    for dx, dc in ((1, 0), (1, 1), (0, 1)):
        part_up(dx, dc)
    for dx, dc in ((1, 0), (1, 1), (0, 1)):
        part_down(dx, dc)
    own_up.wait()
    own_down.wait()
    wait_tokens("tok", tok_in, lambda cc: tok, 5)

    @pl.loop(0, HALF // 32)
    def _(i):
        v = tok[at_rows(i * 32, 32, 32), :].astype(F32)
        unit, _ = unit_rows(v)
        n1[at_rows(c * HALF + i * 32, 32, 32), :] = (unit * norm_row[0:1] + norm_row[2:3]).astype(BF)

    s_n1 = links.base("n1", 1)
    half_at = lambda ref, cc: ref.at[at_rows(cc * HALF, HALF, 64), :]
    links.put(half_at(n1, c), half_at(n1, c), s_n1, s_n1, to_c)
    attn_forward_far(3)
    wait_parts(up_shard, s_up)
    up_fan.begin()
    wait_parts(down_shard, s_down)
    down_fan.begin()
    links.wait(half_at(n1, 1 - c), s_n1, to_c)
    attn_finish()

    @pl.loop(0, 6)
    def _(j):
        columns = at_rows(j * 256, 256, 256)
        proj[:, columns] = (mm(n1[...], qkv[:, columns], NN) + qkv_row[:, columns]).astype(BF)

    lane = lax.broadcasted_iota(jnp.int32, (1, 128), 1)
    first_head = lane < 64
    zero = jnp.zeros((), BF)
    factor = jnp.asarray(HD ** (-0.5), BF)

    @pl.loop(0, 4)
    def _(zz):
        keys = proj[:, at_rows(zz * 384 + 128, 128, 128)]
        values = proj[:, at_rows(zz * 384 + 256, 128, 128)]
        hidden_key = mask[z // 2, z % 2]
        for rb in range(2):
            rows = pl.ds(rb * HALF, HALF)
            pair = proj[rows, at_rows(zz * 384, 128, 128)]
            outs = []
            for hh in range(2):
                own = jnp.where(first_head if hh == 0 else jnp.logical_not(first_head), pair, zero)
                scores = mm(own * factor, keys, NT) + hidden_key
                highest = jnp.max(scores, axis=-1, keepdims=True)
                exponent = jnp.exp(scores - highest)
                total = jnp.sum(exponent, axis=-1, keepdims=True)
                low = (exponent * (1.0 / total)).astype(BF)
                head = 2 * zz + hh
                lse[rows, :] = jnp.where(lane == head, highest + jnp.log(total), lse[rows, :])
                outs.append(mm(low, values, NN))
            mix[rows, at_rows(zz * 128, 128, 128)] = jnp.where(first_head, outs[0], outs[1]).astype(BF)

        @pl.when(zz == 0)
        def _():
            wait_tokens("cot", cot_in, lambda cc: block_at(cot, 2 * x + cc), 8)
            spread_start("cot", cot)

        @pl.when(zz == 1)
        def _():
            up_fan.pair()

    s_part = links.base("part", 1)

    def project_out(cc, target):
        @pl.loop(0, 4)
        def _(j):
            columns = at_rows(j * 256, 256, 256)
            target[:, columns] = mm(mix[at_rows(cc * HALF, HALF, 64), :], wo[:, columns], NN)

    project_out(1 - c, part)
    links.put(part, got_part, s_part, s_part, to_c)
    project_out(c, hid)
    links.wait(got_part, s_part, to_c)

    @pl.loop(0, HALF // 32)
    def _(i):
        rows = at_rows(i * 32, 32, 32)
        v = hid[rows, :] + got_part[rows, :] + tok[rows, :].astype(F32) + norm_row[4:5]
        hid[rows, :] = v
        unit, _ = unit_rows(v)
        n2[block_rows(q, i * 32, 32), :] = (unit * norm_row[1:2] + norm_row[3:4]).astype(BF)

    spread_start("n2", n2)
    up_fan.far()
    down_fan.pair()
    spread_forward("cot", cot)
    spread_wait_near("cot", cot)

    def expand(o, start, blocks):
        columns = at_rows(o * 256, 256, 256)

        @pl.loop(0, blocks)
        def _(i):
            rows = at_rows(start + i * Q, Q, 32)
            v = mm(n2[rows, :], up[:, columns], NN) + up_row[:, columns]
            value, grade = gelu_both(v)
            act[rows, columns] = value.astype(BF)
            slope[rows, columns] = grade.astype(BF)

    n1_t[...] = n1[...].T
    spread_wait_near("n2", n2)
    for at, o in enumerate((z, z1, z2, z3)):
        links.wait(up_at(1 - y, o), s_upy + o, to_y)
        expand(o, 2 * x * HALF, 4)
        if at == 0:
            up_fan.diagonal()
        if at == 2:
            down_fan.far()
    spread_forward("n2", n2)
    for at, o in enumerate((z, z1, z2, z3)):
        expand(o, (2 * (1 - x) + c) * HALF, 2)
    down_fan.diagonal()
    spread_wait_far("n2", n2)
    for o in (z, z1, z2, z3):
        expand(o, (2 * (1 - x) + 1 - c) * HALF, 2)
    spread_wait_far("cot", cot)

    forward_sends = len(links.sends)
    near_other, far_own, far_other = 2 * x + 1 - c, 2 * (1 - x) + c, 2 * (1 - x) + 1 - c
    sums[...] = jnp.zeros_like(sums)
    gb1[...] = jnp.zeros_like(gb1)

    def fold(v):
        return v[0:8] + v[8:16] + v[16:24] + v[24:32]

    def tally(row, v):
        sums[row * 8 : row * 8 + 8, :] += fold(v)

    def send_later(make):
        links.start(make)

    def through_slope(t):
        @pl.loop(0, 4)
        def _(j):
            columns = at_rows(j * 256, 256, 256)
            rows = block_rows(t, 0, HALF)
            v = mm(cot[rows, :], down[columns, :], NT) * slope[rows, columns].astype(F32)
            gb1[:, columns] += jnp.sum(v.reshape(HALF // 8, 8, 256), axis=0)
            slope[rows, columns] = v.astype(BF)

    def back_part(t, target):
        @pl.loop(0, 4)
        def _(j):
            columns = at_rows(j * 256, 256, 256)
            target[:, columns] = mm(slope[block_rows(t, 0, HALF), :], up[columns, :], NT).astype(target.dtype)

    def add_rows(target, *sources):
        @pl.loop(0, HALF // 32)
        def _(i):
            rows = at_rows(i * 32, 32, 32)
            total = sources[0][rows, :].astype(F32)
            for source in sources[1:]:
                total = total + source[rows, :].astype(F32)
            target[rows, :] = total.astype(target.dtype)

    z_order = (z3, z1, z2, z)
    s_rdown, s_rup = links.base("rdown", 4), links.base("rup", 4)
    d_down_at = lambda yy, o: d_down.at[at_rows(o * 256, 256, 256), at_rows(yy * 512, 512, 512)]
    d_up_at = lambda yy, o: d_up.at[at_rows(yy * 512, 512, 512), at_rows(o * 256, 256, 256)]
    r_down_at = lambda o: r_down.at[at_rows(o * 256, 256, 256), :]
    r_up_at = lambda o: r_up.at[:, at_rows(o * 256, 256, 256)]

    def accumulate(target, *sources):
        step = 64 if target.shape[0] % 64 == 0 else 32
        count = target.shape[0] // step

        @pl.loop(0, count)
        def _(i):
            rows = at_rows(i * step, step, step)
            total = target[rows, :].astype(F32)
            for source in sources:
                total = total + source[rows, :].astype(F32)
            target[rows, :] = total.astype(target.dtype)

    class Fold:
        def __init__(self, key, piece, over_z, final):
            self.piece, self.over_z, self.final = piece, over_z, final
            self.sz = links.base((key, "z"), 3)

        def push(self, o, slot, to):
            links.start(lambda: (self.piece(o), self.over_z.at[slot], self.sz + slot, self.sz + slot, to, None))

        def pair_far(self):
            self.collect(z3)
            self.push(z3, 0, to_z1)

        def pair_near(self):
            self.collect(z1)
            self.push(z1, 1, to_z1)

        def far(self):
            self.collect(z2)
            links.wait(self.over_z.at[0], self.sz, to_z1)
            accumulate(self.piece(z2), self.over_z.at[0])
            self.push(z2, 2, to_z2)

        def last(self):
            self.collect(z)
            links.wait(self.over_z.at[1], self.sz + 1, to_z1)
            links.wait(self.over_z.at[2], self.sz + 2, to_z2)
            own, others = self.piece(z), [self.over_z.at[1], self.over_z.at[2]]
            count = own.shape[0] // 64

            @pl.loop(0, count)
            def _(i):
                rows = at_rows(i * 64, 64, 64)
                total = own[rows, :].astype(F32)
                for other in others:
                    total = total + other[rows, :].astype(F32)
                self.final[rows, :] = total.astype(BF)

    class Half(Fold):
        def __init__(self, key, at, got_at, s_got, over_z, final):
            super().__init__(key, lambda o: at(y, o), over_z, final)
            self.got_at, self.s_got = got_at, s_got

        def collect(self, o):
            links.wait(self.got_at(o), self.s_got + o, to_y)
            accumulate(self.piece(o), self.got_at(o))

    half_down = Half("half_down", d_down_at, r_down_at, s_rdown, z_down, f_down)
    half_up = Half("half_up", d_up_at, r_up_at, s_rup, z_up, f_up)

    def give_down(o):
        rows = at_rows(o * 256, 256, 256)
        d_down[rows, :] = mm(act[:, rows], cot[...], TN).astype(BF)
        links.start(lambda: (d_down_at(1 - y, o), r_down_at(o), s_rdown + o, s_rdown + o, to_y, None))

    def give_up(o):
        columns = at_rows(o * 256, 256, 256)
        d_up[:, columns] = mm(n2[...], slope[:, columns], TN).astype(BF)
        links.start(lambda: (d_up_at(1 - y, o), r_up_at(o), s_rup + o, s_rup + o, to_y, None))

    for o in z_order:
        give_down(o)
    for o in range(4):
        links.wait(down_at(1 - y, o), s_downy + o, to_y)
    links.reuse(forward_sends, ("rdown",))

    s_gfar, s_gmid, s_gnear = links.base("gfar", 1), links.base("gmid", 1), links.base("gnear", 1)
    s_bfar, s_bmid, s_bnear = links.base("bfar", 1), links.base("bmid", 1), links.base("bnear", 1)
    through_slope(far_other)
    back_part(far_other, s_far)
    links.put(s_far, g_far, s_gfar, s_gfar, to_c)
    through_slope(far_own)
    back_part(far_own, part)
    links.wait(g_far, s_gfar, to_c)
    add_rows(s_mid, part, g_far)
    links.put(s_mid, g_mid, s_gmid, s_gmid, to_x)
    half_down.pair_far()
    through_slope(near_other)
    back_part(near_other, s_near)
    links.put(s_near, g_near, s_gnear, s_gnear, to_c)
    half_down.pair_near()
    through_slope(q)
    back_part(q, part)
    def down_part(t, target, base=None):
        @pl.loop(0, 4)
        def _(j):
            columns = at_rows(j * 256, 256, 256)
            v = mm(act[block_rows(t, 0, HALF), :], down[:, columns], NN)
            target[:, columns] = (v if base is None else v + base[:, columns]).astype(target.dtype)

    links.copy(s_far, g_far, s_gfar, s_gfar, to_c).wait_send()
    links.drop(s_gfar)
    down_part(far_other, s_far)
    links.put(s_far, b_far, s_bfar, s_bfar, to_c)
    down_part(far_own, got_part)
    half_down.far()
    give_up(z3)
    give_up(z1)
    links.wait(b_far, s_bfar, to_c)
    links.copy(s_mid, g_mid, s_gmid, s_gmid, to_x).wait_send()
    links.drop(s_gmid)
    add_rows(s_mid, got_part, b_far)
    links.put(s_mid, b_mid, s_bmid, s_bmid, to_x)
    give_up(z2)
    give_up(z)

    links.wait(g_near, s_gnear, to_c)
    links.wait(g_mid, s_gmid, to_x)

    @pl.loop(0, HALF // 32)
    def _(i):
        rows = at_rows(i * 32, 32, 32)
        grad = part[rows, :] + g_near[rows, :].astype(F32) + g_mid[rows, :].astype(F32)
        unit, scale = unit_rows(hid[rows, :])
        out = cot[block_rows(q, i * 32, 32), :].astype(F32)
        scaled = grad * norm_row[1:2]
        moved = scale * (
            scaled
            - jnp.mean(scaled, axis=-1, keepdims=True)
            - unit * jnp.mean(scaled * unit, axis=-1, keepdims=True)
        )
        total = out + moved
        tally(1, grad * unit)
        tally(3, grad)
        tally(4, total)
        tally(5, out)
        got_part[rows, :] = total
        ga[at_rows(c * HALF + i * 32, 32, 32), :] = total.astype(BF)

    s_ga = links.base("ga", 1)
    links.put(half_at(ga, c), half_at(ga, c), s_ga, s_ga, to_c)

    links.copy(s_near, g_near, s_gnear, s_gnear, to_c).wait_send()
    links.drop(s_gnear)
    down_part(near_other, s_near)
    links.put(s_near, b_near, s_bnear, s_bnear, to_c)
    down_part(q, hid, hid)
    half_up.pair_far()
    links.wait(half_at(ga, 1 - c), s_ga, to_c)

    @pl.loop(0, 2)
    def _(j):
        columns = at_rows(j * 256, 256, 256)
        gmix[:, columns] = mm(ga[...], wo[columns, :], NT).astype(BF)

    @pl.loop(0, 2)
    def _(j):
        columns = at_rows(j * 256, 256, 256)
        d_wo[columns, :] = mm(mix[:, columns], ga[...], TN).astype(BF)

    d_qkv_at = lambda rr, o, start, size: d_qkv.at[at_rows(rr * 256 + start, size, 32), at_rows(o * 384, 384, 128)]
    d_wo_at = lambda rr, o, start, size: d_wo.at[at_rows(o * 128, 128, 128), at_rows(rr * 256 + start, size, 128)]

    class Reduce(Fold):
        def __init__(self, key, at, parts, first, second, over_z, final):
            super().__init__(key, lambda o: at(r, o, 0, parts[-1][0] + parts[-1][1]), over_z, final)
            self.at, self.parts, self.first, self.second = at, parts, first, second
            self.s1 = [links.base((key, "first", i), 4 * len(parts)) for i in range(2)]
            self.s2 = links.base((key, "second"), 4 * len(parts))

        def block(self, rr, o, p):
            return self.at(rr, o, self.parts[p][0], self.parts[p][1])

        def spot(self, ref, p):
            return cut_of(self, ref, self.parts[p][0], self.parts[p][1])

        def make(self, o, p, i):
            way = self.parts[p][2]
            rr, sem = (r_first[way] if i == 0 else r_xy), self.s1[i] + (len(self.parts) * o + p)
            return self.block(rr, o, p), self.spot(self.first.at[i, o], p), sem, sem, to_first[way], None

        def offer(self, o):
            for p in range(len(self.parts)):
                for i in (1, 0):
                    links.each(functools.partial(self.make, o, p, i), lambda copy: copy.start())

        def promised(self):
            for o in range(4):
                for p in range(len(self.parts)):
                    for i in range(2):
                        links.sends.append(functools.partial(self.make, o, p, i))

        def middle(self, o):
            for p in range(len(self.parts)):
                way = self.parts[p][2]
                got = self.spot(self.first.at[1, o], p)
                links.wait(got, self.s1[1] + (len(self.parts) * o + p), to_x)
                accumulate(self.block(r_second[way], o, p), got)

                def make(p=p, way=way):
                    sem = self.s2 + (len(self.parts) * o + p)
                    return self.block(r_second[way], o, p), self.spot(self.second.at[o], p), sem, sem, to_second[way], None

                links.start(make)

        def collect(self, o):
            for p in range(len(self.parts)):
                links.wait(self.spot(self.first.at[0, o], p), self.s1[0] + (len(self.parts) * o + p), to_x)
                links.wait(self.spot(self.second.at[o], p), self.s2 + (len(self.parts) * o + p), to_x)
            accumulate(self.piece(o), self.first.at[0, o], self.second.at[o])

    def cut_of(owner, ref, start, size):
        return ref.at[pl.ds(start, size), :] if owner.by_rows else ref.at[:, pl.ds(start, size)]

    Reduce.by_rows = True
    red_wo = Reduce("red_wo", d_wo_at, ((0, 256, 0),), first_wo, second_wo, z_wo, f_wo)
    red_wo.by_rows = False
    red_qkv = Reduce("red_qkv", d_qkv_at, ((0, 160, 0), (160, 96, 1)), first_qkv, second_qkv, z_qkv, f_qkv)
    for o in z_order:
        red_wo.offer(o)
    red_wo.promised()

    half_up.pair_near()

    s_oup, s_odown = links.base("oup", 4), links.base("odown", 4)

    def scatter_down():
        for dx, dc in ((1, 0), (1, 1), (0, 1)):
            def make(dx=dx, dc=dc):
                rel, tx, tc = 2 * dx + dc, (x + dx) % 2, (c + dc) % 2
                columns = at_rows((2 * tx + tc) * 128, 128, 128)
                return f_down.at[:, columns], o_down.at[q], s_odown + rel, s_odown + rel, place(y, tx, tc, z), None

            links.start(make)

    def scatter_up():
        for dx, dc in ((1, 0), (1, 1), (0, 1)):
            def make(dx=dx, dc=dc):
                rel, tx, tc = 2 * dx + dc, (x + dx) % 2, (c + dc) % 2
                rows = at_rows((2 * tx + tc) * 128, 128, 128)
                return f_up.at[rows, :], o_up.at[q], s_oup + rel, s_oup + rel, place(y, tx, tc, z), None

            links.start(make)

    def send_home(key, source, target, at):
        base, got = links.base((key, "sent"), 2), links.base((key, "got"), 2)
        for j in range(2):
            def make(j=j):
                here = jnp.logical_and(z // 2 == c, z == 2 * c + j)
                to = place(y, x, z // 2, 2 * c + j)
                to = (jnp.where(here, place(y, x, 1 - c, z)[0], to[0]), to[1])
                return source.at[pl.ds(j * Q, SENT)], target.at[z % 2, pl.ds(0, SENT)], base + j, got + z % 2, to, jnp.logical_not(here)

            links.start(make)

            @pl.when(jnp.logical_and(z // 2 == c, z == 2 * c + j))
            def _(j=j):
                local(at, source.at[pl.ds(j * Q, SENT)], target.at[z % 2, pl.ds(0, SENT)]).start()

    def wait_home(key, source, target, at):
        got = links.base((key, "got"), 2)
        for i in range(2):
            here = jnp.logical_and(z // 2 == c, z % 2 == i)

            @pl.when(here)
            def _(i=i):
                local(at, source.at[pl.ds(0, SENT)], target.at[i, pl.ds(0, SENT)]).wait()

            @pl.when(jnp.logical_not(here))
            def _(i=i):
                links.wait(target.at[i, pl.ds(0, SENT)], got + i, to_c)

    def finish_block():
        links.wait(b_near, s_bnear, to_c)
        links.wait(b_mid, s_bmid, to_x)
        links.copy(s_near, b_near, s_bnear, s_bnear, to_c).wait_send()

        @pl.loop(0, HALF // 32)
        def _(i):
            rows = at_rows(i * 32, 32, 32)
            total = hid[rows, :] + b_near[rows, :].astype(F32) + b_mid[rows, :].astype(F32) + norm_row[5:6]
            s_near[rows, :] = total.astype(BF)

        send_home("block", s_near, block_out, 9)

    links.drop(s_bnear)

    kept = []

    def keep(at, source, target):
        kept.append(local(at, source, target))
        kept[-1].start()

    @pl.loop(0, 4)
    def _(kk):
        zz = 2 * ((z // 2 + 1 - kk % 2) % 2) + (z % 2 + 1 - kk // 2) % 2
        base = zz * 384
        keys = proj[:, at_rows(base + 128, 128, 128)]
        values = proj[:, at_rows(base + 256, 128, 128)]
        hidden_key = mask[z // 2, z % 2]
        d_keys = d_values = None
        sum_queries = None
        for rb in range(2):
            rows = pl.ds(rb * HALF, HALF)
            pair = proj[rows, at_rows(base, 128, 128)]
            grads = gmix[rows, at_rows(zz * 128, 128, 128)]
            outs = []
            for hh in range(2):
                keep = first_head if hh == 0 else jnp.logical_not(first_head)
                own = jnp.where(keep, pair, zero)
                own_grad = jnp.where(keep, grads, zero)
                level = jnp.sum(jnp.where(lane == 2 * zz + hh, lse[rows, :], 0.0), axis=-1, keepdims=True)
                attention = jnp.exp(mm(own, keys, NT) * (HD ** (-0.5)) + hidden_key - level)
                grad_attention = mm(own_grad, values, NT)
                inner = jnp.sum(attention * grad_attention, axis=-1, keepdims=True)
                low = (attention * (grad_attention - inner)).astype(BF)
                more_values = mm(attention.astype(BF), own_grad, TN)
                more_keys = mm(low, own, TN)
                d_values = more_values if d_values is None else d_values + more_values
                d_keys = more_keys if d_keys is None else d_keys + more_keys
                outs.append(mm(low, keys, NN))
            d_queries = jnp.where(first_head, outs[0], outs[1]) * (HD ** (-0.5))
            total = jnp.sum(d_queries.reshape(HALF // 8, 8, 128), axis=0)
            sum_queries = total if sum_queries is None else sum_queries + total
            gproj[rows, at_rows(base, 128, 128)] = d_queries.astype(BF)
        gproj[:, at_rows(base + 128, 128, 128)] = (d_keys * (HD ** (-0.5))).astype(BF)
        gproj[:, at_rows(base + 256, 128, 128)] = d_values.astype(BF)
        gbq[:, at_rows(zz * 128, 128, 128)] = sum_queries
        gbv[:, at_rows(zz * 128, 128, 128)] = jnp.sum(d_values.reshape(FULL // 8, 8, 128), axis=0)

        columns = at_rows(base, 384, 128)
        for rr in range(4):
            rows = pl.ds(rr * 256, 256)
            d_qkv[rows, columns] = mm(n1_t[rows, :], gproj[:, columns], NN).astype(BF)
        red_qkv.offer(zz)

        @pl.when(kk == 0)
        def _():
            finish_block()

        @pl.when(kk == 1)
        def _():
            half_up.far()

        @pl.when(kk == 2)
        def _():
            red_qkv.middle(z3)

        @pl.when(kk == 3)
        def _():
            for o in z_order:
                red_wo.middle(o)

    red_qkv.promised()
    for zz in range(4):
        flat = lambda ref, start: jnp.sum(ref[:, start : start + 128], axis=0, keepdims=True)
        bias_pack[zz, 0:1] = flat(gbq, zz * 128)
        bias_pack[zz, 1:2] = flat(gbv, zz * 128)
        bias_pack[zz, 2:3] = flat(gb1, zz * 256)
        bias_pack[zz, 3:4] = flat(gb1, zz * 256 + 128)
        bias_pack[zz, 4:8] = jnp.zeros((4, 128), F32)
    s_bz, s_ball = links.base("bz", 4), links.base("ball", 8)
    for dz in range(1, 4):
        def make(dz=dz):
            tz = (z + dz) % 4
            return bias_pack.at[tz], bias_got.at[dz], s_bz + dz, s_bz + dz, place(y, x, c, tz), None

        links.start(make)

    def front_part(cc, target):
        @pl.loop(0, 4)
        def _(j):
            columns = at_rows(j * 256, 256, 256)
            target[:, columns] = mm(gproj[at_rows(cc * HALF, HALF, 64), :], qkv[columns, :], NT).astype(target.dtype)

    s_gn1 = links.base("gn1", 1)
    links.copy(s_far, b_far, s_bfar, s_bfar, to_c).wait_send()
    links.drop(s_bfar)
    front_part(1 - c, s_far)
    links.put(s_far, g_n1, s_gn1, s_gn1, to_c)
    front_part(c, part)
    links.wait(g_n1, s_gn1, to_c)
    links.copy(s_mid, b_mid, s_bmid, s_bmid, to_x).wait_send()
    links.drop(s_bmid)

    @pl.loop(0, HALF // 32)
    def _(i):
        rows = at_rows(i * 32, 32, 32)
        grad = part[rows, :] + g_n1[rows, :].astype(F32)
        unit, scale = unit_rows(tok[rows, :].astype(F32))
        scaled = grad * norm_row[0:1]
        moved = scale * (
            scaled
            - jnp.mean(scaled, axis=-1, keepdims=True)
            - unit * jnp.mean(scaled * unit, axis=-1, keepdims=True)
        )
        tally(0, grad * unit)
        tally(2, grad)
        s_mid[rows, :] = (got_part[rows, :] + moved).astype(BF)

    for row in range(6):
        sums_row[row : row + 1, :] = jnp.sum(sums[row * 8 : row * 8 + 8, :], axis=0, keepdims=True)
    sums_row[6:8, :] = jnp.zeros((2, 1024), F32)
    for dd in range(8):
        norm[dd] = sums_row[:, dd * 128 : dd * 128 + 128]
    s_sum, s_sumz = links.base("sum", 8), links.base("sumz", 4)
    for dd in range(1, 8):
        def make(dd=dd):
            ty, tx, tc = (y + dd // 4) % 2, (x + (dd // 2) % 2) % 2, (c + dd % 2) % 2
            return norm.at[4 * ty + 2 * tx + tc], sums_got.at[dd], s_sum + dd, s_sum + dd, place(ty, tx, tc, z), None

        links.start(make)
    send_home("home", s_mid, grad_out, 10)
    for o in (z1, z2):
        red_qkv.middle(o)
    red_qkv.pair_far()
    red_qkv.pair_near()
    red_qkv.middle(z)
    red_qkv.far()
    red_wo.pair_far()
    red_wo.pair_near()
    red_wo.far()
    half_down.last()
    scatter_down()
    keep(17, f_down.at[:, at_rows(q * 128, 128, 128)], o_down.at[q])
    half_up.last()
    scatter_up()
    keep(18, f_up.at[at_rows(q * 128, 128, 128), :], o_up.at[q])
    for dz in range(1, 4):
        links.wait(bias_got.at[dz], s_bz + dz, to_c)
    bias_own[...] = bias_pack[z] + bias_got[1] + bias_got[2] + bias_got[3]
    keep(13, bias_own, bias_all.at[d])
    for dd in range(1, 8):
        def make(dd=dd):
            to = place((y + dd // 4) % 2, (x + (dd // 2) % 2) % 2, (c + dd % 2) % 2, z)
            return bias_own, bias_all.at[d], s_ball + dd, s_ball + dd, to, None

        links.start(make)
    for dd in range(1, 8):
        links.wait(sums_got.at[dd], s_sum + dd, to_c)
    total = norm[d]
    for dd in range(1, 8):
        total = total + sums_got[dd]
    sums_own[...] = total
    keep(14, sums_own, sums_z.at[0])
    for dz in range(1, 4):
        def make(dz=dz):
            return sums_own, sums_z.at[dz], s_sumz + dz, s_sumz + dz, place(y, x, c, (z + dz) % 4), None

        links.start(make)
    red_wo.last()
    s_owo = links.base("owo", 1)
    links.put(f_wo.at[:, at_rows((1 - c) * 128, 128, 128)], o_wo.at[c], s_owo, s_owo, to_c)
    keep(16, f_wo.at[:, at_rows(c * 128, 128, 128)], o_wo.at[c])

    for dx, dc in ((1, 0), (1, 1), (0, 1)):
        rel, source = 2 * dx + dc, 2 * ((x + dx) % 2) + (c + dc) % 2
        links.wait(o_up.at[source], s_oup + rel, to_c)
        links.wait(o_down.at[source], s_odown + rel, to_c)

    for dd in range(1, 8):
        source = 4 * ((y + dd // 4) % 2) + 2 * ((x + (dd // 2) % 2) % 2) + (c + dd % 2) % 2
        links.wait(bias_all.at[source], s_ball + dd, to_c)
    for dz in range(1, 4):
        links.wait(sums_z.at[dz], s_sumz + dz, to_c)

    red_qkv.last()
    s_oqkv, s_owo = links.base("oqkv", 1), links.base("owo", 1)
    links.put(f_qkv.at[at_rows((1 - c) * 128, 128, 128), :], o_qkv.at[c], s_oqkv, s_oqkv, to_c)
    keep(15, f_qkv.at[at_rows(c * 128, 128, 128), :], o_qkv.at[c])
    links.wait(o_qkv.at[1 - c], s_oqkv, to_c)
    links.wait(o_wo.at[1 - c], s_owo, to_c)
    wait_home("block", s_near, block_out, 9)
    wait_home("home", s_mid, grad_out, 10)
    for one in kept:
        one.wait()
    links.finish()
    assert links.got_at["next"] <= recv_sem.shape[0]
    assert links.sent_at["next"] <= send_sem.shape[0]


def layer_call(*operands):
    shape = jax.ShapeDtypeStruct
    hbm, vmem = pl.BlockSpec(memory_space=pl.ANY), pl.BlockSpec(memory_space=pltpu.VMEM)
    outs = [
        shape((2, Q, 1024), BF), shape((2, Q, 1024), BF), shape((4, 128, 256), BF), shape((4, 256, 128), BF),
        shape((2, 128, 384), BF), shape((2, 128, 128), BF), shape((8, 8, 128), F32), shape((4, 8, 128), F32),
    ]
    low = lambda *dims: pltpu.VMEM(dims, BF)
    wide = lambda *dims: pltpu.VMEM(dims, F32)
    scratch = [
        low(*operands[0].shape), low(*operands[0].shape), low(2, Q, 1024), low(2, Q, 1024), wide(2, 1, FULL), wide(8, 128), wide(8, 128),
        low(HALF, 1024), low(4 * HALF, 1024), wide(2, 2, 1, FULL), wide(8, 8, 128), wide(4, 8, 128),
        low(1024, 1536), low(512, 1024), low(1024, 1024), low(1024, 1024),
        low(FULL, 1024), low(FULL, 1536), wide(FULL, 128), low(FULL, 512), wide(HALF, 1024),
        low(4 * HALF, 1024), low(4 * HALF, 1024), low(4 * HALF, 1024),
        wide(8, 1024), wide(1, 1536), wide(1, 1024), wide(HALF, 1024), wide(HALF, 1024),
        low(1024, FULL), low(FULL, 1024), low(FULL, 512), low(FULL, 1536),
        low(1024, 1024), low(1024, 1024), low(1024, 1536), low(512, 1024),
        low(512, 1024), low(1024, 512), low(3, 512, 256), low(3, 256, 512),
        low(512, 256), low(256, 512),
        low(2, 4, 256, 384), low(2, 4, 128, 256), low(4, 256, 384), low(4, 128, 256),
        low(3, 256, 384), low(3, 128, 256), low(256, 384), low(128, 256),
        *[low(HALF, 1024)] * 10,
        wide(48, 1024), wide(8, 1024), wide(8, 8, 128), wide(8, 128),
        wide(8, 1024), wide(8, 512), wide(8, 512), wide(4, 8, 128), wide(4, 8, 128), wide(8, 128),
        pltpu.SemaphoreType.DMA((21,)), pltpu.SemaphoreType.DMA((130,)), pltpu.SemaphoreType.DMA((212,)),
    ]
    return pl.pallas_call(
        layer_kernel,
        out_shape=outs,
        in_specs=[hbm] * 2 + [vmem] * 5 + [hbm] * 4,
        out_specs=[hbm] * 8,
        scratch_shapes=scratch,
        compiler_params=pltpu.CompilerParams(collective_id=0, has_side_effects=True, vmem_limit_bytes=67043328),
        name="layer",
    )(*operands)


def finish_kernel(
    block_in, grad_in, up_in, down_in, qkv_in, wo_in, bias_in, sums_in,
    block, grad, gain, shift, qkv, qv, wo, w1, b1, w2,
):
    rows = grad.shape[0]
    for i in range(2):
        grad[:, i, :] = grad_in[i, 0:rows, :].astype(F32)
    block[...] = jnp.stack([block_in[0, 0:rows, :], block_in[1, 0:rows, :]], axis=1)
    total = sums_in[0] + sums_in[1] + sums_in[2] + sums_in[3]
    gain[...] = total[0:2]
    shift[...] = total[2:6]
    for cc in range(2):
        lanes = pl.ds(cc * 128, 128)
        for t in range(3):
            qkv[t, :, lanes] = qkv_in[cc, :, t * 128 : t * 128 + 128].astype(F32)
        qv[:, lanes] = (bias_in[cc] + bias_in[2 + cc] + bias_in[4 + cc] + bias_in[6 + cc])[0:2]
        wo[pl.ds(cc * 128, 128), :] = wo_in[cc].astype(F32)
    for qq in range(4):
        w1[:, pl.ds(qq * 256, 256)] = up_in[qq].astype(F32)
        w2[pl.ds(qq * 256, 256), :] = down_in[qq].astype(F32)
        b1[pl.ds(qq * 2, 2), :] = (bias_in[qq] + bias_in[4 + qq])[2:4]


def finish_call(rows, *parts):
    shape = jax.ShapeDtypeStruct
    return pl.pallas_call(
        finish_kernel,
        out_shape=[
            shape((rows, 2, 1024), BF), shape((rows, 2, 1024), F32), shape((2, 128), F32), shape((4, 128), F32),
            shape((3, 128, 256), F32), shape((2, 256), F32), shape((256, 128), F32), shape((128, 1024), F32),
            shape((8, 128), F32), shape((1024, 128), F32),
        ],
        in_specs=[pl.BlockSpec(memory_space=pltpu.VMEM)] * 8,
        out_specs=[pl.BlockSpec(memory_space=pltpu.VMEM)] * 10,
        name="finish",
    )(*parts)


def fast_body(inputs, valid_mask, cotangent, ln_gain, d_bias, w_qkv, b_qv, w_o, w_1, b_1, w_2):
    rows = inputs.shape[0]
    parts = layer_call(
        inputs, cotangent, valid_mask, ln_gain, d_bias, b_qv, b_1.reshape(8, 128),
        jnp.transpose(w_qkv, (1, 0, 2)), w_o, w_1, w_2,
    )
    block, grad, gain, shift, qkv, qv, wo, w1, b1, w2 = finish_call(rows, *parts)
    return block, grad, gain, shift, jnp.transpose(qkv, (1, 0, 2)), qv, wo, w1, b1.reshape(1024), w2


def solution(mesh):
    in_specs = (
        P("tensor", "dp", None),
        P("dp", None),
        P("tensor", "dp", None),
        P(None, "dp"),
        P(None, "dp"),
        P("dp", None, "tensor"),
        P(None, "tensor"),
        P("tensor", "dp"),
        P("dp", "tensor"),
        P("tensor"),
        P("tensor", "dp"),
    )
    out_specs = (
        P("tensor", "dp", None),
        P("tensor", "dp", None),
        P(None, "dp"),
        P(None, "dp"),
        P("dp", None, "tensor"),
        P(None, "tensor"),
        P("tensor", "dp"),
        P("dp", "tensor"),
        P("tensor"),
        P("tensor", "dp"),
    )
    run = fast_body if dict(mesh.shape) == {"dp": 8, "tensor": 4} else body
    return jax.shard_map(run, mesh=mesh, in_specs=in_specs, out_specs=out_specs, check_vma=False)
```
